256 devices in a mesh: rep: 1, dp: 256 (over x, y, z, core).
Axes of the slice: x: 4, y: 4, z: 8, core: 2. Of those that a mesh axis runs over, the one named last changes fastest.
Arguments:
- x: bfloat16 [256, 1024, 1024], P(('rep', 'dp'))
- dy: bfloat16 [256, 1024, 1024], P(('rep', 'dp'))
- w_gate: bfloat16 [2, 1024, 3328], replicated
- w_up: bfloat16 [2, 1024, 3328], replicated
- w_down: bfloat16 [2, 3328, 1024], replicated
- m_w_gate: float32 [2, 1024, 3328], P(None, 'dp')
- m_w_up: float32 [2, 1024, 3328], P(None, 'dp')
- m_w_down: float32 [2, 3328, 1024], P(None, 'dp')
- v_w_gate: float32 [2, 1024, 3328], P(None, 'dp')
- v_w_up: float32 [2, 1024, 3328], P(None, 'dp')
- v_w_down: float32 [2, 3328, 1024], P(None, 'dp')
Outputs:
- output 1: bfloat16 [2, 1024, 3328], P('rep')
- output 2: bfloat16 [2, 1024, 3328], P('rep')
- output 3: bfloat16 [2, 3328, 1024], P('rep')
- output 4: float32 [2, 1024, 3328], P('rep', 'dp')
- output 5: float32 [2, 1024, 3328], P('rep', 'dp')
- output 6: float32 [2, 3328, 1024], P('rep', 'dp')
- output 7: float32 [2, 1024, 3328], P('rep', 'dp')
- output 8: float32 [2, 1024, 3328], P('rep', 'dp')
- output 9: float32 [2, 3328, 1024], P('rep', 'dp')
All inputs are finite; a program needn't handle non-finite values.
Results may differ from the reference program's by a relative error of at most 0.022.
Values are sent between devices in bfloat16 or wider.
A program may use at most 768 MiB of HBM per device.

```python
import jax
import jax.numpy as jnp
from jax import lax

SEQUENCES = 256
TOKENS = 1024
D = 1024
FF = 3328
LAYERS = 2
NAMES = ("w_gate", "w_up", "w_down")
SHAPES = {"w_gate": (LAYERS, D, FF), "w_up": (LAYERS, D, FF), "w_down": (LAYERS, FF, D)}


def bump(key, n, height):
    away = (jnp.arange(n, dtype=jnp.int32) - jax.random.randint(key, (), 0, n, jnp.int32)) % n
    return jnp.where(away < n // 8, height, 1.0)


def together(key, own, strength):
    shared = jax.random.normal(key, own.shape[1:], jnp.float32)
    return (own + strength * shared) * lax.rsqrt(1 + strength * strength)


def setup_inputs(seed: int = 0, part: int = 0) -> dict:
    kx, kdy, ka, kb, kz, kf, kh, kl, *keys = jax.random.split(jax.random.key(seed), 8 + 3 * len(NAMES))
    kx, kdy, ka, kb = (jax.random.fold_in(k, part) for k in (kx, kdy, ka, kb))
    kw, km, kv = (keys[i::3] for i in range(3))
    shape = (SEQUENCES, TOKENS, D)
    much_x, much_dy = jax.random.uniform(kz, (2,), jnp.float32, 0.0, 1.0)
    loud = 2.0 ** jax.random.uniform(jax.random.fold_in(kz, 1), (), jnp.float32, -1.0, 2.0)
    layers = 2.0 ** jax.random.uniform(kl, (LAYERS, 1, 1), jnp.float32, -1.0, 1.0)
    x = together(ka, jax.random.normal(kx, shape, jnp.float32), much_x) * bump(kf, D, 4.0)
    dy = together(kb, jax.random.normal(kdy, shape, jnp.float32), much_dy)
    drawn = {"x": x.astype(jnp.bfloat16), "dy": (loud * dy * (SEQUENCES * TOKENS) ** -0.5).astype(jnp.bfloat16)}
    for key, name in zip(kw, NAMES, strict=True):
        w = jax.random.normal(key, SHAPES[name], jnp.float32) * SHAPES[name][1] ** -0.5
        drawn[name] = (w * {"w_gate": 1.0, "w_up": bump(kh, FF, 4.0), "w_down": layers}[name]).astype(jnp.bfloat16)
    for key, name in zip(km, NAMES, strict=True):
        drawn[f"m_{name}"] = 0.1 * jax.random.normal(key, SHAPES[name], jnp.float32)
    for key, name in zip(kv, NAMES, strict=True):
        drawn[f"v_{name}"] = jax.random.uniform(key, SHAPES[name], jnp.float32, 0.005, 0.015)
    return drawn


def matmul(a, w):
    return jnp.dot(a, w, preferred_element_type=jnp.float32).astype(jnp.bfloat16)


def normed(h):
    wide = h.astype(jnp.float32)
    scale = lax.rsqrt(jnp.mean(wide**2, -1, keepdims=True) + 1e-6)
    return (wide * scale).astype(jnp.bfloat16)


def layer(h, w):
    a = normed(h)
    gate = jnp.dot(a, w["w_gate"], preferred_element_type=jnp.float32)
    up = jnp.dot(a, w["w_up"], preferred_element_type=jnp.float32)
    return h + matmul((jax.nn.silu(gate) * up).astype(jnp.bfloat16), w["w_down"])


def adamw(w, m, v, g):
    m = 0.9 * m + 0.1 * g
    v = 0.95 * v + 0.05 * g * g
    step = m * lax.rsqrt(v + 1e-8) + 0.1 * w
    return (w - 0.02 * step).astype(jnp.bfloat16), m, v


def clipped(gradients, sum_of_squares, count):
    factor = jnp.minimum(1.0, 0.5 * lax.rsqrt(sum_of_squares / count + 1e-30))
    return [g * factor for g in gradients]


def stack(weights, h):
    return lax.scan(lambda h, w: (layer(h, w), None), h, weights)[0]


def reference(x, dy, w_gate, w_up, w_down, m_w_gate, m_w_up, m_w_down, v_w_gate, v_w_up, v_w_down):
    weights = dict(zip(NAMES, (w_gate, w_up, w_down), strict=True))

    def take(so_far, sequence):
        h, by_y = sequence
        _, back = jax.vjp(lambda w: stack(w, h), weights)
        return jax.tree.map(lambda total, term: total + term.astype(jnp.float32), so_far, back(by_y)[0]), None

    none_yet = {name: jnp.zeros(w.shape, jnp.float32) for name, w in weights.items()}
    by_weights, _ = lax.scan(take, none_yet, (x, dy))
    gradients = [by_weights[name].astype(jnp.bfloat16).astype(jnp.float32) for name in NAMES]
    gradients = clipped(gradients, sum(jnp.sum(g * g) for g in gradients), sum(g.size for g in gradients))
    new = [
        adamw(w.astype(jnp.float32), m, v, g)
        for w, m, v, g in zip((w_gate, w_up, w_down), (m_w_gate, m_w_up, m_w_down), (v_w_gate, v_w_up, v_w_down), gradients, strict=True)
    ]
    return tuple(one[which] for which in range(3) for one in new)
```

```python
import functools
import heapq
import math

import jax, jax.numpy as jnp
from jax import lax
from jax.experimental import pallas as pl
from jax.experimental.pallas import tpu as pltpu
from jax.sharding import PartitionSpec as P
MESH = pl.DeviceIdType.MESH
BF, F32 = jnp.bfloat16, jnp.float32
SIZE = {"x": 4, "y": 4, "z": 8}


def coords():
    i = lax.axis_index("dp")
    return {"x": i // 64, "y": (i // 16) % 4, "z": (i // 2) % 8, "c": i % 2}


def device(at):
    return {"dp": ((at["x"] * 4 + at["y"]) * 8 + at["z"]) * 2 + at["c"]}


def moved(at, dim, by):
    n = SIZE[dim]
    return {**at, dim: lax.rem(at[dim] + by + n, n)}


UNITS = [
    ("u", 0, 1664, "zxy"), ("g", 0, 896, "xyz"), ("g", 1664, 896, "yxz"), ("d", 0, 256, "xyz"), ("d", 512, 256, "yxz"),
    ("u", 1664, 1664, "zxy"), ("g", 896, 768, "xyz"), ("g", 2560, 768, "yxz"), ("d", 256, 256, "xyz"), ("d", 768, 256, "yxz"),
]
DEPTH = {"u": 4, "g": 8, "d": 26}
WIDTH = {"u": 3328, "g": 3328, "d": 1024}
TALL = {"u": 1, "g": 1, "d": 4}
ROWS = {"u": 4, "g": 4, "d": 16}
COUNT = 2 * 3 * 1024 * 3328
LASTDIM = {"u": "y", "g": "z", "d": "z"}
NB = 3


def sub(a, v):
    return pl.ds(13 * (v // 4) + 3 * lax.rem(v, 4), 4) if a == "d" else pl.ds(v, 1)


def view(a, order, at, level, v):
    al = slice(None)
    if level == 0:
        return {"z": (al, al, v), "x": (v,), "y": (al, v)}[order[0]]
    if level == 1:
        return {"zxy": (v, al, at["z"]), "xyz": (at["x"], v), "yxz": (v, at["y"])}[order]
    return (at["x"], sub(a, v), at["z"]) if a == "u" else (at["x"], at["y"], sub(a, v))


def plan():
    RATE, LAT, DRATE, DLAT = 46.0e3, 2.6, 550.0e3, 1.5
    block = {i: 4 * DEPTH[u[0]] * 8 * u[2] * 2 for i, u in enumerate(UNITS)}
    jobs = []
    for i, u in enumerate(UNITS):
        n = SIZE[u[3][0]]
        h = n // 2
        offs = [h] + [s * (h - k) for k in range(1, h) for s in (1, -1)] + [0]
        jobs += [(i, o) for o in offs]
    rank = {}
    for i, o in jobs:
        nth = sum(k[0] == i for k in rank)
        rank[i, o] = (i // 5) + 0.9 * nth / SIZE[UNITS[i][3][0]]
    jobs.sort(key=rank.get)
    t, arrive = 1.0, {}
    for j in jobs:
        t += block[j[0]] / DRATE
        arrive[j] = t + DLAT
    free = {}
    now = 3.0
    heap = []
    order = []
    def send(t0, link, nbytes):
        s = max(free.get(link, 0.0), t0)
        free[link] = s + nbytes / RATE
        return s + nbytes / RATE + LAT
    ring = {}
    for i, u in enumerate(UNITS):
        ring[0, i] = (u[3][0], block[i])
        ring[1, i] = (u[3][1], block[i] // 4)
    for a in "ugd":
        ring[2, a] = (LASTDIM[a], TALL[a] * 8 * WIDTH[a] * 2)
    done = {}
    seqno = [0]
    def push(t0, ev):
        seqno[0] += 1
        heapq.heappush(heap, (t0, seqno[0], ev))
    for i, u in enumerate(UNITS):
        push(arrive[i, SIZE[u[3][0]] // 2], ("start", 0, i, 0, 0))
    finished = {}
    end = None
    while heap:
        t0, _, ev = heapq.heappop(heap)
        kind, level, key, s, k = ev
        dim, nbytes = ring[level, key]
        n = SIZE[dim]
        h = n // 2
        if level == 0 and kind == "step":
            o = s * (h - k)
            if k < h and arrive[key, o] > t0 + 1e-9:
                push(arrive[key, o], ev)
                continue
        now = max(now, t0)
        order.append(ev)
        cost = 0.1 + nbytes * (4 + 2 * level) / 9.0e6
        if kind == "start":
            now += cost
            for s in (1, -1):
                push(send(now, (dim, s), nbytes // 2), ("step", level, key, s, 1))
        elif k < h:
            now += cost
            push(send(now, (dim, s), nbytes), ("step", level, key, s, k + 1))
        else:
            finished[level, key] = finished.get((level, key), 0) + 1
            if finished[level, key] == 2:
                if level == 0:
                    push(max(now, arrive[key, 0]), ("start", 1, key, 0, 0))
                elif level == 1:
                    a = UNITS[key][0]
                    done[a] = done.get(a, 0) + 1
                    if done[a] == sum(u[0] == a for u in UNITS):
                        push(now, ("start", 2, a, 0, 0))
    return jobs, order, now, free


def addsum(dst, srcs):
    def add(*at):
        acc = srcs[0][at].astype(F32)
        for s in srcs[1:]:
            acc = acc + s[at].astype(F32)
        dst[at] = acc.astype(BF)

    if len(dst.shape) == 4:

        def body(i, _):
            add(i)
            return 0
        lax.fori_loop(0, dst.shape[0], body, 0)
    else:
        add(...)


def block_shape(i, level):
    a, _, cols, _ = UNITS[i]
    return ((4, DEPTH[a], 8, cols), (DEPTH[a], 8, cols))[level]


def rs_scratch():
    sh = {}
    for a, n in (("u", 8), ("g", 8), ("d", 26)):
        sh["loc_" + a] = pltpu.VMEM((4, 4, n, 8, WIDTH[a]), BF)
        sh["stage_" + a] = pltpu.VMEM((NB, 4, DEPTH[a], 8, max(u[2] for u in UNITS if u[0] == a)), BF)
        sh["stsem_" + a] = pltpu.SemaphoreType.DMA((NB,))
        h = SIZE[LASTDIM[a]] // 2
        sh["slot2_" + a] = pltpu.VMEM((2, h, TALL[a], 8, WIDTH[a]), BF)
        sh["r2_" + a] = pltpu.SemaphoreType.DMA((2, h + 1))
        sh["s2_" + a] = pltpu.SemaphoreType.DMA((2, h + 1))
        sh["first_" + a] = pltpu.VMEM((TALL[a], 8, WIDTH[a]), BF)
        sh["red_" + a] = pltpu.VMEM((TALL[a], 8, WIDTH[a]), BF)
    for i, u in enumerate(UNITS):
        h = SIZE[u[3][0]] // 2
        sh["own_%d" % i] = pltpu.VMEM(block_shape(i, 0), BF)
        sh["slot0_%d" % i] = pltpu.VMEM((2, h) + block_shape(i, 0), BF)
        sh["slot1_%d" % i] = pltpu.VMEM((2, 2) + block_shape(i, 1), BF)
        for lv, hh in ((0, h), (1, 2)):
            sh["r%d_%d" % (lv, i)] = pltpu.SemaphoreType.DMA((2, hh + 1))
            sh["s%d_%d" % (lv, i)] = pltpu.SemaphoreType.DMA((2, hh + 1))
    sh["ownsem"] = pltpu.SemaphoreType.DMA((len(UNITS),))
    sh["dr"] = pltpu.SemaphoreType.DMA((48,))
    sh["ds"] = pltpu.SemaphoreType.DMA((48,))
    sh["ar_z"] = pltpu.VMEM((16, 8, 128), F32)
    sh["ar_p"] = pltpu.VMEM((16, 8, 128), F32)
    sh["arsem"] = pltpu.SemaphoreType.DMA((4, 16))
    for a in "ugd":
        sh["mv_" + a] = pltpu.VMEM((2, 2, ROWS[a], WIDTH[a]), F32)
        sh["w_" + a] = pltpu.VMEM((TALL[a], 8, WIDTH[a]), BF)
    sh["new_u"] = pltpu.VMEM((8, 3328), BF)
    sh["new_g"] = pltpu.VMEM((8, 3328), BF)
    sh["new_d"] = pltpu.VMEM((2, 16, 1024), BF)
    sh["mv_r"] = pltpu.SemaphoreType.DMA((3, 2, 2))
    sh["mv_s"] = pltpu.SemaphoreType.DMA((3, 2, 2))
    sh["w_s"] = pltpu.SemaphoreType.DMA((3,))
    sh["fin_r"] = pltpu.SemaphoreType.DMA((3, 2))
    sh["fin_s"] = pltpu.SemaphoreType.DMA((3, 5))
    return sh


def rs_kernel(names, *refs):
    g = {(a, l): refs[2 * j + l] for j, a in enumerate("ugd") for l in (0, 1)}
    weights = {a: refs[6 + j] for j, a in enumerate("ugd")}
    moments = {a: (refs[9 + j], refs[12 + j]) for j, a in enumerate("ugd")}
    new = {a: refs[15 + j] for j, a in enumerate("ugd")}
    new_moments = {a: (refs[18 + j], refs[21 + j]) for j, a in enumerate("ugd")}
    S = dict(zip(names, refs[24:], strict=True))
    at = coords()
    c = at["c"]
    sib = device({**at, "c": 1 - c})
    jobs, order, _, _ = plan()

    peers = [device({**at, "z": lax.rem(at["z"] + dz, 8), "c": lax.rem(c + dc, 2)}) for dz in range(8) for dc in range(2)][1:]
    peers += [device({**at, "x": lax.rem(at["x"] + dx, 4), "y": lax.rem(at["y"] + dy, 4)}) for dx in range(4) for dy in range(4)][1:]
    bar = pltpu.get_barrier_semaphore()
    for p in peers:
        pl.semaphore_signal(bar, inc=1, device_id=p, device_id_type=MESH)
    pl.semaphore_wait(bar, len(peers))

    pend = []

    def remote(src, dst, ss, rs, to):
        cp = pltpu.make_async_remote_copy(src_ref=src, dst_ref=dst, send_sem=ss, recv_sem=rs, device_id=to, device_id_type=MESH)
        cp.start()
        pend.append(cp)
        return cp

    def cols(i):
        return pl.ds(UNITS[i][1], UNITS[i][2])

    def region(ref, i, level, v):
        a, _, _, o = UNITS[i]
        idx = view(a, o, at, level, v)
        return ref.at[(*idx, *([slice(None)] * (4 - len(idx))), cols(i))]

    def pos(i, level, off):
        dim = UNITS[i][3][level] if level < 2 else LASTDIM[UNITS[i][0]]
        return lax.rem(at[dim] + off + SIZE[dim], SIZE[dim])

    moment_copies = []
    for j, a in enumerate("ugd"):
        for q in (0, 1):
            ref = moments[a][q]
            moment_copies.append(remote(ref.at[1 - c], S["mv_" + a].at[q, c], S["mv_s"].at[j, q, 0], S["mv_r"].at[j, q, 0], sib))
            cp = pltpu.make_async_copy(ref.at[c], S["mv_" + a].at[q, c], S["mv_r"].at[j, q, 1])
            cp.start()
            moment_copies.append(cp)
        w = weights[a]
        ref = w.at[c, at["x"], at["y"], sub("d", at["z"])] if a == "d" else w.at[c, at["x"], at["y"], pl.ds(at["z"], 1)]
        cp = pltpu.make_async_copy(ref, S["w_" + a], S["w_s"].at[j])
        cp.start()
        moment_copies.append(cp)

    dcopy = {}
    for j, (i, off) in enumerate(jobs):
        a = UNITS[i][0]
        dst = region(S["loc_" + a], i, 0, pos(i, 0, off))
        for cc in (0, 1):
            src = region(g[a, 1 - cc], i, 0, pos(i, 0, off))
            cp = pltpu.make_async_remote_copy(src_ref=src, dst_ref=dst, send_sem=S["ds"].at[j], recv_sem=S["dr"].at[j], device_id=sib, device_id_type=MESH)
            pl.when(c == cc)(cp.start)
        pend.append(cp)
        dcopy[i, off] = cp

    uses = {a: [] for a in "ugd"}
    for kind, level, key, s, k in order:
        if level == 0:
            h = SIZE[UNITS[key][3][0]] // 2
            if kind == "start":
                uses[UNITS[key][0]].append((key, h))
            elif k < h:
                uses[UNITS[key][0]].append((key, s * (h - k)))
    nth = {a: 0 for a in "ugd"}

    def fetch(a, n, start):
        if n >= len(uses[a]):
            return None
        i, off = uses[a][n]
        buf = S["stage_" + a].at[n % NB, :, :, :, pl.ds(0, UNITS[i][2])]
        for cc in (0, 1):
            cp = pltpu.make_async_copy(region(g[a, cc], i, 0, pos(i, 0, off)), buf, S["stsem_" + a].at[n % NB])
            if start:
                pl.when(c == cc)(cp.start)
        if not start:
            cp.wait()
        return buf
    for n in range(NB):
        for a in "ugd":
            fetch(a, n, True)

    def fetch_own(i, start):
        a = UNITS[i][0]
        for cc in (0, 1):
            cp = pltpu.make_async_copy(region(g[a, cc], i, 0, pos(i, 0, 0)), S["own_%d" % i], S["ownsem"].at[i])
            if start:
                pl.when(c == cc)(cp.start)
        if not start:
            cp.wait()

    waited = set()

    def sibling_block(i, off):
        if (i, off) not in waited:
            waited.add((i, off))
            dcopy[i, off].wait_recv()

    def operands(level, i, off):
        a, _, _, o = UNITS[i]
        v = pos(i, level, off)
        l = region(S["loc_" + a], i, level, v)
        if level == 0:
            sibling_block(i, off)
            buf = fetch(a, nth[a], False)
            assert uses[a][nth[a]] == (i, off)
            nth[a] += 1
            return [buf, l]
        h = SIZE[o[0]] // 2
        first = [S["own_%d" % i]] + [S["slot0_%d" % i].at[d, h - 1] for d in (0, 1)]
        if level == 1:
            return [l] + [f.at[v] for f in first]
        w = pos(i, 1, 0)
        return [l] + [f.at[w, sub(a, v)] for f in first] + [S["slot1_%d" % i].at[d, 1, sub(a, v)] for d in (0, 1)]

    def half(ref, which, level, a):
        if level == 2 and TALL[a] == 1:
            n = ref.shape[-1] // 2
            return ref.at[..., pl.ds(n * which, n)]
        n = ref.shape[0] // 2
        return ref.at[pl.ds(n * which, n)]

    def parts(level, key):
        if level < 2:
            return [(key, None)]
        return [(i, cols(i)) for i, u in enumerate(UNITS) if u[0] == key]

    def cut(ref, cs):
        return ref if cs is None else ref.at[..., cs]

    for kind, level, key, s, k in order:
        a = UNITS[key][0] if level < 2 else key
        dim = UNITS[key][3][level] if level < 2 else LASTDIM[a]
        h = SIZE[dim] // 2
        slot, rsem, ssem = (S["%s%d_%s" % (n, level, key)] for n in ("slot", "r", "s"))
        d = 0 if s > 0 else 1

        def send(src, dst, d, k, dim=dim, rsem=rsem, ssem=ssem):
            remote(src, dst, ssem.at[d, k], rsem.at[d, k], device(moved(at, dim, 1 - 2 * d)))

        if kind == "start":
            if level == 0:
                fetch_own(key, True)
            if level == 1:
                sibling_block(key, 0)
                fetch_own(key, False)
            if level == 2:
                dst = S["first_" + a]
            else:
                dst = region(S["loc_" + a], key, level, pos(key, level, h))
            for i, cs in parts(level, key):
                addsum(cut(dst, cs), operands(level, i, h))
            for d in (0, 1):
                send(half(dst, d, level, a), half(slot.at[d, 0], d, level, a), d, 0)
            if level == 0:
                fetch(a, nth[a] - 1 + NB, True)
            continue
        block = slot.at[d, k - 1]
        got = half(block, d, level, a) if k == 1 else block
        pltpu.make_async_remote_copy(src_ref=got, dst_ref=got, send_sem=ssem.at[d, k - 1], recv_sem=rsem.at[d, k - 1], device_id=sib, device_id_type=MESH).wait_recv()
        if k == h:
            continue
        off = s * (h - k)
        for i, cs in parts(level, key):
            ops = operands(level, i, off)
            mine = cut(block, cs)
            if k > 1:
                addsum(mine, [mine] + ops)
            elif level == 2 and TALL[a] == 1:
                inside = (UNITS[i][1] >= WIDTH[a] // 2) == (d == 1)
                addsum(mine, ([mine] if inside else []) + ops)
            else:
                for w in (0, 1):
                    hops = [half(r, w, level, a) for r in ops]
                    hm = half(mine, w, level, a)
                    addsum(hm, ([hm] if w == d else []) + hops)
        send(block, slot.at[d, k], d, k)
        if level == 0:
            fetch(a, nth[a] - 1 + NB, True)

    total = jnp.zeros((8, 128), F32)
    zz = lax.rem(at["z"], 4)
    for j, a in enumerate("ugd"):
        h = SIZE[LASTDIM[a]] // 2
        for i, cs in parts(2, a):
            ops = operands(2, i, 0) + [S["slot2_" + a].at[d, h - 1, :, :, cs] for d in (0, 1)]
            for t in range(TALL[a]):
                for q in range(UNITS[i][2] // 128):
                    acc = ops[0][t, :, q * 128:q * 128 + 128].astype(F32)
                    for o in ops[1:]:
                        acc = acc + o[t, :, q * 128:q * 128 + 128].astype(F32)
                    acc = acc.astype(BF)
                    S["red_" + a][t, :, pl.ds(UNITS[i][1] + q * 128, 128)] = acc
                    acc = acc.astype(F32)
                    if a == "d":
                        row = lax.broadcasted_iota(jnp.int32, (8, 128), 0) + 8 * t
                        acc = jnp.where((row >= 2 * zz) & (row < 2 * zz + 26), acc, 0.0)
                    total = total + acc * acc
    for r, (buf, ds) in enumerate(((S["ar_z"], [(0, 0, q // 2, q % 2) for q in range(16)]), (S["ar_p"], [(q // 4, q % 4, 0, 0) for q in range(16)]))):
        buf[0] = total
        cps = []
        for q in range(1, 16):
            dx, dy, dz, dc = ds[q]
            to = device({"x": lax.rem(at["x"] + dx, 4), "y": lax.rem(at["y"] + dy, 4), "z": lax.rem(at["z"] + dz, 8), "c": lax.rem(c + dc, 2)})
            cps.append(remote(buf.at[0], buf.at[q], S["arsem"].at[2 * r, q], S["arsem"].at[2 * r + 1, q], to))
        for cp in cps:
            cp.wait_recv()
        total = buf[0]
        for q in range(1, 16):
            total = total + buf[q]
    mean = jnp.sum(jnp.sum(total, axis=1, keepdims=True), axis=0, keepdims=True) / COUNT
    factor = jnp.minimum(1.0, 0.5 * lax.rsqrt(mean + 1e-30))
    for cp in moment_copies:
        cp.wait_recv() if cp.is_remote else cp.wait()

    def adamw(w, m, v, g):
        g = g * factor
        m = 0.9 * m + 0.1 * g
        v = 0.95 * v + 0.05 * g * g
        step = m * lax.rsqrt(v + 1e-8) + 0.1 * w
        return (w - 0.02 * step).astype(BF), m, v

    for a in "ug":
        mv, red, wv = S["mv_" + a], S["red_" + a], S["w_" + a]

        def body(q, _, mv=mv, red=red, wv=wv, a=a):
            cs = pl.ds(pl.multiple_of(q * 256, 256), 256)
            m, v = (jnp.concatenate([mv[e, 0, :, cs], mv[e, 1, :, cs]], axis=0) for e in (0, 1))
            n, m, v = adamw(wv[0, :, cs].astype(F32), m, v, red[0, :, cs].astype(F32))
            S["new_" + a][:, cs] = n
            for e, t in enumerate((m, v)):
                for s in (0, 1):
                    mv[e, s, :, cs] = t[4 * s:4 * s + 4]
            return 0
        lax.fori_loop(0, 3328 // 256, body, 0)
    row = lax.broadcasted_iota(jnp.int32, (32, 32), 0)
    column = lax.broadcasted_iota(jnp.int32, (32, 32), 1)
    pick = (column == 2 * zz + 13 * (row >> 4) + (row & 15)) & ((row & 15) < 13)
    pick = jnp.where(pick, 1.0, 0.0).astype(BF)
    gd, wd = (jnp.dot(pick, S[n][...].reshape(32, 1024), preferred_element_type=F32) for n in ("red_d", "w_d"))
    for s in (0, 1):
        rows = slice(16 * s, 16 * s + 16)
        n, m, v = adamw(wd[rows], S["mv_d"][0, s], S["mv_d"][1, s], gd[rows])
        S["new_d"][s] = n
        S["mv_d"][0, s] = m
        S["mv_d"][1, s] = v
    ends = []
    for j, a in enumerate("ugd"):
        cp = pltpu.make_async_copy(S["new_" + a], new[a], S["fin_s"].at[j, 4])
        cp.start()
        pend.append(cp)
        for q in (0, 1):
            ends.append(remote(S["mv_" + a].at[q, 1 - c], new_moments[a][q].at[c], S["fin_s"].at[j, q], S["fin_r"].at[j, q], sib))
            cp = pltpu.make_async_copy(S["mv_" + a].at[q, c], new_moments[a][q].at[c], S["fin_s"].at[j, 2 + q])
            cp.start()
            pend.append(cp)
    for cp in ends:
        cp.wait_recv()
    for cp in pend:
        cp.wait_send() if cp.is_remote else cp.wait()


def reduce_scatter(u, g, d, weights, m, v):
    args = [t.reshape(4, 4, 8, 8, 3328) for t in (*u, *g)] + [t.reshape(4, 4, 26, 8, 1024) for t in d]
    args += [w.reshape(2, 4, 4, -1, 8, w.shape[-1]) for w in weights]
    args += [*m, *v]
    sh = rs_scratch()
    any_ = pl.BlockSpec(memory_space=pl.ANY)
    outs = [jax.ShapeDtypeStruct(s, BF) for s in ((8, 3328), (8, 3328), (2, 16, 1024))] + [jax.ShapeDtypeStruct(t.shape, F32) for t in (*m, *v)]
    outs = pl.pallas_call(
        functools.partial(rs_kernel, list(sh)), out_shape=outs, in_specs=[any_] * 15, out_specs=[any_] * 9, scratch_shapes=list(sh.values()), name="reduce_scatter",
        compiler_params=pltpu.CompilerParams(collective_id=0, has_side_effects=True, vmem_limit_bytes=67043328))(*args)
    return outs[:3], outs[3:6], outs[6:]


def plan_ag():
    RATE, LAT = 46.0e3, 2.9
    free, heap, order, n_ = {}, [], [], [0]

    def push(t0, ev):
        n_[0] += 1
        heapq.heappush(heap, (t0, n_[0], ev))

    def send(t0, link, nbytes):
        s = max(free.get(link, 0.0), t0)
        free[link] = s + nbytes / RATE
        return free[link] + LAT
    ring = {(2, a): (LASTDIM[a], {"u": 8 * 3328, "g": 8 * 3328, "d": 32 * 1024}[a] * 2) for a in "ugd"}
    for i, (a, _, cols, o) in enumerate(UNITS):
        ring[1, i] = (o[1], DEPTH[a] * 8 * cols * 2)
        ring[0, i] = (o[0], 4 * DEPTH[a] * 8 * cols * 2)
    got = {}
    for a in "gdu":
        push(1.0, ("start", 2, a, 0, 0))
    now = 1.0
    while heap:
        t0, _, ev = heapq.heappop(heap)
        kind, level, key, s, k = ev
        dim, nbytes = ring[level, key]
        h = SIZE[dim] // 2
        now = max(now, t0) + 0.1
        order.append(ev)
        if kind == "start":
            for s in (1, -1):
                push(send(now, (dim, s), nbytes), ("step", level, key, s, 1))
            continue
        if k < h:
            push(send(now, (dim, s), nbytes if k < h - 1 else nbytes // 2), ("step", level, key, s, k + 1))
            continue
        got[level, key] = got.get((level, key), 0) + 1
        if got[level, key] < 2:
            continue
        if level == 2:
            for i, u in enumerate(UNITS):
                if u[0] == key:
                    push(now + (1.0 if key == "d" else 0), ("start", 1, i, 0, 0))
        elif level == 1:
            push(now, ("start", 0, key, 0, 0))
    return order, now, free


def ag_scratch():
    sh = {"pc": pltpu.VMEM((8, 2, 16, 1024), BF), "asm": pltpu.VMEM((26, 8, 1024), BF), "loc": pltpu.SemaphoreType.DMA((4,)),
          "sr": pltpu.SemaphoreType.DMA((128,)), "ss": pltpu.SemaphoreType.DMA((128,))}
    for a in "ugd":
        h = SIZE[LASTDIM[a]] // 2
        for n in "rs":
            sh["%s2_%s" % (n, a)] = pltpu.SemaphoreType.DMA((2, h))
    for i, u in enumerate(UNITS):
        for lv in (0, 1):
            for n in "rs":
                sh["%s%d_%d" % (n, lv, i)] = pltpu.SemaphoreType.DMA((2, SIZE[u[3][lv]] // 2))
    return sh


def ag_kernel(names, *refs):
    own = {a: refs[j] for j, a in enumerate("ugd")}
    outs = {a: refs[3 + j] for j, a in enumerate("ugd")}
    S = dict(zip(names, refs[6:], strict=True))
    at = coords()
    c = at["c"]
    sib = device({**at, "c": 1 - c})
    out = {a: r.at[c] for a, r in outs.items()}
    order, _, _ = plan_ag()
    peers = [sib] + [device(moved(at, d, s)) for d in "xyz" for s in (1, -1)]
    bar = pltpu.get_barrier_semaphore()
    for p in peers:
        pl.semaphore_signal(bar, inc=1, device_id=p, device_id_type=MESH)
    x, y, z = at["x"], at["y"], at["z"]
    locals_ = [pltpu.make_async_copy(own["u"], out["u"].at[x, y, z], S["loc"].at[0]), pltpu.make_async_copy(own["g"], out["g"].at[x, y, z], S["loc"].at[1]),
               pltpu.make_async_copy(own["d"], S["pc"].at[z], S["loc"].at[2])]
    for cp in locals_:
        cp.start()
    pl.semaphore_wait(bar, len(peers))
    for cp in locals_:
        cp.wait()
    pend, twin = [], []

    def remote(src, dst, ss, rs, to):
        cp = pltpu.make_async_remote_copy(src_ref=src, dst_ref=dst, send_sem=ss, recv_sem=rs, device_id=to, device_id_type=MESH)
        cp.start()
        pend.append(cp)

    def to_sibling(ref):
        n = len(twin)
        remote(ref, ref, S["ss"].at[n], S["sr"].at[n], sib)
        twin.append(ref)

    def region(level, key, v):
        if level == 2:
            return {"u": lambda: out["u"].at[x, v, z], "g": lambda: out["g"].at[x, y, v], "d": lambda: S["pc"].at[v]}[key]()
        a, col, n, o = UNITS[key]
        idx = view(a, o, at, level, v)
        return out[a].at[(*idx, *([slice(None)] * (4 - len(idx))), pl.ds(col, n))]

    def half(ref, which, level, key):
        if level == 2 and key != "d":
            return ref.at[:, pl.ds(1664 * which, 1664)]
        n = ref.shape[0] // 2
        return ref.at[pl.ds(n * which, n)]

    got = {}
    for kind, level, key, s, k in order:
        dim = UNITS[key][3][level] if level < 2 else LASTDIM[key]
        n = SIZE[dim]
        h = n // 2
        rsem, ssem = S["r%d_%s" % (level, key)], S["s%d_%s" % (level, key)]

        def send(src, d, k, dim=dim, rsem=rsem, ssem=ssem):
            remote(src, src, ssem.at[d, k], rsem.at[d, k], device(moved(at, dim, 1 - 2 * d)))

        if kind == "start":
            for d in (0, 1):
                send(region(level, key, at[dim]), d, 0)
            continue
        d = 0 if s > 0 else 1
        block = region(level, key, lax.rem(at[dim] - s * k + n, n))
        if k == h:
            block = half(block, d, level, key)
        pltpu.make_async_remote_copy(src_ref=block, dst_ref=block, send_sem=ssem.at[d, k - 1], recv_sem=rsem.at[d, k - 1], device_id=sib, device_id_type=MESH).wait_recv()
        if k < h - 1:
            send(block, d, k)
        elif k == h - 1:
            send(half(block, d, level, key), d, k)
        if level < 2:
            to_sibling(block)
        if k == h:
            got[level, key] = got.get((level, key), 0) + 1
            if level == 2 and got[level, key] == 2:
                if key == "d":
                    q = lax.broadcasted_iota(jnp.int32, (208, 256), 1)
                    r = lax.broadcasted_iota(jnp.int32, (208, 256), 0)
                    e = q & 15
                    pick = (r == 26 * (q >> 5) + 13 * ((q >> 4) & 1) + e) & (e < 13)
                    got_rows = jnp.dot(jnp.where(pick, 1.0, 0.0).astype(BF), S["pc"][...].reshape(256, 1024), preferred_element_type=F32)
                    S["asm"][...] = got_rows.reshape(26, 8, 1024).astype(BF)
                    cp = pltpu.make_async_copy(S["asm"], out["d"].at[x, y], S["loc"].at[3])
                    cp.start()
                    cp.wait()
                to_sibling({"u": lambda: out["u"].at[x, :, z], "g": lambda: out["g"].at[x, y], "d": lambda: out["d"].at[x, y]}[key]())
    for n, ref in enumerate(twin):
        other = ref
        pltpu.make_async_remote_copy(src_ref=other, dst_ref=other, send_sem=S["ss"].at[n], recv_sem=S["sr"].at[n], device_id=sib, device_id_type=MESH).wait_recv()
    for cp in pend:
        cp.wait_send()


def all_gather(u, g, d):
    sh = ag_scratch()
    any_ = pl.BlockSpec(memory_space=pl.ANY)
    outs = [jax.ShapeDtypeStruct((2, 4, 4, n, 8, w), BF) for n, w in ((8, 3328), (8, 3328), (26, 1024))]
    return pl.pallas_call(
        functools.partial(ag_kernel, list(sh)), out_shape=outs, in_specs=[any_] * 3, out_specs=[any_] * 3, scratch_shapes=list(sh.values()), name="all_gather",
        compiler_params=pltpu.CompilerParams(collective_id=1, has_side_effects=True, vmem_limit_bytes=67043328))(u, g, d)


NAMES = ("w_gate", "w_up", "w_down")


def matmul(a, w):
    return jnp.dot(a, w, preferred_element_type=F32).astype(BF)


def normed(h):
    wide = h.astype(F32)
    scale = lax.rsqrt(jnp.mean(wide**2, -1, keepdims=True) + 1e-6)
    return (wide * scale).astype(BF)


def layer(h, w):
    a = normed(h)
    gate = jnp.dot(a, w["w_gate"], preferred_element_type=F32)
    up = jnp.dot(a, w["w_up"], preferred_element_type=F32)
    return h + matmul((jax.nn.silu(gate) * up).astype(BF), w["w_down"])


def solution(mesh):
    def step(x, dy, w_gate, w_up, w_down, *moments):
        weights = [{n: w[i] for n, w in zip(NAMES, (w_gate, w_up, w_down), strict=True)} for i in (0, 1)]

        def stack(weights):
            h = x[0]
            for w in weights:
                h = layer(h, w)
            return h

        _, back = jax.vjp(stack, weights)
        grads = back(dy[0])[0]
        gate, up, down = ([grads[i][n] for i in (0, 1)] for n in NAMES)
        m, v = moments[:3], moments[3:]
        order = lambda t: (t[1], t[0], t[2])
        pad = lambda t: (*t[:2], jnp.pad(t[2], ((0, 0), (0, 3), (0, 0))))
        new, m, v = reduce_scatter(up, gate, down, order((w_gate, w_up, w_down)), pad(order(m)), pad(order(v)))
        u, g, d = all_gather(*new)
        w = (g.reshape(w_gate.shape), u.reshape(w_up.shape), d.reshape(w_down.shape))
        cut = lambda t: (t[1], t[0], t[2][:, :13])
        return (*w, *cut(m), *cut(v))

    data, whole, rows = P(("rep", "dp"), None, None), P(), P(None, "dp", None)
    out = P("rep", None, None)
    return jax.shard_map(step, mesh=mesh, in_specs=(data, data) + (whole,) * 3 + (rows,) * 6, out_specs=(out,) * 3 + (P("rep", "dp", None),) * 6, check_vma=False)
```

```python
import functools
import heapq

import jax
import jax.numpy as jnp
from jax import lax
from jax.experimental import pallas as pl
from jax.experimental.pallas import tpu as pltpu
from jax.sharding import PartitionSpec as P

MESH = pl.DeviceIdType.MESH
BF, F32 = jnp.bfloat16, jnp.float32
SIZE = {"x": 4, "y": 4, "z": 8}
VMEM_BYTES = 67043328
ALL = slice(None)


def coords():
    i = lax.axis_index("dp")
    return {"x": i // 64, "y": lax.rem(i // 16, 4), "z": lax.rem(i // 2, 8), "c": lax.rem(i, 2)}


def device(at):
    return {"dp": ((at["x"] * 4 + at["y"]) * 8 + at["z"]) * 2 + at["c"]}


def places(at):
    spots = {d: [at[d]] + [lax.rem(at[d] + k, n) for k in range(1, n)] for d, n in SIZE.items()}
    return spots, {(d, s): device({**at, d: spots[d][s]}) for d in SIZE for s in (1, -1)}


UNITS = [
    (1, "d", 0, 256, "xyz"), (1, "d", 256, 256, "yxz"), (1, "u", 0, 896, "zxy"), (1, "u", 896, 768, "zxy"), (1, "g", 0, 896, "xyz"), (1, "g", 896, 768, "yxz"),
    (0, "d", 0, 256, "xyz"), (0, "d", 256, 256, "yxz"), (0, "u", 0, 896, "zxy"), (0, "u", 896, 768, "zxy"), (0, "g", 0, 896, "yxz"), (0, "g", 896, 768, "xyz"),
]
DEPTH = {"u": 4, "g": 8, "d": 26}
TILES = {"u": 8, "g": 8, "d": 26}
WIDTH = {"u": 1664, "g": 1664, "d": 512}
TALL = {"u": 1, "g": 1, "d": 4}
LASTDIM = {"u": "y", "g": "z", "d": "z"}
ROWS = {"u": 4, "g": 4, "d": 16}
COUNT = 2 * 3 * 1024 * 3328
NB = 2


def view(a, order, at, level, v):
    if level == 0:
        return {"z": (ALL, ALL, v), "x": (v,), "y": (ALL, v)}[order[0]]
    if level == 1:
        return {"zxy": (v, ALL, at["z"]), "xyz": (at["x"], v), "yxz": (v, at["y"])}[order]
    return (at["x"], v, at["z"]) if a == "u" else (at["x"], at["y"], v)


def block_shape(i, level):
    _, a, _, cols, _ = UNITS[i]
    return ((4, DEPTH[a], 8, cols), (DEPTH[a], 8, cols))[level]


def remote_copy(src, dst, ss, rs, to):
    return pltpu.make_async_remote_copy(src_ref=src, dst_ref=dst, send_sem=ss, recv_sem=rs, device_id=to, device_id_type=MESH)


GROUPS = [(1, "d"), (1, "u"), (1, "g"), (0, "u"), (0, "d"), (0, "g")]
OFFSETS = (2, 1, 3, 0)


def plan():
    RATE, LAT, TASK, DRATE, DLAT = 46.0e3, 2.6, 1.15, 550.0e3, 1.7
    free, heap, seq = {}, [], [0]

    def send(t, link, nbytes):
        free[link] = max(free.get(link, 0.0), t) + nbytes / RATE
        return free[link] + LAT

    def push(t, ev):
        seq[0] += 1
        heapq.heappush(heap, (t, seq[0], ev))
    ring = {}
    for i, (l, a, _, cols, o) in enumerate(UNITS):
        ring[0, i] = (o[0], 4 * DEPTH[a] * 8 * cols * 2)
        ring[1, i] = (o[1], DEPTH[a] * 8 * cols * 2)
        ring[2, (l, a)] = (LASTDIM[a], TALL[a] * 8 * WIDTH[a] * 2)
    have = {}
    got, steps, now = {}, [], 4.0

    def ready(i, off):
        l, a, _, _, o = UNITS[i]
        need = [(l, a, off % 4)] if o[0] == "x" else [(l, a, b) for b in range(4)]
        return max(have[n] for n in need) if all(n in have for n in need) else None

    def run(until):
        nonlocal now
        taken = []
        while heap and heap[0][0] <= until:
            t, _, ev = heapq.heappop(heap)
            kind, level, key, s, k = ev
            dim, nbytes = ring[level, key]
            h = SIZE[dim] // 2
            if level == 0 and kind == "step" and k < h:
                when = ready(key, s * (h - k))
                if when is None or when > t:
                    push(t + 0.5 if when is None else when, ev)
                    continue
            now = max(now, t)
            taken.append(ev)
            cost = 0.15 + nbytes * (4 + 2 * level) / 7.0e6
            if kind == "end":
                continue
            if kind == "start":
                now += cost
                for s in (1, -1):
                    push(send(now, (dim, s), nbytes // 2), ("step", level, key, s, 1))
            elif k < h:
                now += cost
                push(send(now, (dim, s), nbytes), ("step", level, key, s, k + 1))
            else:
                got[level, key] = got.get((level, key), 0) + 1
                if got[level, key] < 2:
                    continue
                if level == 0:
                    push(now, ("start", 1, key, 0, 0))
                elif level == 1:
                    ka = UNITS[key][:2]
                    if all(got.get((1, i)) == 2 for i, u in enumerate(UNITS) if u[:2] == ka):
                        push(now, ("start", 2, ka, 0, 0))
                else:
                    push(now, ("end", 2, key, 0, 0))
        return taken
    dfree = 0.0
    for l, a in GROUPS:
        own = {}
        steps.append(((l, a), run(now)))
        for s in range(8):
            now += TASK
            block, half = (s // 2, s % 2) if a == "d" else (s % 4, s // 4)
            off = OFFSETS[block]
            if half == 0:
                dfree = max(dfree, now) + 4 * TILES[a] * 8 * WIDTH[a] * 2 / DRATE
                own[off] = dfree + DLAT
            else:
                have[l, a, off] = max(now + 2.0, own[off])
            if a == "d" and half == 1 and block == 0:
                push(have[l, a, off], ("start", 0, next(i for i, u in enumerate(UNITS) if u[:2] == (l, a) and u[4][0] == "x"), 0, 0))
        for i, u in enumerate(UNITS):
            if u[:2] == (l, a) and not (a == "d" and u[4][0] == "x"):
                push(ready(i, SIZE[u[4][0]] // 2), ("start", 0, i, 0, 0))
    steps.append((None, run(float("inf"))))
    return steps, now, free


def addsum(dst, srcs):
    def add(*at):
        acc = srcs[0][at].astype(F32)
        for s in srcs[1:]:
            acc = acc + s[at].astype(F32)
        dst[at] = acc.astype(BF)

    if len(dst.shape) == 4:

        def body(i, _):
            add(i)
            return 0
        lax.fori_loop(0, dst.shape[0], body, 0)
    else:
        add(...)


def rs_scratch():
    sh = {}
    sem = pltpu.SemaphoreType.DMA
    for a in "ugd":
        sh["loc_" + a] = pltpu.VMEM((2, 4, 4, TILES[a], 8, WIDTH[a]), BF)
        sh["stage_" + a] = pltpu.VMEM((NB, 4, DEPTH[a], 8, max(u[3] for u in UNITS if u[1] == a)), BF)
        sh["stsem_" + a] = sem((NB,))
        sh["red_" + a] = pltpu.VMEM((2, TALL[a], 8, WIDTH[a]), BF)
        sh["mv_" + a] = pltpu.VMEM((2, 2, 2, ROWS[a], WIDTH[a]), F32)
        sh["w_" + a] = pltpu.VMEM((2, TALL[a], 8, WIDTH[a]), BF)
        h = SIZE[LASTDIM[a]] // 2
        for l in (0, 1):
            sh["slot2_%d%s" % (l, a)] = pltpu.VMEM((2, h, TALL[a], 8, WIDTH[a]), BF)
            sh["first_%d%s" % (l, a)] = pltpu.VMEM((TALL[a], 8, WIDTH[a]), BF)
            for n in "rs":
                sh["%s2_%d%s" % (n, l, a)] = sem((2, h))
    sh["new_d"] = pltpu.VMEM((2, 2, 16, 512), BF)
    for i, u in enumerate(UNITS):
        h = SIZE[u[4][0]] // 2
        if not u[0]:
            sh["own_%d" % i] = pltpu.VMEM(block_shape(i, 0), BF)
        sh["slot0_%d" % i] = pltpu.VMEM((2, h) + block_shape(i, 0), BF)
        sh["slot1_%d" % i] = pltpu.VMEM((2, 2) + block_shape(i, 1), BF)
        for n in "rs":
            sh["%s0_%d" % (n, i)] = sem((2, h))
            sh["%s1_%d" % (n, i)] = sem((2, 2))
    sh["ownsem"] = sem((len(UNITS),))
    sh["left"] = pltpu.VMEM((1024, 1024), BF)
    sh["leftsem"] = sem((1,))
    sh["right"] = pltpu.VMEM((2, 1024, 1664), BF)
    sh["rightsem"] = sem((2,))
    sh["res_u"] = pltpu.VMEM((2, 4, 8, 8, 1664), BF)
    sh["res_d"] = pltpu.VMEM((2, 4, 26, 8, 512), BF)
    sh["dr"] = sem((6, 4))
    sh["ds"] = sem((6, 4))
    sh["os"] = sem((6, 4))
    sh["ar_z"] = pltpu.VMEM((16, 1, 128), F32)
    sh["ar_p"] = pltpu.VMEM((16, 1, 128), F32)
    sh["arsem"] = sem((4, 16))
    sh["mvsem"] = sem((3, 2, 3))
    sh["wsem"] = sem((3,))
    sh["finsem"] = sem((3, 2, 3))
    sh["newsem"] = sem((3,))
    return sh


def rs_kernel(names, *refs):
    act = {(n, l): refs[2 * j + l] for j, n in enumerate(("a", "h", "u", "g", "y")) for l in (0, 1)}
    weights = {a: refs[10 + j] for j, a in enumerate("ugd")}
    moments = {a: (refs[13 + j], refs[16 + j]) for j, a in enumerate("ugd")}
    new = {a: refs[19 + j] for j, a in enumerate("ugd")}
    new_moments = {a: (refs[22 + j], refs[25 + j]) for j, a in enumerate("ugd")}
    mine = {a: refs[28 + j] for j, a in enumerate("ugd")}
    S = dict(zip(names, refs[31:], strict=True))
    at = coords()
    c, x = at["c"], at["x"]
    sib = device({**at, "c": 1 - c})
    steps, _, _ = plan()
    spots, near = places(at)
    windows = [pl.ds(13 * lax.div(v, 4) + 3 * lax.rem(v, 4), 4) for v in spots["z"]]
    zz = lax.rem(at["z"], 4)

    peers = [device({**at, "z": lax.rem(at["z"] + dz, 8), "c": lax.rem(c + dc, 2)}) for dz in range(8) for dc in range(2)][1:]
    peers += [device({**at, "x": lax.rem(at["x"] + dx, 4), "y": lax.rem(at["y"] + dy, 4)}) for dx in range(4) for dy in range(4)][1:]
    bar = pltpu.get_barrier_semaphore()
    for p in peers:
        pl.semaphore_signal(bar, inc=1, device_id=p, device_id_type=MESH)

    def halfcols(a, which):
        w = WIDTH[a]
        return pl.ds(pl.multiple_of((c if which else 1 - c) * w, 128), w)

    def left(l, a):
        return pltpu.make_async_copy(act["y" if a == "d" else "a", l], S["left"], S["leftsem"].at[0])
    loads = []
    for l, a in GROUPS:
        loads += [(l, a, n) for n in range(4 if a == "d" else 2)]

    def right(n):
        l, a, k = loads[n]
        if a == "d":
            b = spots["x"][OFFSETS[k]]
            src = act["h", l].at[pl.ds(pl.multiple_of(832 * b, 832), 832)]
            dst = S["right"].at[n % 2, pl.ds(0, 832), pl.ds(0, 1024)]
        else:
            src = act[a, l].at[:, halfcols(a, k)]
            dst = S["right"].at[n % 2]
        return pltpu.make_async_copy(src, dst, S["rightsem"].at[n % 2])
    left(*GROUPS[0]).start()
    right(0).start()
    right(1).start()

    moment_copies = []
    for j, a in enumerate("ugd"):
        for q in (0, 1):
            ref = moments[a][q]
            moment_copies.append(pltpu.make_async_copy(ref.at[:, :, halfcols(a, 1)], S["mv_" + a].at[q, c], S["mvsem"].at[j, q, 2]))
        tile = windows[0] if a == "d" else pl.ds(at["z"], 1)
        moment_copies.append(pltpu.make_async_copy(weights[a].at[:, at["x"], at["y"], tile, :, halfcols(a, 1)], S["w_" + a], S["wsem"].at[j]))
    for cp in moment_copies:
        cp.start()
    pl.semaphore_wait(bar, len(peers))
    pend = []

    def remote(make):
        cp = make()
        cp.start()
        pend.append(make)
        return cp
    for j, a in enumerate("ugd"):
        for q in (0, 1):
            moment_copies.append(remote(lambda j=j, a=a, q=q: remote_copy(
                moments[a][q].at[:, :, halfcols(a, 0)], S["mv_" + a].at[q, c], S["mvsem"].at[j, q, 0], S["mvsem"].at[j, q, 1], sib)))

    def region(ref, i, level, v):
        l, a, col, n, o = UNITS[i]
        idx = view(a, o, at, level, v)
        return ref.at[(l, *idx, *([ALL] * (4 - len(idx))), pl.ds(col, n))]

    def pos(i, level, off):
        a = UNITS[i][1]
        dim = UNITS[i][4][level] if level < 2 else LASTDIM[a]
        off %= SIZE[dim]
        if level < 2:
            return spots[dim][off]
        return windows[off] if a == "d" else pl.ds(spots[dim][off], 1)

    def result(gi, block, half):
        l, a = GROUPS[gi]
        b = spots["x"][OFFSETS[block]]
        task = 2 * block + half if a == "d" else 4 * half + block
        buf = S["res_d" if a == "d" else "res_u"].at[task % 2]
        if half == 0:
            return lambda: remote_copy(buf, S["loc_" + a].at[l, b], S["ds"].at[gi, block], S["dr"].at[gi, block], sib)
        return lambda: pltpu.make_async_copy(buf, mine[a].at[l, b], S["os"].at[gi, block])

    def offset_of(block):
        return lax.select(block == 0, 2, lax.select(block == 1, 1, lax.select(block == 2, 3, 0)))

    def task_of(a, s):
        return (s // 2, s % 2) if a == "d" else (s % 4, s // 4)

    out_waited, sib_waited = set(), set()

    def wait_out(gi, block, half):
        if (gi, block, half) not in out_waited:
            out_waited.add((gi, block, half))
            cp = result(gi, block, half)()
            cp.wait() if half else cp.wait_send()

    def wait_terms(i, off):
        l, a, _, _, o = UNITS[i]
        gi = GROUPS.index((l, a))
        for block, b in enumerate(OFFSETS):
            if o[0] == "x" and b != off % 4:
                continue
            wait_out(gi, block, 1)
            if (gi, block) not in sib_waited:
                sib_waited.add((gi, block))
                result(gi, block, 0)().wait_recv()

    uses = {a: [] for a in "ugd"}
    for _, events in steps:
        for kind, level, key, s, k in events:
            if level == 0:
                h = SIZE[UNITS[key][4][0]] // 2
                if kind == "start" or k < h:
                    uses[UNITS[key][1]].append((key, h if kind == "start" else s * (h - k)))
    nth = {a: 0 for a in "ugd"}
    fetched = {a: 0 for a in "ugd"}

    def stage(a, n):
        i, off = uses[a][n]
        buf = S["stage_" + a].at[n % NB, :, :, :, pl.ds(0, UNITS[i][3])]
        return pltpu.make_async_copy(region(mine[a], i, 0, pos(i, 0, off)), buf, S["stsem_" + a].at[n % NB]), buf

    complete = set()

    def fetch_ahead(a):
        while fetched[a] < min(len(uses[a]), nth[a] + NB):
            i, off = uses[a][fetched[a]]
            if UNITS[i][:2] not in complete:
                return
            wait_terms(i, off)
            stage(a, fetched[a])[0].start()
            fetched[a] += 1

    def fetch_now(a, n):
        if fetched[a] == n:
            wait_terms(*uses[a][n])
            stage(a, n)[0].start()
            fetched[a] += 1

    own_fetched = set()

    sent = {}

    def own_buffer(i):
        return S["slot0_%d" % i].at[0, 0] if UNITS[i][0] else S["own_%d" % i]

    def own(i):
        return pltpu.make_async_copy(region(mine[UNITS[i][1]], i, 0, pos(i, 0, 0)), own_buffer(i), S["ownsem"].at[i])

    def fetch_own(i):
        if i in own_fetched or (UNITS[i][0] and i not in sent):
            return
        if UNITS[i][0]:
            sent[i]().wait_send()
        own_fetched.add(i)
        wait_terms(i, 0)
        own(i).start()

    def operands(level, i, off):
        _, a, _, _, o = UNITS[i]
        v = pos(i, level, off)
        here = region(S["loc_" + a], i, level, v)
        if level == 0:
            wait_terms(i, off)
            n = nth[a]
            assert uses[a][n] == (i, off)
            fetch_now(a, n)
            cp, buf = stage(a, n)
            cp.wait()
            nth[a] += 1
            return [buf, here]
        h = SIZE[o[0]] // 2
        first = [own_buffer(i)] + [S["slot0_%d" % i].at[d, h - 1] for d in (0, 1)]
        if level == 1:
            return [here] + [f.at[v] for f in first]
        w = pos(i, 1, 0)
        return [here] + [f.at[w, v] for f in first] + [S["slot1_%d" % i].at[d, 1, v] for d in (0, 1)]

    def half(ref, which, level, a):
        if level == 2 and TALL[a] == 1:
            return ref.at[..., pl.ds(896, 768) if which else pl.ds(0, 896)]
        n = ref.shape[0] // 2
        return ref.at[pl.ds(n * which, n)]

    def parts(key):
        r = []
        for i, u in enumerate(UNITS):
            if u[:2] == key:
                for lo, hi in ((0, 896), (896, 1664)):
                    a, b = max(lo, u[2]), min(hi, u[2] + u[3])
                    if a < b:
                        r.append((i, pl.ds(a - u[2], b - a), pl.ds(a, b - a), lo > 0))
        return r

    def cut(ref, cs):
        return ref.at[..., cs]

    def event(ev):
        kind, level, key, s, k = ev
        l, a = UNITS[key][:2] if level < 2 else key
        tag = "%d" % key if level < 2 else "%d%s" % key
        dim = UNITS[key][4][level] if level < 2 else LASTDIM[a]
        h = SIZE[dim] // 2
        if kind == "end":
            finish(l, a)
            return
        slot, rsem, ssem = (S["%s%d_%s" % (n, level, tag)] for n in ("slot", "r", "s"))

        def send(src, d, k):
            dst = lambda: slot.at[d, k] if k else half(slot.at[d, 0], d, level, a)
            remote(lambda: remote_copy(src(), dst(), ssem.at[d, k], rsem.at[d, k], near[dim, 1 - 2 * d]))

        if kind == "start":
            if level == 1:
                wait_terms(key, 0)
                fetch_own(key)
                assert key in own_fetched
                own(key).wait()
            dst = (lambda: S["first_" + tag]) if level == 2 else (lambda: region(S["loc_" + a], key, level, pos(key, level, h)))
            if level < 2:
                addsum(dst(), operands(level, key, h))
            else:
                for i, uc, sc, _ in parts(key):
                    addsum(cut(dst(), sc), [cut(o, uc) for o in operands(level, i, h)])
            for d in (0, 1):
                send(lambda d=d: half(dst(), d, level, a), d, 0)
            if level == 0:
                fetch_own(key)
                fetch_ahead(a)
            return
        d = 0 if s > 0 else 1
        block = slot.at[d, k - 1]
        got = half(block, d, level, a) if k == 1 else block
        remote_copy(got, got, ssem.at[d, k - 1], rsem.at[d, k - 1], sib).wait_recv()
        if k == h:
            if level == 0:
                fetch_own(key)
            return
        off = s * (h - k)
        if level < 2:
            ops = operands(level, key, off)
            if k > 1:
                addsum(block, [block] + ops)
            else:
                for w in (0, 1):
                    hm = half(block, w, level, a)
                    addsum(hm, ([hm] if w == d else []) + [half(r, w, level, a) for r in ops])
        else:
            for i, uc, sc, w in parts(key):
                ops = [cut(o, uc) for o in operands(level, i, off)]
                m = cut(block, sc)
                if k > 1:
                    addsum(m, [m] + ops)
                elif TALL[a] == 1:
                    addsum(m, ([m] if w == (d == 1) else []) + ops)
                else:
                    for w in (0, 1):
                        hm = half(m, w, level, a)
                        addsum(hm, ([hm] if w == d else []) + [half(r, w, level, a) for r in ops])
        send(lambda: slot.at[d, k - 1], d, k)
        if (level, d, k) == (0, 0, 1) and l:
            sent[key] = pend.pop()
        if level == 0:
            fetch_ahead(a)

    def finish(l, a):
        h = SIZE[LASTDIM[a]] // 2
        for i, uc, sc, _ in parts((l, a)):
            ops = [cut(o, uc) for o in operands(2, i, 0)] + [cut(S["slot2_%d%s" % (l, a)].at[d, h - 1], sc) for d in (0, 1)]
            addsum(cut(S["red_" + a].at[l], sc), ops)

    filled = {}
    holds = ("y", 1)
    left(*GROUPS[0]).wait()
    for gi, (l, a) in enumerate(GROUPS):
        wants = ("y" if a == "d" else "a", l)
        if wants != holds:
            left(l, a).start()
            left(l, a).wait()
            holds = wants
        first_load = sum(4 if g[1] == "d" else 2 for g in GROUPS[:gi])

        for k in (0, 1):
            if (a == "d", k) in filled:
                wait_out(*filled[a == "d", k])
        for ev in steps[gi][1]:
            event(ev)
        res = S["res_d" if a == "d" else "res_u"]

        def away(s, block, half_, gi=gi, l=l, a=a, res=res):
            b = lax.rem(x + offset_of(block), 4)
            buf = res.at[lax.rem(s, 2)]
            return (remote_copy(buf, S["loc_" + a].at[l, b], S["ds"].at[gi, block], S["dr"].at[gi, block], sib),
                    pltpu.make_async_copy(buf, mine[a].at[l, b], S["os"].at[gi, block]))

        def loop(s, _, l=l, a=a, first_load=first_load, res=res, away=away):
            block, half_ = (lax.div(s, 2), lax.rem(s, 2)) if a == "d" else (lax.rem(s, 4), lax.div(s, 4))
            n = lax.rem(block, 2) if a == "d" else half_

            @pl.when((half_ if a == "d" else block) == 0)
            def _():
                src, buf = (act["h", l].at[pl.ds(0, 832)], S["right"].at[n, pl.ds(0, 832), pl.ds(0, 1024)]) if a == "d" else (act[a, l].at[:, pl.ds(0, 1664)], S["right"].at[n])
                pltpu.make_async_copy(src, buf, S["rightsem"].at[n]).wait()
            before = (lax.div(s - 2, 2), half_) if a == "d" else (lax.rem(s - 2, 4), lax.div(s - 2, 4))
            send, keep = away(s, *before)

            @pl.when((s >= 2) & (before[1] == 0))
            def _():
                send.wait_send()

            @pl.when((s >= 2) & (before[1] == 1))
            def _():
                keep.wait()
            if a == "d":
                cols = pl.ds(pl.multiple_of(lax.select(half_ == 0, 1 - c, c) * 512, 512), 512)
                t = jnp.dot(S["right"][n, pl.ds(0, 832), pl.ds(0, 1024)], S["left"][:, cols], preferred_element_type=F32)
                res[lax.rem(s, 2)] = t.reshape(4, 26, 8, 512).astype(BF)
            else:
                rows = pl.ds(pl.multiple_of(lax.rem(x + offset_of(block), 4) * 256, 256), 256)
                t = jnp.dot(S["left"][rows], S["right"][half_], preferred_element_type=F32)
                res[lax.rem(s, 2)] = t.reshape(4, 8, 8, 1664).astype(BF)
            send, keep = away(s, block, half_)
            pl.when(half_ == 0)(send.start)
            pl.when(half_ == 1)(keep.start)
            for k in range(4 if a == "d" else 2):
                if first_load + k + 2 < len(loads):
                    pl.when(s == (2 * k + 1 if a == "d" else 4 * k + 3))(right(first_load + k + 2).start)
            return 0
        lax.fori_loop(0, 8, loop, 0)
        for k in range(6):
            out_waited.add((gi, *task_of(a, k)))
        for k in (0, 1):
            filled[a == "d", k] = gi, *task_of(a, 6 + k)
        complete.add((l, a))
        fetch_ahead(a)
    for ev in steps[-1][1]:
        event(ev)
    for gi, (l, a) in enumerate(GROUPS):
        for k in range(8):
            wait_out(gi, *task_of(a, k))

    total = jnp.zeros((8, 128), F32)
    for a in "ugd":
        for l in (0, 1):
            for t in range(TALL[a]):
                for q in range(WIDTH[a] // 128):
                    g = S["red_" + a][l, t, :, q * 128:q * 128 + 128].astype(F32)
                    if a == "d":
                        row = lax.broadcasted_iota(jnp.int32, (8, 128), 0) + 8 * t
                        g = jnp.where((row >= 2 * zz) & (row < 2 * zz + 26), g, 0.0)
                    total = total + g * g
    total = jnp.sum(total, axis=0, keepdims=True)
    for r, (buf, ds) in enumerate(((S["ar_z"], [(0, 0, q // 2, q % 2) for q in range(16)]), (S["ar_p"], [(q // 4, q % 4, 0, 0) for q in range(16)]))):
        buf[0] = total
        cps = []
        for q in range(1, 16):
            dx, dy, dz, dc = ds[q]
            to = device({"x": lax.rem(at["x"] + dx, 4), "y": lax.rem(at["y"] + dy, 4), "z": lax.rem(at["z"] + dz, 8), "c": lax.rem(c + dc, 2)})
            cps.append(remote(lambda q=q, to=to: remote_copy(buf.at[0], buf.at[q], S["arsem"].at[2 * r, q], S["arsem"].at[2 * r + 1, q], to)))
        for cp in cps:
            cp.wait_recv()
            cp.wait_send()
            pend.pop()
        total = buf[0]
        for q in range(1, 16):
            total = total + buf[q]
    mean = jnp.sum(total, axis=1, keepdims=True) / COUNT
    factor = jnp.minimum(1.0, 0.5 * lax.rsqrt(mean + 1e-30))
    for cp in moment_copies:
        cp.wait_recv() if cp.is_remote else cp.wait()

    def adamw(w, m, v, g):
        g = g * factor
        m = 0.9 * m + 0.1 * g
        v = 0.95 * v + 0.05 * g * g
        step = m * lax.rsqrt(v + 1e-8) + 0.1 * w
        return (w - 0.02 * step).astype(BF), m, v

    for a in "ug":
        mv, red, wv = S["mv_" + a], S["red_" + a], S["w_" + a]

        def body(q, _, mv=mv, red=red, wv=wv, a=a):
            cs = pl.ds(pl.multiple_of(q * 128, 128), 128)
            for l in (0, 1):
                m, v = (jnp.concatenate([mv[e, 0, l, :, cs], mv[e, 1, l, :, cs]], axis=0) for e in (0, 1))
                n, m, v = adamw(wv[l, 0, :, cs].astype(F32), m, v, red[l, 0, :, cs].astype(F32))
                wv[l, 0, :, cs] = n
                for e, t in enumerate((m, v)):
                    for s in (0, 1):
                        mv[e, s, l, :, cs] = t[4 * s:4 * s + 4]
            return 0
        lax.fori_loop(0, 13, body, 0)
    row = lax.broadcasted_iota(jnp.int32, (32, 32), 0)
    column = lax.broadcasted_iota(jnp.int32, (32, 32), 1)
    pick = (column == 2 * zz + 13 * (row >> 4) + (row & 15)) & ((row & 15) < 13)
    pick = jnp.where(pick, 1.0, 0.0).astype(BF)
    for l in (0, 1):
        gd, wd = (jnp.dot(pick, S[n][l].reshape(32, 512), preferred_element_type=F32) for n in ("red_d", "w_d"))
        for s in (0, 1):
            rows = slice(16 * s, 16 * s + 16)
            n, m, v = adamw(wd[rows], S["mv_d"][0, s, l], S["mv_d"][1, s, l], gd[rows])
            S["new_d"][l, s] = n
            S["mv_d"][0, s, l] = m
            S["mv_d"][1, s, l] = v
    ends = []
    for j, a in enumerate("ugd"):
        cp = pltpu.make_async_copy(S["new_d"] if a == "d" else S["w_" + a].at[:, 0], new[a], S["newsem"].at[j])
        cp.start()
        ends.append(cp.wait)
        for q in (0, 1):
            out = new_moments[a][q].at[:, :, halfcols(a, 1)]
            cp = remote_copy(S["mv_" + a].at[q, 1 - c], out, S["finsem"].at[j, q, 0], S["finsem"].at[j, q, 1], sib)
            cp.start()
            back = remote_copy(S["mv_" + a].at[q, 1 - c], new_moments[a][q].at[:, :, halfcols(a, 0)], S["finsem"].at[j, q, 0], S["finsem"].at[j, q, 1], sib)
            ends += [cp.wait_send, back.wait_recv]
            cp = pltpu.make_async_copy(S["mv_" + a].at[q, c], out, S["finsem"].at[j, q, 2])
            cp.start()
            ends.append(cp.wait)
    for wait in ends:
        wait()
    for make in pend:
        make().wait_send()


def reduce_scatter(acts, weights, m, v):
    args = list(acts) + [w.reshape(2, 4, 4, -1, 8, w.shape[-1]) for w in weights] + [*m, *v]
    sh = rs_scratch()
    any_ = pl.BlockSpec(memory_space=pl.ANY)
    outs = [jax.ShapeDtypeStruct(s, BF) for s in ((2, 8, 1664), (2, 8, 1664), (2, 2, 16, 512))] + [jax.ShapeDtypeStruct(t.shape, F32) for t in (*m, *v)]
    outs += [jax.ShapeDtypeStruct((2, 4, 4, TILES[a], 8, WIDTH[a]), BF) for a in "ugd"]
    outs = pl.pallas_call(
        functools.partial(rs_kernel, list(sh)), out_shape=outs, in_specs=[any_] * 19, out_specs=[any_] * 12, scratch_shapes=list(sh.values()), name="reduce_scatter",
        compiler_params=pltpu.CompilerParams(collective_id=0, has_side_effects=True, vmem_limit_bytes=VMEM_BYTES))(*args)
    return outs[:3], outs[3:6], outs[6:9]


def plan_ag():
    RATE, LAT = 46.0e3, 2.9
    free, heap, order, seq, got, now = {}, [], [], [0], {}, 1.0

    def push(t, ev):
        seq[0] += 1
        heapq.heappush(heap, (t, seq[0], ev))

    def send(t, link, nbytes):
        free[link] = max(free.get(link, 0.0), t) + nbytes / RATE
        return free[link] + LAT
    ring = {(2, a): (LASTDIM[a], {"u": 8 * 1664, "g": 8 * 1664, "d": 32 * 512}[a] * 4) for a in "ugd"}
    for i, (_, a, _, cols, o) in enumerate(UNITS):
        ring[1, i] = (o[1], DEPTH[a] * 8 * cols * 2)
        ring[0, i] = (o[0], 4 * DEPTH[a] * 8 * cols * 2)
    for a in "gdu":
        push(1.0, ("start", 2, a, 0, 0))
    while heap:
        t, _, ev = heapq.heappop(heap)
        kind, level, key, s, k = ev
        dim, nbytes = ring[level, key]
        h = SIZE[dim] // 2
        now = max(now, t) + 0.1
        order.append(ev)
        if kind == "start":
            for s in (1, -1):
                push(send(now, (dim, s), nbytes), ("step", level, key, s, 1))
            continue
        if k < h:
            push(send(now, (dim, s), nbytes if k < h - 1 else nbytes // 2), ("step", level, key, s, k + 1))
            continue
        got[level, key] = got.get((level, key), 0) + 1
        if got[level, key] < 2:
            continue
        if level == 2:
            for i, u in enumerate(UNITS):
                if u[1] == key:
                    push(now + (1.0 if key == "d" else 0), ("start", 1, i, 0, 0))
        elif level == 1:
            push(now, ("start", 0, key, 0, 0))
    return order, now, free


def ag_scratch():
    sem = pltpu.SemaphoreType.DMA
    sh = {"pc": pltpu.VMEM((8, 2, 2, 16, 512), BF), "asm": pltpu.VMEM((2, 26, 8, 512), BF), "loc": sem((4,)), "sr": sem((128,)), "ss": sem((128,))}
    for n in "rs":
        for a in "ugd":
            sh["%s2_%s" % (n, a)] = sem((2, SIZE[LASTDIM[a]] // 2))
        for i, u in enumerate(UNITS):
            for lv in (0, 1):
                sh["%s%d_%d" % (n, lv, i)] = sem((2, SIZE[u[4][lv]] // 2))
    return sh


def ag_kernel(names, *refs):
    own = {a: refs[j] for j, a in enumerate("ugd")}
    out = {a: refs[3 + j] for j, a in enumerate("ugd")}
    S = dict(zip(names, refs[6:], strict=True))
    at = coords()
    c, x, y, z = at["c"], at["x"], at["y"], at["z"]
    sib = device({**at, "c": 1 - c})
    order, _, _ = plan_ag()
    spots, near = places(at)
    peers = [sib, *near.values()]
    bar = pltpu.get_barrier_semaphore()
    for p in peers:
        pl.semaphore_signal(bar, inc=1, device_id=p, device_id_type=MESH)

    def hc(a, col=0, n=None):
        return pl.ds(pl.multiple_of(c * WIDTH[a] + col, 128), WIDTH[a] if n is None else n)
    local = [pltpu.make_async_copy(own["u"], out["u"].at[:, x, y, z, :, hc("u")], S["loc"].at[0]),
             pltpu.make_async_copy(own["g"], out["g"].at[:, x, y, z, :, hc("g")], S["loc"].at[1]),
             pltpu.make_async_copy(own["d"], S["pc"].at[z], S["loc"].at[2])]
    for cp in local:
        cp.start()
    pl.semaphore_wait(bar, len(peers))
    for cp in local:
        cp.wait()
    pend, twin = [], []

    def remote(src, ss, rs, to):
        cp = remote_copy(src, src, ss, rs, to)
        cp.start()
        pend.append(cp)

    def to_sibling(ref):
        n = len(twin)
        remote(ref, S["ss"].at[n], S["sr"].at[n], sib)
        twin.append(ref)

    def region(level, key, v):
        if level == 2:
            if key == "d":
                return S["pc"].at[v]
            return out["u"].at[:, x, v, z, :, hc("u")] if key == "u" else out["g"].at[:, x, y, v, :, hc("g")]
        l, a, col, n, o = UNITS[key]
        idx = view(a, o, at, level, v)
        return out[a].at[(l, *idx, *([ALL] * (4 - len(idx))), hc(a, col, n))]

    def half(ref, which):
        n = ref.shape[0] // 2
        return ref.at[pl.ds(n * which, n)]

    got = {}
    for kind, level, key, s, k in order:
        dim = UNITS[key][4][level] if level < 2 else LASTDIM[key]
        n = SIZE[dim]
        h = n // 2
        rsem, ssem = S["r%d_%s" % (level, key)], S["s%d_%s" % (level, key)]

        def send(src, d, k, dim=dim, rsem=rsem, ssem=ssem):
            remote(src, ssem.at[d, k], rsem.at[d, k], near[dim, 1 - 2 * d])

        if kind == "start":
            for d in (0, 1):
                send(region(level, key, at[dim]), d, 0)
            continue
        d = 0 if s > 0 else 1
        block = region(level, key, spots[dim][-s * k % n])
        if k == h:
            block = half(block, d)
        remote_copy(block, block, ssem.at[d, k - 1], rsem.at[d, k - 1], sib).wait_recv()
        if k < h - 1:
            send(block, d, k)
        elif k == h - 1:
            send(half(block, d), d, k)
        if level < 2:
            to_sibling(block)
        if k == h:
            got[level, key] = got.get((level, key), 0) + 1
            if level == 2 and got[level, key] == 2:
                if key == "d":
                    q = lax.broadcasted_iota(jnp.int32, (208, 256), 1)
                    r = lax.broadcasted_iota(jnp.int32, (208, 256), 0)
                    e = q & 15
                    pick = (r == 26 * (q >> 5) + 13 * ((q >> 4) & 1) + e) & (e < 13)
                    pick = jnp.where(pick, 1.0, 0.0).astype(BF)
                    for l in (0, 1):
                        rows = jnp.dot(pick, S["pc"][:, l].reshape(256, 512), preferred_element_type=F32)
                        S["asm"][l] = rows.reshape(26, 8, 512).astype(BF)
                    cp = pltpu.make_async_copy(S["asm"], out["d"].at[:, x, y, :, :, hc("d")], S["loc"].at[3])
                    cp.start()
                    cp.wait()
                idx = (ALL, x, ALL, z, ALL) if key == "u" else (ALL, x, y, ALL, ALL)
                to_sibling(out[key].at[(*idx, hc(key))])
    for n, ref in enumerate(twin):
        remote_copy(ref, ref, S["ss"].at[n], S["sr"].at[n], sib).wait_recv()
    for cp in pend:
        cp.wait_send()


def all_gather(u, g, d):
    sh = ag_scratch()
    any_ = pl.BlockSpec(memory_space=pl.ANY)
    outs = [jax.ShapeDtypeStruct((2, 4, 4, TILES[a], 8, 2 * WIDTH[a]), BF) for a in "ugd"]
    return pl.pallas_call(
        functools.partial(ag_kernel, list(sh)), out_shape=outs, in_specs=[any_] * 3, out_specs=[any_] * 3, scratch_shapes=list(sh.values()), name="all_gather",
        compiler_params=pltpu.CompilerParams(collective_id=1, has_side_effects=True, vmem_limit_bytes=VMEM_BYTES))(u, g, d)


T = 1024
B = 256
N = 3328 // B
NT = (((1,), (1,)), ((), ()))


def dot(a, b, dims=(((1,), (0,)), ((), ()))):
    return lax.dot_general(a, b, dims, preferred_element_type=F32)


def norm_scale(wide):
    return lax.rsqrt(jnp.mean(wide**2, -1, keepdims=True) + 1e-6)


def rowwise(n, body, step=128):
    def one(i, _):
        body(pl.ds(pl.multiple_of(i * step, step), step))
        return 0
    lax.fori_loop(0, n // step, one, 0)


def silu_back(g, u, dh):
    s = jax.nn.sigmoid(g)
    silu = g * s
    return silu, (dh * u * (s + silu * (1.0 - s))).astype(BF), (dh * silu).astype(BF)


def norm_into(h, a):
    def norm(rows):
        wide = h[rows].astype(F32)
        a[rows] = (wide * norm_scale(wide)).astype(BF)
    rowwise(T, norm)


def pipelined(chunk, first, second):
    held = None
    for m in range(0, T, chunk):
        rows = slice(m, m + chunk)
        now = first(rows)
        if held is not None:
            second(*held)
        held = rows, now
    second(*held)


def fwd0(C, tr, x, wg, wu, wd, gate, up, ht, h1, at, a, hid):
    j = pl.program_id(0)

    @pl.when(j == 0)
    def _():
        norm_into(x, a)
        at[...] = a[...].T if tr else a[...]

    @pl.when(j < N)
    def _():
        def first(rows):
            return dot(a[rows], wg[...]), dot(a[rows], wu[...])

        def second(rows, gu):
            g, u = gu
            gate[rows] = g
            up[rows] = u
            v = (g * jax.nn.sigmoid(g) * u).astype(BF)
            hid[j, rows] = v
            if tr:
                ht[:, rows] = v.T
            else:
                ht[rows] = v
        pipelined(C, first, second)

    @pl.when(j >= N)
    def _():
        def first(rows):
            return sum(dot(hid[i, rows], wd[i * B:i * B + B]) for i in range(N))

        def second(rows, y):
            n = pl.ds(pl.multiple_of((j - N) * B, B), B)
            h1[rows] = (x[rows, n].astype(F32) + y.astype(BF).astype(F32)).astype(BF)
        pipelined(C, first, second)


def layer0(x, w_gate, w_up, w_down, C=512, tr=True):
    whole = pl.BlockSpec((T, T), lambda j: (0, 0))
    cap = lambda j: jnp.minimum(j, N - 1)
    cols = pl.BlockSpec((T, B), lambda j: (0, cap(j)))
    wcols = pl.BlockSpec((None, T, B), lambda j: (0, 0, cap(j)))
    late = lambda j: jnp.maximum(j - N, 0)
    wrows = pl.BlockSpec((None, 3328, B), lambda j: (0, 0, late(j)))
    rows = pl.BlockSpec((B, T), lambda j: (cap(j), 0)) if tr else cols
    o = jax.ShapeDtypeStruct
    blk = pl.BlockSpec((None, T, B), lambda j: (cap(j), 0, 0))
    return pl.pallas_call(functools.partial(fwd0, C, tr), grid=(N + 4,), in_specs=[whole, wcols, wcols, wrows],
        out_specs=[blk, blk, rows, pl.BlockSpec((T, B), lambda j: (0, late(j))), whole],
        out_shape=[o((N, T, B), F32)] * 2 + [o((3328, T) if tr else (T, 3328), BF), o((T, T), BF), o((T, T), BF)],
        scratch_shapes=[pltpu.VMEM((T, T), BF), pltpu.VMEM((N, T, B), BF)], name="layer0",
        compiler_params=pltpu.CompilerParams(vmem_limit_bytes=VMEM_BYTES))(x, w_gate, w_up, w_down)


def both1(C, tr, h, dy, wg, wu, wd, wg2, wu2, ht, dg, du, at, dh1, a, gs, us, acc):
    j = pl.program_id(0)

    @pl.when(j == 0)
    def _():
        norm_into(h, a)
        at[...] = a[...].T if tr else a[...]

    @pl.when(j < N)
    def _():
        def first(rows):
            return dot(a[rows], wg[...]), dot(a[rows], wu[...]), dot(dy[rows], wd[...], NT)

        def second(rows, parts):
            g, u, dh = parts
            silu, dgate, dup = silu_back(g, u, dh.astype(BF).astype(F32))
            v = (silu * u).astype(BF)
            if tr:
                ht[:, rows] = v.T
            else:
                ht[rows] = v
            dg[rows] = dgate
            gs[j, rows] = dgate
            du[rows] = dup
            us[j, rows] = dup
        pipelined(C, first, second)

    @pl.when(j >= N)
    def _():
        def first(rows):
            return sum(dot(gs[i, rows], wg2[:, i * B:i * B + B], NT) + dot(us[i, rows], wu2[:, i * B:i * B + B], NT) for i in range(N))

        def second(rows, y):
            n = pl.ds(pl.multiple_of((j - N) * B, B), B)
            acc[rows, n] = y
        pipelined(C, first, second)

    @pl.when(j == N + 3)
    def _():
        def back(rows):
            wide = h[rows].astype(F32)
            scale = norm_scale(wide)
            d = acc[rows].astype(BF).astype(F32)
            d = d * scale - wide * (scale * scale * scale * jnp.mean(d * wide, -1, keepdims=True))
            dh1[rows] = (dy[rows].astype(F32) + d.astype(BF).astype(F32)).astype(BF)
        rowwise(T, back)


def layer1(h, dy, w_gate, w_up, w_down, C=512, tr=True):
    cap = lambda j: jnp.minimum(j, N - 1)
    late = lambda j: jnp.maximum(j - N, 0)
    whole = pl.BlockSpec((T, T), lambda j: (0, 0))
    cols = pl.BlockSpec((T, B), lambda j: (0, cap(j)))
    wcols = pl.BlockSpec((None, T, B), lambda j: (1, 0, cap(j)))
    wrows = pl.BlockSpec((None, B, T), lambda j: (1, cap(j), 0))
    wtall = pl.BlockSpec((None, B, 3328), lambda j: (1, late(j), 0))
    rows = pl.BlockSpec((B, T), lambda j: (cap(j), 0)) if tr else cols
    o = jax.ShapeDtypeStruct
    blk = pl.BlockSpec((None, T, B), lambda j: (cap(j), 0, 0))
    return pl.pallas_call(functools.partial(both1, C, tr), grid=(N + 4,), in_specs=[whole, whole, wcols, wcols, wrows, wtall, wtall], out_specs=[rows, cols, cols, whole, whole],
        out_shape=[o((3328, T) if tr else (T, 3328), BF)] + [o((T, 3328), BF)] * 2 + [o((T, T), BF)] * 2,
        scratch_shapes=[pltpu.VMEM((T, T), BF), pltpu.VMEM((N, T, B), BF), pltpu.VMEM((N, T, B), BF), pltpu.VMEM((T, T), F32)], name="layer1",
        compiler_params=pltpu.CompilerParams(vmem_limit_bytes=VMEM_BYTES))(h, dy, w_gate, w_up, w_down, w_gate, w_up)


def back0(C, dh1, gate, up, wd, dg, du):
    def first(rows):
        return dot(dh1[rows], wd[...], NT)

    def second(rows, dh):
        _, dg[rows], du[rows] = silu_back(gate[rows], up[rows], dh.astype(BF).astype(F32))
    pipelined(C, first, second)


def back(dh1, gate, up, w_down, C=512):
    whole = pl.BlockSpec((T, T), lambda j: (0, 0))
    blk = pl.BlockSpec((None, T, B), lambda j: (j, 0, 0))
    cols = pl.BlockSpec((T, B), lambda j: (0, j))
    wrows = pl.BlockSpec((None, B, T), lambda j: (0, j, 0))
    o = jax.ShapeDtypeStruct
    return pl.pallas_call(functools.partial(back0, C), grid=(N,), in_specs=[whole, blk, blk, wrows], out_specs=[cols, cols],
        out_shape=[o((T, 3328), BF)] * 2, name="back0",
        compiler_params=pltpu.CompilerParams(vmem_limit_bytes=VMEM_BYTES))(dh1, gate, up, w_down)


def solution(mesh):
    def step(x, dy, w_gate, w_up, w_down, *moments):
        x, dy = x[0], dy[0]
        gate0, up0, hid0, h1, a0 = layer0(x, w_gate, w_up, w_down)
        hid1, dgate1, dup1, a1, dh1 = layer1(h1, dy, w_gate, w_up, w_down)
        dgate0, dup0 = back(dh1, gate0, up0, w_down)
        m, v = moments[:3], moments[3:]
        order = lambda t: (t[1], t[0], t[2])
        pad = lambda t: (*t[:2], jnp.pad(t[2], ((0, 0), (0, 3), (0, 0))))
        acts = (a0, a1, hid0, hid1, dup0, dup1, dgate0, dgate1, dh1, dy)
        new, m, v = reduce_scatter(acts, order((w_gate, w_up, w_down)), pad(order(m)), pad(order(v)))
        u, g, d = all_gather(*new)
        w = (g.reshape(w_gate.shape), u.reshape(w_up.shape), d.reshape(w_down.shape))
        cut = lambda t: (t[1], t[0], t[2][:, :13])
        return (*w, *cut(m), *cut(v))

    data, whole, rows = P(("rep", "dp"), None, None), P(), P(None, "dp", None)
    out = P("rep", None, None)
    return jax.shard_map(step, mesh=mesh, in_specs=(data, data) + (whole,) * 3 + (rows,) * 6, out_specs=(out,) * 3 + (P("rep", "dp", None),) * 6, check_vma=False)
```

```python
import functools
import heapq

import jax
import jax.numpy as jnp
from jax import lax
from jax.experimental import pallas as pl
from jax.experimental.pallas import tpu as pltpu
from jax.sharding import PartitionSpec as P

MESH = pl.DeviceIdType.MESH
BF, F32 = jnp.bfloat16, jnp.float32
SIZE = {"x": 4, "y": 4, "z": 8}
VMEM_BYTES = 67043328
ALL = slice(None)


def coords():
    i = lax.axis_index("dp")
    return {"x": i // 64, "y": lax.rem(i // 16, 4), "z": lax.rem(i // 2, 8), "c": lax.rem(i, 2)}


def device(at):
    return {"dp": ((at["x"] * 4 + at["y"]) * 8 + at["z"]) * 2 + at["c"]}


def places(at):
    spots = {d: [at[d]] + [lax.rem(at[d] + k, n) for k in range(1, n)] for d, n in SIZE.items()}
    return spots, {(d, s): device({**at, d: spots[d][s]}) for d in SIZE for s in (1, -1)}


UNITS = [
    (1, "d", 0, 256, "xyz"), (1, "d", 256, 256, "yxz"), (1, "u", 0, 896, "zxy"), (1, "u", 896, 768, "zxy"), (1, "g", 0, 896, "xyz"), (1, "g", 896, 768, "yxz"),
    (0, "d", 0, 256, "xyz"), (0, "d", 256, 256, "yxz"), (0, "u", 0, 896, "zxy"), (0, "u", 896, 768, "zxy"), (0, "g", 0, 896, "yxz"), (0, "g", 896, 768, "xyz"),
]
DEPTH = {"u": 4, "g": 8, "d": 26}
TILES = {"u": 8, "g": 8, "d": 26}
WIDTH = {"u": 1664, "g": 1664, "d": 512}
TALL = {"u": 1, "g": 1, "d": 4}
LASTDIM = {"u": "y", "g": "z", "d": "z"}
ROWS = {"u": 4, "g": 4, "d": 16}
COUNT = 2 * 3 * 1024 * 3328
NB = 2


def view(a, order, at, level, v):
    if level == 0:
        return {"z": (ALL, ALL, v), "x": (v,), "y": (ALL, v)}[order[0]]
    if level == 1:
        return {"zxy": (v, ALL, at["z"]), "xyz": (at["x"], v), "yxz": (v, at["y"])}[order]
    return (at["x"], v, at["z"]) if a == "u" else (at["x"], at["y"], v)


def block_shape(i, level):
    _, a, _, cols, _ = UNITS[i]
    return ((4, DEPTH[a], 8, cols), (DEPTH[a], 8, cols))[level]


def remote_copy(src, dst, ss, rs, to):
    return pltpu.make_async_remote_copy(src_ref=src, dst_ref=dst, send_sem=ss, recv_sem=rs, device_id=to, device_id_type=MESH)


T = 1024
B = 256
N = 3328 // B
NT = (((1,), (1,)), ((), ()))


def dot(a, b, dims=(((1,), (0,)), ((), ()))):
    return lax.dot_general(a, b, dims, preferred_element_type=F32)


def norm_scale(wide):
    return lax.rsqrt(jnp.mean(wide**2, -1, keepdims=True) + 1e-6)


def rowwise(n, body, step=128):
    def one(i, _):
        body(pl.ds(pl.multiple_of(i * step, step), step))
        return 0
    lax.fori_loop(0, n // step, one, 0)


def silu_back(g, u, dh):
    s = jax.nn.sigmoid(g)
    silu = g * s
    return silu, (dh * u * (s + silu * (1.0 - s))).astype(BF), (dh * silu).astype(BF)


def norm_into(h, a):
    def norm(rows):
        wide = h[rows].astype(F32)
        a[rows] = (wide * norm_scale(wide)).astype(BF)
    rowwise(T, norm)


def pipelined(chunk, first, second):
    held = None
    for m in range(0, T, chunk):
        rows = slice(m, m + chunk)
        now = first(rows)
        if held is not None:
            second(*held)
        held = rows, now
    second(*held)


def fwd0(C, tr, x, wg, wu, wd, gate, up, ht, h1, at, a, hid):
    j = pl.program_id(0)

    @pl.when(j == 0)
    def _():
        norm_into(x, a)
        at[...] = a[...].T if tr else a[...]

    @pl.when(j < N)
    def _():
        def first(rows):
            return dot(a[rows], wg[...]), dot(a[rows], wu[...])

        def second(rows, gu):
            g, u = gu
            gate[rows] = g
            up[rows] = u
            v = (g * jax.nn.sigmoid(g) * u).astype(BF)
            hid[j, rows] = v
            if tr:
                ht[:, rows] = v.T
            else:
                ht[rows] = v
        pipelined(C, first, second)

    @pl.when(j >= N)
    def _():
        def first(rows):
            return sum(dot(hid[i, rows], wd[i * B:i * B + B]) for i in range(N))

        def second(rows, y):
            n = pl.ds(pl.multiple_of((j - N) * B, B), B)
            h1[rows] = (x[rows, n].astype(F32) + y.astype(BF).astype(F32)).astype(BF)
        pipelined(C, first, second)


def layer0(x, w_gate, w_up, w_down, C=512, tr=True):
    whole = pl.BlockSpec((T, T), lambda j: (0, 0))
    cap = lambda j: jnp.minimum(j, N - 1)
    cols = pl.BlockSpec((T, B), lambda j: (0, cap(j)))
    wcols = pl.BlockSpec((None, T, B), lambda j: (0, 0, cap(j)))
    late = lambda j: jnp.maximum(j - N, 0)
    wrows = pl.BlockSpec((None, 3328, B), lambda j: (0, 0, late(j)))
    rows = pl.BlockSpec((B, T), lambda j: (cap(j), 0)) if tr else cols
    o = jax.ShapeDtypeStruct
    blk = pl.BlockSpec((None, T, B), lambda j: (cap(j), 0, 0))
    return pl.pallas_call(functools.partial(fwd0, C, tr), grid=(N + 4,), in_specs=[whole, wcols, wcols, wrows],
        out_specs=[blk, blk, rows, pl.BlockSpec((T, B), lambda j: (0, late(j))), whole],
        out_shape=[o((N, T, B), F32)] * 2 + [o((3328, T) if tr else (T, 3328), BF), o((T, T), BF), o((T, T), BF)],
        scratch_shapes=[pltpu.VMEM((T, T), BF), pltpu.VMEM((N, T, B), BF)], name="layer0",
        compiler_params=pltpu.CompilerParams(vmem_limit_bytes=VMEM_BYTES))(x, w_gate, w_up, w_down)


def both1(C, h, dy, wg, wu, wd, wg2, wu2, dwd, dwg, dwu, dh1, a, at, gs, us, acc):
    j = pl.program_id(0)

    @pl.when(j == 0)
    def _():
        norm_into(h, a)
        at[...] = a[...].T

    @pl.when(j < N)
    def _():
        g, u = dot(a[...], wg[...]), dot(a[...], wu[...])
        dh = dot(dy[...], wd[...], NT).astype(BF).astype(F32)
        silu, dgate, dup = silu_back(g, u, dh)
        gs[j] = dgate
        us[j] = dup
        hid = (silu * u).astype(BF)
        dwg[...] = dot(at[...], dgate).astype(BF)
        dwu[...] = dot(at[...], dup).astype(BF)
        dwd[...] = dot(hid.T, dy[...]).astype(BF)

    @pl.when(j >= N)
    def _():
        y = sum(dot(gs[i], wg2[:, i * B:i * B + B], NT) + dot(us[i], wu2[:, i * B:i * B + B], NT) for i in range(N))
        acc[:, pl.ds(pl.multiple_of((j - N) * B, B), B)] = y

    @pl.when(j == N + 3)
    def _():
        def back(rows):
            wide = h[rows].astype(F32)
            scale = norm_scale(wide)
            d = acc[rows].astype(BF).astype(F32)
            d = d * scale - wide * (scale * scale * scale * jnp.mean(d * wide, -1, keepdims=True))
            dh1[rows] = (dy[rows].astype(F32) + d.astype(BF).astype(F32)).astype(BF)
        rowwise(T, back)


def layer1(h, dy, w_gate, w_up, w_down, C=512):
    cap = lambda j: jnp.minimum(j, N - 1)
    late = lambda j: jnp.maximum(j - N, 0)
    whole = pl.BlockSpec((T, T), lambda j: (0, 0))
    cols = pl.BlockSpec((T, B), lambda j: (0, cap(j)))
    wcols = pl.BlockSpec((None, T, B), lambda j: (1, 0, cap(j)))
    wrows = pl.BlockSpec((None, B, T), lambda j: (1, cap(j), 0))
    wtall = pl.BlockSpec((None, B, 3328), lambda j: (1, late(j), 0))
    rows = pl.BlockSpec((B, T), lambda j: (cap(j), 0))
    o = jax.ShapeDtypeStruct
    return pl.pallas_call(functools.partial(both1, C), grid=(N + 4,), in_specs=[whole, whole, wcols, wcols, wrows, wtall, wtall], out_specs=[rows, cols, cols, whole],
        out_shape=[o((3328, T), BF)] + [o((T, 3328), BF)] * 2 + [o((T, T), BF)],
        scratch_shapes=[pltpu.VMEM((T, T), BF)] * 2 + [pltpu.VMEM((N, T, B), BF)] * 2 + [pltpu.VMEM((T, T), F32)], name="layer1",
        compiler_params=pltpu.CompilerParams(vmem_limit_bytes=VMEM_BYTES))(h, dy, w_gate, w_up, w_down, w_gate, w_up)


TASKS = (3, 3, 3, 4)


def jobs_of(layer):
    rank = {}
    for i, u in enumerate(UNITS):
        if u[0] == layer:
            n = SIZE[u[4][0]]
            h = n // 2
            for at, off in enumerate([h] + [s * (h - k) for k in range(1, h) for s in (1, -1)] + [0]):
                rank[i, off] = (at / n, i)
    return sorted(rank, key=rank.get)


def plan():
    RATE, LAT, TASK, DRATE, DLAT = 46.0e3, 2.6, 3.3, 500.0e3, 2.0
    free, heap, seq = {}, [], [0]

    def send(t, link, nbytes):
        free[link] = max(free.get(link, 0.0), t) + nbytes / RATE
        return free[link] + LAT

    def push(t, ev):
        seq[0] += 1
        heapq.heappush(heap, (t, seq[0], ev))
    ring = {}
    for i, (l, a, _, cols, o) in enumerate(UNITS):
        ring[0, i] = (o[0], 4 * DEPTH[a] * 8 * cols * 2)
        ring[1, i] = (o[1], DEPTH[a] * 8 * cols * 2)
        ring[2, (l, a)] = (LASTDIM[a], TALL[a] * 8 * WIDTH[a] * 2)
    arrive, got, steps, now = {}, {}, [], 2.0

    def exchange(layer, t):
        for i, off in jobs_of(layer):
            t += ring[0, i][1] / DRATE
            arrive[i, off] = t + DLAT
            if off == SIZE[UNITS[i][4][0]] // 2:
                push(arrive[i, off], ("start", 0, i, 0, 0))

    def run(until):
        nonlocal now
        taken = []
        while heap and heap[0][0] <= until:
            t, _, ev = heapq.heappop(heap)
            kind, level, key, s, k = ev
            dim, nbytes = ring[level, key]
            h = SIZE[dim] // 2
            if level == 0 and kind == "step" and k < h and arrive[key, s * (h - k)] > t:
                push(arrive[key, s * (h - k)], ev)
                continue
            now = max(now, t)
            taken.append(ev)
            cost = 0.15 + nbytes * (4 + 2 * level) / 7.0e6
            if kind == "end":
                continue
            if kind == "start":
                now += cost
                for s in (1, -1):
                    push(send(now, (dim, s), nbytes // 2), ("step", level, key, s, 1))
            elif k < h:
                now += cost
                push(send(now, (dim, s), nbytes), ("step", level, key, s, k + 1))
            else:
                got[level, key] = got.get((level, key), 0) + 1
                if got[level, key] < 2:
                    continue
                if level == 0:
                    push(now, ("start", 1, key, 0, 0))
                elif level == 1:
                    ka = UNITS[key][:2]
                    if all(got.get((1, i)) == 2 for i, u in enumerate(UNITS) if u[:2] == ka):
                        push(now, ("start", 2, ka, 0, 0))
                else:
                    push(now, ("end", 2, key, 0, 0))
        return taken
    exchange(1, now)
    now = max(now, FIRST)
    for n in TASKS:
        steps.append(run(now))
        now += n * TASK
    exchange(0, now)
    steps.append(run(float("inf")))
    return steps, now, free


FIRST = 6.5


def addsum(dst, srcs):
    def add(*at):
        acc = srcs[0][at].astype(F32)
        for s in srcs[1:]:
            acc = acc + s[at].astype(F32)
        dst[at] = acc.astype(BF)

    if len(dst.shape) == 4:

        def body(i, _):
            add(i)
            return 0
        lax.fori_loop(0, dst.shape[0], body, 0)
    else:
        add(...)


def rs_scratch():
    sh = {}
    sem = pltpu.SemaphoreType.DMA
    for a in "ugd":
        sh["loc_" + a] = pltpu.VMEM((2, 4, 4, TILES[a], 8, WIDTH[a]), BF)
        sh["stage_" + a] = pltpu.VMEM((NB, 4, DEPTH[a], 8, max(u[3] for u in UNITS if u[1] == a)), BF)
        sh["stsem_" + a] = sem((NB,))
        sh["red_" + a] = pltpu.VMEM((2, TALL[a], 8, WIDTH[a]), BF)
        sh["mv_" + a] = pltpu.VMEM((2, 2, 2, ROWS[a], WIDTH[a]), F32)
        sh["w_" + a] = pltpu.VMEM((2, TALL[a], 8, WIDTH[a]), BF)
        h = SIZE[LASTDIM[a]] // 2
        for l in (0, 1):
            sh["slot2_%d%s" % (l, a)] = pltpu.VMEM((2, h, TALL[a], 8, WIDTH[a]), BF)
            sh["first_%d%s" % (l, a)] = pltpu.VMEM((TALL[a], 8, WIDTH[a]), BF)
            for n in "rs":
                sh["%s2_%d%s" % (n, l, a)] = sem((2, h))
    sh["new_d"] = pltpu.VMEM((2, 2, 16, 512), BF)
    for i, u in enumerate(UNITS):
        h = SIZE[u[4][0]] // 2
        sh["slot0_%d" % i] = pltpu.VMEM((2, h) + block_shape(i, 0), BF)
        sh["slot1_%d" % i] = pltpu.VMEM((2, 2) + block_shape(i, 1), BF)
        for n in "rs":
            sh["%s0_%d" % (n, i)] = sem((2, h))
            sh["%s1_%d" % (n, i)] = sem((2, 2))
    sh["ownsem"] = sem((len(UNITS),))
    sh["dh"] = pltpu.VMEM((1024, 1024), BF)
    sh["at"] = pltpu.VMEM((1024, 1024), BF)
    sh["gate"] = pltpu.VMEM((2, 1024, 256), F32)
    sh["up"] = pltpu.VMEM((2, 1024, 256), F32)
    sh["wd"] = pltpu.VMEM((2, 256, 1024), BF)
    sh["ht"] = pltpu.VMEM((2, 256, 1024), BF)
    sh["res_u"] = pltpu.VMEM((2, 4, 4, 8, 8, 256), BF)
    sh["res_g"] = pltpu.VMEM((2, 4, 4, 8, 8, 256), BF)
    sh["res_d"] = pltpu.VMEM((2, 32, 8, 1024), BF)
    sh["insem"] = sem((4, 2))
    sh["outsem"] = sem((3, 2))
    sh["wholesem"] = sem((2,))
    sh["dr"] = sem((64,))
    sh["ds"] = sem((64,))
    sh["ar_z"] = pltpu.VMEM((16, 1, 128), F32)
    sh["ar_p"] = pltpu.VMEM((16, 1, 128), F32)
    sh["arsem"] = sem((4, 16))
    sh["mvsem"] = sem((3, 2, 3))
    sh["wsem"] = sem((3,))
    sh["finsem"] = sem((3, 2, 3))
    sh["newsem"] = sem((3,))
    return sh


def rs_kernel(names, *refs):
    given = {a: refs[j] for j, a in enumerate("ugd")}
    acts = dict(zip(("dh", "at", "gate", "up", "ht"), refs[3:8], strict=True))
    weights = {a: refs[8 + j] for j, a in enumerate("ugd")}
    w_down = refs[11]
    moments = {a: (refs[12 + j], refs[15 + j]) for j, a in enumerate("ugd")}
    new = {a: refs[18 + j] for j, a in enumerate("ugd")}
    new_moments = {a: (refs[21 + j], refs[24 + j]) for j, a in enumerate("ugd")}
    made = {a: refs[27 + j] for j, a in enumerate("ugd")}
    S = dict(zip(names, refs[30:], strict=True))
    at = coords()
    c, x = at["c"], at["x"]
    sib = device({**at, "c": 1 - c})
    steps, _, _ = plan()
    spots, near = places(at)
    windows = [pl.ds(13 * lax.div(v, 4) + 3 * lax.rem(v, 4), 4) for v in spots["z"]]
    zz = lax.rem(at["z"], 4)

    peers = [device({**at, "z": lax.rem(at["z"] + dz, 8), "c": lax.rem(c + dc, 2)}) for dz in range(8) for dc in range(2)][1:]
    peers += [device({**at, "x": lax.rem(at["x"] + dx, 4), "y": lax.rem(at["y"] + dy, 4)}) for dx in range(4) for dy in range(4)][1:]
    bar = pltpu.get_barrier_semaphore()
    for p in peers:
        pl.semaphore_signal(bar, inc=1, device_id=p, device_id_type=MESH)

    def halfcols(a, which):
        w = WIDTH[a]
        return pl.ds(pl.multiple_of((c if which else 1 - c) * w, 128), w)

    def inputs(j, p):
        rows = pl.ds(pl.multiple_of(j * 256, 256), 256)
        pairs = ((acts["gate"].at[j], S["gate"]), (acts["up"].at[j], S["up"]), (w_down.at[0, rows], S["wd"]), (acts["ht"].at[rows], S["ht"]))
        return [pltpu.make_async_copy(src, dst.at[p], S["insem"].at[n, p]) for n, (src, dst) in enumerate(pairs)]

    def outputs(j, p):
        cols = pl.ds(pl.multiple_of(j * 256, 256), 256)
        pairs = [(S["res_" + a].at[p], made[a].at[:, :, :, :, cols], n) for n, a in enumerate("ug")]
        for q in range(4):
            tile = j * 32 + 8 * q
            pairs.append((S["res_d"].at[p, pl.ds(8 * q, 8)], made["d"].at[lax.div(tile, 104), pl.ds(lax.rem(tile, 104), 8)], 2))
        return [pltpu.make_async_copy(src, dst, S["outsem"].at[n, p]) for src, dst, n in pairs]

    def outputs_done(p):
        return [pltpu.make_async_copy(S["res_" + a].at[p], S["res_" + a].at[p], S["outsem"].at[n, p]) for n, a in enumerate("ugd")]
    whole = [pltpu.make_async_copy(acts[n], S[n], S["wholesem"].at[k]) for k, n in enumerate(("dh", "at"))]
    for cp in [*inputs(0, 0), *whole]:
        cp.start()

    moment_copies = []
    for j, a in enumerate("ugd"):
        for q in (0, 1):
            ref = moments[a][q]
            moment_copies.append(pltpu.make_async_copy(ref.at[:, :, halfcols(a, 1)], S["mv_" + a].at[q, c], S["mvsem"].at[j, q, 2]))
        tile = windows[0] if a == "d" else pl.ds(at["z"], 1)
        moment_copies.append(pltpu.make_async_copy(weights[a].at[:, at["x"], at["y"], tile, :, halfcols(a, 1)], S["w_" + a], S["wsem"].at[j]))
    for cp in moment_copies:
        cp.start()
    pl.semaphore_wait(bar, len(peers))
    pend = []

    def remote(make):
        cp = make()
        cp.start()
        pend.append(make)
        return cp
    for j, a in enumerate("ugd"):
        for q in (0, 1):
            moment_copies.append(remote(lambda j=j, a=a, q=q: remote_copy(
                moments[a][q].at[:, :, halfcols(a, 0)], S["mv_" + a].at[q, c], S["mvsem"].at[j, q, 0], S["mvsem"].at[j, q, 1], sib)))

    def region(ref, i, level, v):
        l, a, col, n, o = UNITS[i]
        idx = view(a, o, at, level, v)
        return ref.at[(l, *idx, *([ALL] * (4 - len(idx))), pl.ds(col, n))]

    def pairs(i, off, which, dst):
        l, a, col, n, o = UNITS[i]
        cols = pl.ds(pl.multiple_of((c if which else 1 - c) * WIDTH[a] + col, 128), n)
        v = pos(i, 0, off)
        if a == "d" and not l:
            if o[0] == "x":
                return [(made["d"].at[v, pl.ds(26 * q, 26), :, cols], dst.at[q]) for q in range(4)]
            return [(made["d"].at[:, pl.ds(26 * v, 26), :, cols], dst)]
        idx = view(a, o, at, 0, v)
        return [((given if l else made)[a].at[(*idx, *([ALL] * (4 - len(idx))), cols)], dst)]

    def pos(i, level, off):
        a = UNITS[i][1]
        dim = UNITS[i][4][level] if level < 2 else LASTDIM[a]
        off %= SIZE[dim]
        if level < 2:
            return spots[dim][off]
        return windows[off] if a == "d" else pl.ds(spots[dim][off], 1)

    jobs = {k: n for n, k in enumerate(jobs_of(1) + jobs_of(0))}

    def landing(i, off):
        return region(S["loc_" + UNITS[i][1]], i, 0, pos(i, 0, off))

    def exchange(layer):
        for i, off in jobs_of(layer):
            n = jobs[i, off]
            for src, dst in pairs(i, off, 0, landing(i, off)):
                remote_copy(src, dst, S["ds"].at[n], S["dr"].at[n], sib).start()

    def exchanged(i, off):
        ref = landing(i, off)
        return remote_copy(ref, ref, S["ds"].at[jobs[i, off]], S["dr"].at[jobs[i, off]], sib)
    exchange(1)
    sib_waited = set()

    def wait_terms(i, off):
        off %= SIZE[UNITS[i][4][0]]
        n = SIZE[UNITS[i][4][0]]
        off = off - n if off > n // 2 else off
        if (i, off) not in sib_waited:
            sib_waited.add((i, off))
            exchanged(i, off).wait_recv()

    uses = {a: [] for a in "ugd"}
    for events in steps:
        for kind, level, key, s, k in events:
            if level == 0:
                h = SIZE[UNITS[key][4][0]] // 2
                if kind == "start" or k < h:
                    uses[UNITS[key][1]].append((key, h if kind == "start" else s * (h - k)))
    nth = {a: 0 for a in "ugd"}
    fetched = {a: 0 for a in "ugd"}

    def stage(a, n):
        i = uses[a][n][0]
        return S["stage_" + a].at[n % NB, :, :, :, pl.ds(0, UNITS[i][3])]

    layers = {1}

    def fetch_ahead(a):
        while fetched[a] < min(len(uses[a]), nth[a] + NB):
            n = fetched[a]
            i, off = uses[a][n]
            if UNITS[i][0] not in layers:
                return
            for src, dst in pairs(i, off, 1, stage(a, n)):
                pltpu.make_async_copy(src, dst, S["stsem_" + a].at[n % NB]).start()
            fetched[a] += 1

    own_fetched = set()

    sent = {}

    def own_buffer(i):
        return S["slot0_%d" % i].at[0, 0]

    def fetch_own(i):
        if i not in own_fetched and i in sent:
            sent[i]().wait_send()
            own_fetched.add(i)
            for src, dst in pairs(i, 0, 1, own_buffer(i)):
                pltpu.make_async_copy(src, dst, S["ownsem"].at[i]).start()

    def operands(level, i, off):
        _, a, _, _, o = UNITS[i]
        v = pos(i, level, off)
        here = region(S["loc_" + a], i, level, v)
        if level == 0:
            wait_terms(i, off)
            n = nth[a]
            assert uses[a][n] == (i, off)
            assert fetched[a] > n
            buf = stage(a, n)
            pltpu.make_async_copy(buf, buf, S["stsem_" + a].at[n % NB]).wait()
            nth[a] += 1
            return [buf, here]
        h = SIZE[o[0]] // 2
        first = [own_buffer(i)] + [S["slot0_%d" % i].at[d, h - 1] for d in (0, 1)]
        if level == 1:
            return [here] + [f.at[v] for f in first]
        w = pos(i, 1, 0)
        return [here] + [f.at[w, v] for f in first] + [S["slot1_%d" % i].at[d, 1, v] for d in (0, 1)]

    def half(ref, which, level, a):
        if level == 2 and TALL[a] == 1:
            return ref.at[..., pl.ds(896, 768) if which else pl.ds(0, 896)]
        n = ref.shape[0] // 2
        return ref.at[pl.ds(n * which, n)]

    def parts(key):
        r = []
        for i, u in enumerate(UNITS):
            if u[:2] == key:
                for lo, hi in ((0, 896), (896, 1664)):
                    a, b = max(lo, u[2]), min(hi, u[2] + u[3])
                    if a < b:
                        r.append((i, pl.ds(a - u[2], b - a), pl.ds(a, b - a), lo > 0))
        return r

    def cut(ref, cs):
        return ref.at[..., cs]

    def event(ev):
        kind, level, key, s, k = ev
        l, a = UNITS[key][:2] if level < 2 else key
        tag = "%d" % key if level < 2 else "%d%s" % key
        dim = UNITS[key][4][level] if level < 2 else LASTDIM[a]
        h = SIZE[dim] // 2
        if kind == "end":
            finish(l, a)
            return
        slot, rsem, ssem = (S["%s%d_%s" % (n, level, tag)] for n in ("slot", "r", "s"))

        def send(src, d, k):
            dst = lambda: slot.at[d, k] if k else half(slot.at[d, 0], d, level, a)
            remote(lambda: remote_copy(src(), dst(), ssem.at[d, k], rsem.at[d, k], near[dim, 1 - 2 * d]))

        if kind == "start":
            if level == 1:
                wait_terms(key, 0)
                fetch_own(key)
                assert key in own_fetched
                pltpu.make_async_copy(own_buffer(key), own_buffer(key), S["ownsem"].at[key]).wait()
            dst = (lambda: S["first_" + tag]) if level == 2 else (lambda: region(S["loc_" + a], key, level, pos(key, level, h)))
            if level < 2:
                addsum(dst(), operands(level, key, h))
            else:
                for i, uc, sc, _ in parts(key):
                    addsum(cut(dst(), sc), [cut(o, uc) for o in operands(level, i, h)])
            for d in (0, 1):
                send(lambda d=d: half(dst(), d, level, a), d, 0)
            if level == 0:
                fetch_own(key)
                fetch_ahead(a)
            return
        d = 0 if s > 0 else 1
        block = slot.at[d, k - 1]
        got = half(block, d, level, a) if k == 1 else block
        remote_copy(got, got, ssem.at[d, k - 1], rsem.at[d, k - 1], sib).wait_recv()
        if k == h:
            if level == 0:
                fetch_own(key)
            return
        off = s * (h - k)
        if level < 2:
            ops = operands(level, key, off)
            if k > 1:
                addsum(block, [block] + ops)
            else:
                for w in (0, 1):
                    hm = half(block, w, level, a)
                    addsum(hm, ([hm] if w == d else []) + [half(r, w, level, a) for r in ops])
        else:
            for i, uc, sc, w in parts(key):
                ops = [cut(o, uc) for o in operands(level, i, off)]
                m = cut(block, sc)
                if k > 1:
                    addsum(m, [m] + ops)
                elif TALL[a] == 1:
                    addsum(m, ([m] if w == (d == 1) else []) + ops)
                else:
                    for w in (0, 1):
                        hm = half(m, w, level, a)
                        addsum(hm, ([hm] if w == d else []) + [half(r, w, level, a) for r in ops])
        send(lambda: slot.at[d, k - 1], d, k)
        if (level, d, k) == (0, 0, 1):
            sent[key] = pend.pop()
        if level == 0:
            fetch_ahead(a)

    def finish(l, a):
        h = SIZE[LASTDIM[a]] // 2
        for i, uc, sc, _ in parts((l, a)):
            ops = [cut(o, uc) for o in operands(2, i, 0)] + [cut(S["slot2_%d%s" % (l, a)].at[d, h - 1], sc) for d in (0, 1)]
            addsum(cut(S["red_" + a].at[l], sc), ops)

    for a in "ugd":
        fetch_ahead(a)
    first = 0
    for n, events in zip(TASKS, steps, strict=False):
        for ev in events:
            event(ev)
        if not first:
            for cp in whole:
                cp.wait()

        def task(j, _):
            p = lax.rem(j, 2)
            for cp in inputs(j, p):
                cp.wait()

            @pl.when(j < 12)
            def _():
                for cp in inputs(j + 1, 1 - p):
                    cp.start()

            @pl.when(j >= 2)
            def _():
                for cp in outputs_done(p):
                    cp.wait()
            dh = dot(S["dh"][...], S["wd"][p], NT).astype(BF).astype(F32)
            _, dgate, dup = silu_back(S["gate"][p], S["up"][p], dh)
            S["res_u"][p] = dot(S["at"][...], dup).reshape(4, 4, 8, 8, 256).astype(BF)
            S["res_g"][p] = dot(S["at"][...], dgate).reshape(4, 4, 8, 8, 256).astype(BF)
            S["res_d"][p] = dot(S["ht"][p], S["dh"][...]).reshape(32, 8, 1024).astype(BF)
            for cp in outputs(j, p):
                cp.start()
            return 0
        lax.fori_loop(first, first + n, task, 0)
        first += n
    for p in (1, 0):
        for cp in outputs_done(p):
            cp.wait()
    exchange(0)
    layers.add(0)
    for a in "ugd":
        fetch_ahead(a)
    for ev in steps[-1]:
        event(ev)
    for i, off in jobs:
        exchanged(i, off).wait_send()
        wait_terms(i, off)

    total = jnp.zeros((8, 128), F32)
    for a in "ugd":
        for l in (0, 1):
            for t in range(TALL[a]):
                for q in range(WIDTH[a] // 128):
                    g = S["red_" + a][l, t, :, q * 128:q * 128 + 128].astype(F32)
                    if a == "d":
                        row = lax.broadcasted_iota(jnp.int32, (8, 128), 0) + 8 * t
                        g = jnp.where((row >= 2 * zz) & (row < 2 * zz + 26), g, 0.0)
                    total = total + g * g
    total = jnp.sum(total, axis=0, keepdims=True)
    for r, (buf, ds) in enumerate(((S["ar_z"], [(0, 0, q // 2, q % 2) for q in range(16)]), (S["ar_p"], [(q // 4, q % 4, 0, 0) for q in range(16)]))):
        buf[0] = total
        cps = []
        for q in range(1, 16):
            dx, dy, dz, dc = ds[q]
            to = device({"x": lax.rem(at["x"] + dx, 4), "y": lax.rem(at["y"] + dy, 4), "z": lax.rem(at["z"] + dz, 8), "c": lax.rem(c + dc, 2)})
            cps.append(remote(lambda q=q, to=to: remote_copy(buf.at[0], buf.at[q], S["arsem"].at[2 * r, q], S["arsem"].at[2 * r + 1, q], to)))
        for cp in cps:
            cp.wait_recv()
            cp.wait_send()
            pend.pop()
        total = buf[0]
        for q in range(1, 16):
            total = total + buf[q]
    mean = jnp.sum(total, axis=1, keepdims=True) / COUNT
    factor = jnp.minimum(1.0, 0.5 * lax.rsqrt(mean + 1e-30))
    for cp in moment_copies:
        cp.wait_recv() if cp.is_remote else cp.wait()

    def adamw(w, m, v, g):
        g = g * factor
        m = 0.9 * m + 0.1 * g
        v = 0.95 * v + 0.05 * g * g
        step = m * lax.rsqrt(v + 1e-8) + 0.1 * w
        return (w - 0.02 * step).astype(BF), m, v

    for a in "ug":
        mv, red, wv = S["mv_" + a], S["red_" + a], S["w_" + a]

        def body(q, _, mv=mv, red=red, wv=wv, a=a):
            cs = pl.ds(pl.multiple_of(q * 128, 128), 128)
            for l in (0, 1):
                m, v = (jnp.concatenate([mv[e, 0, l, :, cs], mv[e, 1, l, :, cs]], axis=0) for e in (0, 1))
                n, m, v = adamw(wv[l, 0, :, cs].astype(F32), m, v, red[l, 0, :, cs].astype(F32))
                wv[l, 0, :, cs] = n
                for e, t in enumerate((m, v)):
                    for s in (0, 1):
                        mv[e, s, l, :, cs] = t[4 * s:4 * s + 4]
            return 0
        lax.fori_loop(0, 13, body, 0)
    row = lax.broadcasted_iota(jnp.int32, (32, 32), 0)
    column = lax.broadcasted_iota(jnp.int32, (32, 32), 1)
    pick = (column == 2 * zz + 13 * (row >> 4) + (row & 15)) & ((row & 15) < 13)
    pick = jnp.where(pick, 1.0, 0.0).astype(BF)
    for l in (0, 1):
        gd, wd = (jnp.dot(pick, S[n][l].reshape(32, 512), preferred_element_type=F32) for n in ("red_d", "w_d"))
        for s in (0, 1):
            rows = slice(16 * s, 16 * s + 16)
            n, m, v = adamw(wd[rows], S["mv_d"][0, s, l], S["mv_d"][1, s, l], gd[rows])
            S["new_d"][l, s] = n
            S["mv_d"][0, s, l] = m
            S["mv_d"][1, s, l] = v
    ends = []
    for j, a in enumerate("ugd"):
        cp = pltpu.make_async_copy(S["new_d"] if a == "d" else S["w_" + a].at[:, 0], new[a], S["newsem"].at[j])
        cp.start()
        ends.append(cp.wait)
        for q in (0, 1):
            out = new_moments[a][q].at[:, :, halfcols(a, 1)]
            cp = remote_copy(S["mv_" + a].at[q, 1 - c], out, S["finsem"].at[j, q, 0], S["finsem"].at[j, q, 1], sib)
            cp.start()
            back = remote_copy(S["mv_" + a].at[q, 1 - c], new_moments[a][q].at[:, :, halfcols(a, 0)], S["finsem"].at[j, q, 0], S["finsem"].at[j, q, 1], sib)
            ends += [cp.wait_send, back.wait_recv]
            cp = pltpu.make_async_copy(S["mv_" + a].at[q, c], out, S["finsem"].at[j, q, 2])
            cp.start()
            ends.append(cp.wait)
    for wait in ends:
        wait()
    for make in pend:
        make().wait_send()


def reduce_scatter(grads, acts, weights, w_down, m, v):
    args = [g.reshape(4, 4, -1, 8, g.shape[-1]) for g in grads] + list(acts)
    args += [w.reshape(2, 4, 4, -1, 8, w.shape[-1]) for w in weights] + [w_down, *m, *v]
    sh = rs_scratch()
    any_ = pl.BlockSpec(memory_space=pl.ANY)
    outs = [jax.ShapeDtypeStruct(s, BF) for s in ((2, 8, 1664), (2, 8, 1664), (2, 2, 16, 512))] + [jax.ShapeDtypeStruct(t.shape, F32) for t in (*m, *v)]
    outs += [jax.ShapeDtypeStruct(s, BF) for s in ((4, 4, 8, 8, 3328), (4, 4, 8, 8, 3328), (4, 104, 8, 1024))]
    outs = pl.pallas_call(
        functools.partial(rs_kernel, list(sh)), out_shape=outs, in_specs=[any_] * 18, out_specs=[any_] * 12, scratch_shapes=list(sh.values()), name="reduce_scatter",
        compiler_params=pltpu.CompilerParams(collective_id=0, has_side_effects=True, vmem_limit_bytes=VMEM_BYTES))(*args)
    return outs[:3], outs[3:6], outs[6:9]


def plan_ag():
    RATE, LAT = 46.0e3, 2.9
    free, heap, order, seq, got, now = {}, [], [], [0], {}, 1.0

    def push(t, ev):
        seq[0] += 1
        heapq.heappush(heap, (t, seq[0], ev))

    def send(t, link, nbytes):
        free[link] = max(free.get(link, 0.0), t) + nbytes / RATE
        return free[link] + LAT
    ring = {(2, a): (LASTDIM[a], {"u": 8 * 1664, "g": 8 * 1664, "d": 32 * 512}[a] * 4) for a in "ugd"}
    for i, (_, a, _, cols, o) in enumerate(UNITS):
        ring[1, i] = (o[1], DEPTH[a] * 8 * cols * 2)
        ring[0, i] = (o[0], 4 * DEPTH[a] * 8 * cols * 2)
    for a in "gdu":
        push(1.0, ("start", 2, a, 0, 0))
    while heap:
        t, _, ev = heapq.heappop(heap)
        kind, level, key, s, k = ev
        dim, nbytes = ring[level, key]
        h = SIZE[dim] // 2
        now = max(now, t) + 0.1
        order.append(ev)
        if kind == "start":
            for s in (1, -1):
                push(send(now, (dim, s), nbytes), ("step", level, key, s, 1))
            continue
        if k < h:
            push(send(now, (dim, s), nbytes if k < h - 1 else nbytes // 2), ("step", level, key, s, k + 1))
            continue
        got[level, key] = got.get((level, key), 0) + 1
        if got[level, key] < 2:
            continue
        if level == 2:
            for i, u in enumerate(UNITS):
                if u[1] == key:
                    push(now + (1.0 if key == "d" else 0), ("start", 1, i, 0, 0))
        elif level == 1:
            push(now, ("start", 0, key, 0, 0))
    return order, now, free


def ag_scratch():
    sem = pltpu.SemaphoreType.DMA
    sh = {"pc": pltpu.VMEM((8, 2, 2, 16, 512), BF), "asm": pltpu.VMEM((2, 26, 8, 512), BF), "loc": sem((4,)), "sr": sem((128,)), "ss": sem((128,))}
    for n in "rs":
        for a in "ugd":
            sh["%s2_%s" % (n, a)] = sem((2, SIZE[LASTDIM[a]] // 2))
        for i, u in enumerate(UNITS):
            for lv in (0, 1):
                sh["%s%d_%d" % (n, lv, i)] = sem((2, SIZE[u[4][lv]] // 2))
    return sh


def ag_kernel(names, *refs):
    own = {a: refs[j] for j, a in enumerate("ugd")}
    out = {a: refs[3 + j] for j, a in enumerate("ugd")}
    S = dict(zip(names, refs[6:], strict=True))
    at = coords()
    c, x, y, z = at["c"], at["x"], at["y"], at["z"]
    sib = device({**at, "c": 1 - c})
    order, _, _ = plan_ag()
    spots, near = places(at)
    peers = [sib, *near.values()]
    bar = pltpu.get_barrier_semaphore()
    for p in peers:
        pl.semaphore_signal(bar, inc=1, device_id=p, device_id_type=MESH)

    def hc(a, col=0, n=None):
        return pl.ds(pl.multiple_of(c * WIDTH[a] + col, 128), WIDTH[a] if n is None else n)
    local = [pltpu.make_async_copy(own["u"], out["u"].at[:, x, y, z, :, hc("u")], S["loc"].at[0]),
             pltpu.make_async_copy(own["g"], out["g"].at[:, x, y, z, :, hc("g")], S["loc"].at[1]),
             pltpu.make_async_copy(own["d"], S["pc"].at[z], S["loc"].at[2])]
    for cp in local:
        cp.start()
    pl.semaphore_wait(bar, len(peers))
    for cp in local:
        cp.wait()
    pend, twin = [], []

    def remote(src, ss, rs, to):
        cp = remote_copy(src, src, ss, rs, to)
        cp.start()
        pend.append(cp)

    def to_sibling(ref):
        n = len(twin)
        remote(ref, S["ss"].at[n], S["sr"].at[n], sib)
        twin.append(ref)

    def region(level, key, v):
        if level == 2:
            if key == "d":
                return S["pc"].at[v]
            return out["u"].at[:, x, v, z, :, hc("u")] if key == "u" else out["g"].at[:, x, y, v, :, hc("g")]
        l, a, col, n, o = UNITS[key]
        idx = view(a, o, at, level, v)
        return out[a].at[(l, *idx, *([ALL] * (4 - len(idx))), hc(a, col, n))]

    def half(ref, which):
        n = ref.shape[0] // 2
        return ref.at[pl.ds(n * which, n)]

    got = {}
    for kind, level, key, s, k in order:
        dim = UNITS[key][4][level] if level < 2 else LASTDIM[key]
        n = SIZE[dim]
        h = n // 2
        rsem, ssem = S["r%d_%s" % (level, key)], S["s%d_%s" % (level, key)]

        def send(src, d, k, dim=dim, rsem=rsem, ssem=ssem):
            remote(src, ssem.at[d, k], rsem.at[d, k], near[dim, 1 - 2 * d])

        if kind == "start":
            for d in (0, 1):
                send(region(level, key, at[dim]), d, 0)
            continue
        d = 0 if s > 0 else 1
        block = region(level, key, spots[dim][-s * k % n])
        if k == h:
            block = half(block, d)
        remote_copy(block, block, ssem.at[d, k - 1], rsem.at[d, k - 1], sib).wait_recv()
        if k < h - 1:
            send(block, d, k)
        elif k == h - 1:
            send(half(block, d), d, k)
        if level < 2:
            to_sibling(block)
        if k == h:
            got[level, key] = got.get((level, key), 0) + 1
            if level == 2 and got[level, key] == 2:
                if key == "d":
                    q = lax.broadcasted_iota(jnp.int32, (208, 256), 1)
                    r = lax.broadcasted_iota(jnp.int32, (208, 256), 0)
                    e = q & 15
                    pick = (r == 26 * (q >> 5) + 13 * ((q >> 4) & 1) + e) & (e < 13)
                    pick = jnp.where(pick, 1.0, 0.0).astype(BF)
                    for l in (0, 1):
                        rows = jnp.dot(pick, S["pc"][:, l].reshape(256, 512), preferred_element_type=F32)
                        S["asm"][l] = rows.reshape(26, 8, 512).astype(BF)
                    cp = pltpu.make_async_copy(S["asm"], out["d"].at[:, x, y, :, :, hc("d")], S["loc"].at[3])
                    cp.start()
                    cp.wait()
                idx = (ALL, x, ALL, z, ALL) if key == "u" else (ALL, x, y, ALL, ALL)
                to_sibling(out[key].at[(*idx, hc(key))])
    for n, ref in enumerate(twin):
        remote_copy(ref, ref, S["ss"].at[n], S["sr"].at[n], sib).wait_recv()
    for cp in pend:
        cp.wait_send()


def all_gather(u, g, d):
    sh = ag_scratch()
    any_ = pl.BlockSpec(memory_space=pl.ANY)
    outs = [jax.ShapeDtypeStruct((2, 4, 4, TILES[a], 8, 2 * WIDTH[a]), BF) for a in "ugd"]
    return pl.pallas_call(
        functools.partial(ag_kernel, list(sh)), out_shape=outs, in_specs=[any_] * 3, out_specs=[any_] * 3, scratch_shapes=list(sh.values()), name="all_gather",
        compiler_params=pltpu.CompilerParams(collective_id=1, has_side_effects=True, vmem_limit_bytes=VMEM_BYTES))(u, g, d)


def solution(mesh):
    def step(x, dy, w_gate, w_up, w_down, *moments):
        x, dy = x[0], dy[0]
        gate0, up0, hid0, h1, a0 = layer0(x, w_gate, w_up, w_down)
        down1, gate1, up1, dh1 = layer1(h1, dy, w_gate, w_up, w_down)
        m, v = moments[:3], moments[3:]
        order = lambda t: (t[1], t[0], t[2])
        pad = lambda t: (*t[:2], jnp.pad(t[2], ((0, 0), (0, 3), (0, 0))))
        acts = (dh1, a0, gate0, up0, hid0)
        new, m, v = reduce_scatter((up1, gate1, down1), acts, order((w_gate, w_up, w_down)), w_down, pad(order(m)), pad(order(v)))
        u, g, d = all_gather(*new)
        w = (g.reshape(w_gate.shape), u.reshape(w_up.shape), d.reshape(w_down.shape))
        cut = lambda t: (t[1], t[0], t[2][:, :13])
        return (*w, *cut(m), *cut(v))

    data, whole, rows = P(("rep", "dp"), None, None), P(), P(None, "dp", None)
    out = P("rep", None, None)
    return jax.shard_map(step, mesh=mesh, in_specs=(data, data) + (whole,) * 3 + (rows,) * 6, out_specs=(out,) * 3 + (P("rep", "dp", None),) * 6, check_vma=False)
```

```python
import functools
import heapq

import jax
import jax.numpy as jnp
from jax import lax
from jax.experimental import pallas as pl
from jax.experimental.pallas import tpu as pltpu
from jax.sharding import PartitionSpec as P

MESH = pl.DeviceIdType.MESH
BF, F32 = jnp.bfloat16, jnp.float32
SIZE = {"x": 4, "y": 4, "z": 8}
VMEM_BYTES = 67043328
AG_VMEM = 4 * 2**20
ALL = slice(None)


def coords():
    i = lax.axis_index("dp")
    return {"x": i // 64, "y": lax.rem(i // 16, 4), "z": lax.rem(i // 2, 8), "c": lax.rem(i, 2)}


def device(at):
    return {"dp": ((at["x"] * 4 + at["y"]) * 8 + at["z"]) * 2 + at["c"]}


def places(at):
    spots = {d: [at[d]] + [lax.rem(at[d] + k, n) for k in range(1, n)] for d, n in SIZE.items()}
    return spots, {(d, s): device({**at, d: spots[d][s]}) for d in SIZE for s in (1, -1)}


UNITS = [
    (1, "d", 0, 256, "xyz"), (1, "d", 256, 256, "yxz"), (1, "u", 0, 896, "zxy"), (1, "u", 896, 768, "zxy"), (1, "g", 0, 896, "xyz"), (1, "g", 896, 768, "yxz"),
    (0, "d", 0, 256, "xyz"), (0, "d", 256, 256, "yxz"), (0, "u", 0, 896, "zxy"), (0, "u", 896, 768, "zxy"), (0, "g", 0, 896, "yxz"), (0, "g", 896, 768, "xyz"),
]
DEPTH = {"u": 4, "g": 8, "d": 26}
TILES = {"u": 8, "g": 8, "d": 26}
WIDTH = {"u": 1664, "g": 1664, "d": 512}
TALL = {"u": 1, "g": 1, "d": 4}
LASTDIM = {"u": "y", "g": "z", "d": "z"}
ROWS = {"u": 4, "g": 4, "d": 16}
COUNT = 2 * 3 * 1024 * 3328
NB = 2


def view(a, order, at, level, v):
    if level == 0:
        return {"z": (ALL, ALL, v), "x": (v,), "y": (ALL, v)}[order[0]]
    if level == 1:
        return {"zxy": (v, ALL, at["z"]), "xyz": (at["x"], v), "yxz": (v, at["y"])}[order]
    return (at["x"], v, at["z"]) if a == "u" else (at["x"], at["y"], v)


def block_shape(i, level):
    _, a, _, cols, _ = UNITS[i]
    return ((4, DEPTH[a], 8, cols), (DEPTH[a], 8, cols))[level]


def remote_copy(src, dst, ss, rs, to):
    return pltpu.make_async_remote_copy(src_ref=src, dst_ref=dst, send_sem=ss, recv_sem=rs, device_id=to, device_id_type=MESH)


T = 1024
B = 256
N = 3328 // B
NT = (((1,), (1,)), ((), ()))


def dot(a, b, dims=(((1,), (0,)), ((), ()))):
    return lax.dot_general(a, b, dims, preferred_element_type=F32)


def norm_scale(wide):
    return lax.rsqrt(jnp.mean(wide**2, -1, keepdims=True) + 1e-6)


def rowwise(n, body, step=128):
    def one(i, _):
        body(pl.ds(pl.multiple_of(i * step, step), step))
        return 0
    lax.fori_loop(0, n // step, one, 0)


def silu_back(g, u, dh):
    s = jax.nn.sigmoid(g)
    silu = g * s
    return silu, (dh * u * (s + silu * (1.0 - s))).astype(BF), (dh * silu).astype(BF)


def norm_into(h, a):
    def norm(rows):
        wide = h[rows].astype(F32)
        a[rows] = (wide * norm_scale(wide)).astype(BF)
    rowwise(T, norm)


def pipelined(chunk, first, second):
    held = None
    for m in range(0, T, chunk):
        rows = slice(m, m + chunk)
        now = first(rows)
        if held is not None:
            second(*held)
        held = rows, now
    second(*held)


def fwd0(C, tr, x, wg, wu, wd, gate, up, ht, h1, at, a, hid):
    j = pl.program_id(0)

    @pl.when(j == 0)
    def _():
        norm_into(x, a)
        at[...] = a[...].T if tr else a[...]

    @pl.when(j < N)
    def _():
        def first(rows):
            return dot(a[rows], wg[...]), dot(a[rows], wu[...])

        def second(rows, gu):
            g, u = gu
            gate[rows] = g
            up[rows] = u
            v = (g * jax.nn.sigmoid(g) * u).astype(BF)
            hid[j, rows] = v
            if tr:
                ht[:, rows] = v.T
            else:
                ht[rows] = v
        pipelined(C, first, second)

    @pl.when(j >= N)
    def _():
        def first(rows):
            return sum(dot(hid[i, rows], wd[i * B:i * B + B]) for i in range(N))

        def second(rows, y):
            n = pl.ds(pl.multiple_of((j - N) * B, B), B)
            h1[rows] = (x[rows, n].astype(F32) + y.astype(BF).astype(F32)).astype(BF)
        pipelined(C, first, second)


def layer0(x, w_gate, w_up, w_down, C=512, tr=True):
    whole = pl.BlockSpec((T, T), lambda j: (0, 0))
    cap = lambda j: jnp.minimum(j, N - 1)
    cols = pl.BlockSpec((T, B), lambda j: (0, cap(j)))
    wcols = pl.BlockSpec((None, T, B), lambda j: (0, 0, cap(j)))
    late = lambda j: jnp.maximum(j - N, 0)
    wrows = pl.BlockSpec((None, 3328, B), lambda j: (0, 0, late(j)))
    rows = pl.BlockSpec((B, T), lambda j: (cap(j), 0)) if tr else cols
    o = jax.ShapeDtypeStruct
    blk = pl.BlockSpec((None, T, B), lambda j: (cap(j), 0, 0))
    return pl.pallas_call(functools.partial(fwd0, C, tr), grid=(N + 4,), in_specs=[whole, wcols, wcols, wrows],
        out_specs=[blk, blk, rows, pl.BlockSpec((T, B), lambda j: (0, late(j))), whole],
        out_shape=[o((N, T, B), F32)] * 2 + [o((3328, T) if tr else (T, 3328), BF), o((T, T), BF), o((T, T), BF)],
        scratch_shapes=[pltpu.VMEM((T, T), BF), pltpu.VMEM((N, T, B), BF)], name="layer0",
        compiler_params=pltpu.CompilerParams(vmem_limit_bytes=VMEM_BYTES))(x, w_gate, w_up, w_down)


def both1(h, dy, wg, wu, wd, wg2, wu2, dwd, dwg, dwu, dh1, a, at, gs, us, hta, htb, acc):
    j = pl.program_id(0)

    @pl.when(j == 0)
    def _():
        norm_into(h, a)
        at[...] = a[...].T

    def now():
        return dot(a[...], wg[...]), dot(a[...], wu[...]), dot(dy[...], wd[...], NT)

    def before(ht):
        dwd[...] = dot(ht[...], dy[...]).astype(BF)
        dwg[...] = dot(at[...], gs[j - 1]).astype(BF)
        dwu[...] = dot(at[...], us[j - 1]).astype(BF)

    def then(g, u, dh, ht):
        silu, dgate, dup = silu_back(g, u, dh.astype(BF).astype(F32))
        gs[j] = dgate
        us[j] = dup
        ht[...] = (silu * u).astype(BF).T

    @pl.when(j == 0)
    def _():
        then(*now(), hta)

    for p, (mine, last) in enumerate(((hta, htb), (htb, hta))):
        @pl.when((j > 0) & (j < N) & (lax.rem(j, 2) == p))
        def _():
            x = now()
            before(last)
            then(*x, mine)

    @pl.when(j == N)
    def _():
        before(hta)

    @pl.when(j >= N)
    def _():
        y = sum(dot(gs[i], wg2[:, i * B:i * B + B], NT) + dot(us[i], wu2[:, i * B:i * B + B], NT) for i in range(N))
        acc[:, pl.ds(pl.multiple_of((j - N) * B, B), B)] = y

    @pl.when(j == N + 3)
    def _():
        def back(rows):
            wide = h[rows].astype(F32)
            scale = norm_scale(wide)
            d = acc[rows].astype(BF).astype(F32)
            d = d * scale - wide * (scale * scale * scale * jnp.mean(d * wide, -1, keepdims=True))
            dh1[rows] = (dy[rows].astype(F32) + d.astype(BF).astype(F32)).astype(BF)
        rowwise(T, back)


def layer1(h, dy, w_gate, w_up, w_down):
    cap = lambda j: jnp.minimum(j, N - 1)
    prev = lambda j: jnp.clip(j - 1, 0, N - 1)
    late = lambda j: jnp.maximum(j - N, 0)
    whole = pl.BlockSpec((T, T), lambda j: (0, 0))
    cols = pl.BlockSpec((T, B), lambda j: (0, prev(j)))
    wcols = pl.BlockSpec((None, T, B), lambda j: (1, 0, cap(j)))
    wrows = pl.BlockSpec((None, B, T), lambda j: (1, cap(j), 0))
    wtall = pl.BlockSpec((None, B, 3328), lambda j: (1, late(j), 0))
    rows = pl.BlockSpec((B, T), lambda j: (prev(j), 0))
    o = jax.ShapeDtypeStruct
    return pl.pallas_call(both1, grid=(N + 4,), in_specs=[whole, whole, wcols, wcols, wrows, wtall, wtall], out_specs=[rows, cols, cols, whole],
        out_shape=[o((3328, T), BF)] + [o((T, 3328), BF)] * 2 + [o((T, T), BF)],
        scratch_shapes=[pltpu.VMEM((T, T), BF)] * 2 + [pltpu.VMEM((N, T, B), BF)] * 2 + [pltpu.VMEM((B, T), BF)] * 2 + [pltpu.VMEM((T, T), F32)], name="layer1",
        compiler_params=pltpu.CompilerParams(vmem_limit_bytes=VMEM_BYTES))(h, dy, w_gate, w_up, w_down, w_gate, w_up)


TASKS = (3, 3, 3, 4)


def jobs_of(layer):
    rank = {}
    for i, u in enumerate(UNITS):
        if u[0] == layer:
            n = SIZE[u[4][0]]
            h = n // 2
            for at, off in enumerate([h] + [s * (h - k) for k in range(1, h) for s in (1, -1)] + [0]):
                rank[i, off] = (at / n, i)
    return sorted(rank, key=rank.get)


def plan():
    RATE, LAT, TASK, DRATE, DLAT = 46.0e3, 3.0, 2.7, 600.0e3, 2.0
    free, heap, seq = {}, [], [0]

    def send(t, link, nbytes):
        free[link] = max(free.get(link, 0.0), t) + nbytes / RATE
        return free[link] + LAT

    def push(t, ev):
        seq[0] += 1
        heapq.heappush(heap, (t, seq[0], ev))
    ring = {}
    for i, (l, a, _, cols, o) in enumerate(UNITS):
        ring[0, i] = (o[0], 4 * DEPTH[a] * 8 * cols * 2)
        ring[1, i] = (o[1], DEPTH[a] * 8 * cols * 2)
        ring[2, (l, a)] = (LASTDIM[a], TALL[a] * 8 * WIDTH[a] * 2)
    arrive, got, steps, now = {}, {}, [], 2.0

    def exchange(layer, t):
        for i, off in jobs_of(layer):
            t += ring[0, i][1] / DRATE
            arrive[i, off] = t + DLAT
            if off == SIZE[UNITS[i][4][0]] // 2:
                push(arrive[i, off], ("start", 0, i, 0, 0))

    def run(until):
        nonlocal now
        taken = []
        while heap and heap[0][0] <= until:
            t, _, ev = heapq.heappop(heap)
            kind, level, key, s, k = ev
            dim, nbytes = ring[level, key]
            h = SIZE[dim] // 2
            if level == 0 and kind == "step" and k < h and arrive[key, s * (h - k)] > t:
                push(arrive[key, s * (h - k)], ev)
                continue
            now = max(now, t)
            taken.append(ev)
            cost = 0.15 + nbytes * (4 + 2 * level) / 7.0e6
            if kind == "end":
                continue
            if kind == "start":
                now += cost
                for s in (1, -1):
                    push(send(now, (dim, s), nbytes // 2), ("step", level, key, s, 1))
            elif k < h:
                now += cost
                push(send(now, (dim, s), nbytes), ("step", level, key, s, k + 1))
            else:
                got[level, key] = got.get((level, key), 0) + 1
                if got[level, key] < 2:
                    continue
                if level == 0:
                    push(now, ("start", 1, key, 0, 0))
                elif level == 1:
                    ka = UNITS[key][:2]
                    if all(got.get((1, i)) == 2 for i, u in enumerate(UNITS) if u[:2] == ka):
                        push(now, ("start", 2, ka, 0, 0))
                else:
                    push(now, ("end", 2, key, 0, 0))
        return taken
    exchange(1, now)
    now = max(now, FIRST)
    for n in TASKS:
        steps.append(run(now))
        now += n * TASK
    exchange(0, now)
    steps.append(run(float("inf")))
    return steps, now, free


FIRST = 3.0


def addsum(dst, srcs):
    def add(*at):
        acc = srcs[0][at].astype(F32)
        for s in srcs[1:]:
            acc = acc + s[at].astype(F32)
        dst[at] = acc.astype(BF)

    if len(dst.shape) == 4:

        def body(i, _):
            add(i)
            return 0
        lax.fori_loop(0, dst.shape[0], body, 0)
    else:
        add(...)


def rs_scratch():
    sh = {}
    sem = pltpu.SemaphoreType.DMA
    for a in "ugd":
        sh["loc_" + a] = pltpu.VMEM((2, 4, 4, TILES[a], 8, WIDTH[a]), BF)
        sh["stage_" + a] = pltpu.VMEM((NB, 4, DEPTH[a], 8, max(u[3] for u in UNITS if u[1] == a)), BF)
        sh["stsem_" + a] = sem((NB,))
        sh["red_" + a] = pltpu.VMEM((2, TALL[a], 8, WIDTH[a]), BF)
        sh["mv_" + a] = pltpu.VMEM((2, 2, 2, ROWS[a], WIDTH[a]), F32)
        sh["w_" + a] = pltpu.VMEM((2, TALL[a], 8, WIDTH[a]), BF)
        h = SIZE[LASTDIM[a]] // 2
        for l in (0, 1):
            sh["slot2_%d%s" % (l, a)] = pltpu.VMEM((2, h, TALL[a], 8, WIDTH[a]), BF)
            sh["first_%d%s" % (l, a)] = pltpu.VMEM((TALL[a], 8, WIDTH[a]), BF)
            for n in "rs":
                sh["%s2_%d%s" % (n, l, a)] = sem((2, h))
    sh["new_d"] = pltpu.VMEM((2, 2, 16, 512), BF)
    for i, u in enumerate(UNITS):
        h = SIZE[u[4][0]] // 2
        sh["slot0_%d" % i] = pltpu.VMEM((2, h) + block_shape(i, 0), BF)
        sh["slot1_%d" % i] = pltpu.VMEM((2, 2) + block_shape(i, 1), BF)
        for n in "rs":
            sh["%s0_%d" % (n, i)] = sem((2, h))
            sh["%s1_%d" % (n, i)] = sem((2, 2))
    sh["ownsem"] = sem((len(UNITS),))
    sh["dh"] = pltpu.VMEM((1024, 1024), BF)
    sh["at"] = pltpu.VMEM((1024, 1024), BF)
    sh["gate"] = pltpu.VMEM((2, 1024, 256), F32)
    sh["up"] = pltpu.VMEM((2, 1024, 256), F32)
    sh["wd"] = pltpu.VMEM((2, 256, 1024), BF)
    sh["ht"] = pltpu.VMEM((2, 256, 1024), BF)
    sh["res_u"] = pltpu.VMEM((2, 4, 4, 8, 8, 256), BF)
    sh["res_g"] = pltpu.VMEM((2, 4, 4, 8, 8, 256), BF)
    sh["res_d"] = pltpu.VMEM((2, 32, 8, 1024), BF)
    sh["insem"] = sem((4, 2))
    sh["outsem"] = sem((3, 2))
    sh["wholesem"] = sem((2,))
    sh["dr"] = sem((64,))
    sh["ds"] = sem((64,))
    sh["ar_z"] = pltpu.VMEM((16, 1, 128), F32)
    sh["ar_p"] = pltpu.VMEM((16, 1, 128), F32)
    sh["arsem"] = sem((4, 16))
    sh["mvsem"] = sem((3, 2, 3))
    sh["wsem"] = sem((3,))
    sh["finsem"] = sem((3, 2, 3))
    sh["newsem"] = sem((3,))
    return sh


def rs_kernel(names, *refs):
    given = {a: refs[j] for j, a in enumerate("ugd")}
    acts = dict(zip(("dh", "at", "gate", "up", "ht"), refs[3:8], strict=True))
    weights = {a: refs[8 + j] for j, a in enumerate("ugd")}
    w_down = refs[11]
    moments = {a: (refs[12 + j], refs[15 + j]) for j, a in enumerate("ugd")}
    new = {a: refs[18 + j] for j, a in enumerate("ugd")}
    new_moments = {a: (refs[21 + j], refs[24 + j]) for j, a in enumerate("ugd")}
    made = {a: refs[27 + j] for j, a in enumerate("ugd")}
    S = dict(zip(names, refs[30:], strict=True))
    at = coords()
    c, x = at["c"], at["x"]
    sib = device({**at, "c": 1 - c})
    steps, _, _ = plan()
    spots, near = places(at)
    windows = [pl.ds(13 * lax.div(v, 4) + 3 * lax.rem(v, 4), 4) for v in spots["z"]]
    zz = lax.rem(at["z"], 4)

    peers = [device({**at, "z": lax.rem(at["z"] + dz, 8), "c": lax.rem(c + dc, 2)}) for dz in range(8) for dc in range(2)][1:]
    peers += [device({**at, "x": lax.rem(at["x"] + dx, 4), "y": lax.rem(at["y"] + dy, 4)}) for dx in range(4) for dy in range(4)][1:]
    bar = pltpu.get_barrier_semaphore()
    for p in peers:
        pl.semaphore_signal(bar, inc=1, device_id=p, device_id_type=MESH)

    def halfcols(a, which):
        w = WIDTH[a]
        return pl.ds(pl.multiple_of((c if which else 1 - c) * w, 128), w)

    def inputs(j, p):
        rows = pl.ds(pl.multiple_of(j * 256, 256), 256)
        pairs = ((acts["gate"].at[j], S["gate"]), (acts["up"].at[j], S["up"]), (w_down.at[0, rows], S["wd"]), (acts["ht"].at[rows], S["ht"]))
        return [pltpu.make_async_copy(src, dst.at[p], S["insem"].at[n, p]) for n, (src, dst) in enumerate(pairs)]

    def outputs(j, p):
        cols = pl.ds(pl.multiple_of(j * 256, 256), 256)
        pairs = [(S["res_" + a].at[p], made[a].at[:, :, :, :, cols], n) for n, a in enumerate("ug")]
        for q in range(4):
            tile = j * 32 + 8 * q
            pairs.append((S["res_d"].at[p, pl.ds(8 * q, 8)], made["d"].at[lax.div(tile, 104), pl.ds(lax.rem(tile, 104), 8)], 2))
        return [pltpu.make_async_copy(src, dst, S["outsem"].at[n, p]) for src, dst, n in pairs]

    def outputs_done(p):
        return [pltpu.make_async_copy(S["res_" + a].at[p], S["res_" + a].at[p], S["outsem"].at[n, p]) for n, a in enumerate("ugd")]
    whole = [pltpu.make_async_copy(acts[n], S[n], S["wholesem"].at[k]) for k, n in enumerate(("dh", "at"))]
    for cp in [*inputs(0, 0), *whole]:
        cp.start()

    moment_copies = []
    for j, a in enumerate("ugd"):
        for q in (0, 1):
            ref = moments[a][q]
            moment_copies.append(pltpu.make_async_copy(ref.at[:, :, halfcols(a, 1)], S["mv_" + a].at[q, c], S["mvsem"].at[j, q, 2]))
        tile = windows[0] if a == "d" else pl.ds(at["z"], 1)
        moment_copies.append(pltpu.make_async_copy(weights[a].at[:, at["x"], at["y"], tile, :, halfcols(a, 1)], S["w_" + a], S["wsem"].at[j]))
    for cp in moment_copies:
        cp.start()
    pl.semaphore_wait(bar, len(peers))
    pend = []

    def remote(make):
        cp = make()
        cp.start()
        pend.append(make)
        return cp
    for j, a in enumerate("ugd"):
        for q in (0, 1):
            moment_copies.append(remote(lambda j=j, a=a, q=q: remote_copy(
                moments[a][q].at[:, :, halfcols(a, 0)], S["mv_" + a].at[q, c], S["mvsem"].at[j, q, 0], S["mvsem"].at[j, q, 1], sib)))

    def region(ref, i, level, v):
        l, a, col, n, o = UNITS[i]
        idx = view(a, o, at, level, v)
        return ref.at[(l, *idx, *([ALL] * (4 - len(idx))), pl.ds(col, n))]

    def pairs(i, off, which, dst):
        l, a, col, n, o = UNITS[i]
        cols = pl.ds(pl.multiple_of((c if which else 1 - c) * WIDTH[a] + col, 128), n)
        v = pos(i, 0, off)
        if a == "d" and not l:
            if o[0] == "x":
                return [(made["d"].at[v, pl.ds(26 * q, 26), :, cols], dst.at[q]) for q in range(4)]
            return [(made["d"].at[:, pl.ds(26 * v, 26), :, cols], dst)]
        idx = view(a, o, at, 0, v)
        return [((given if l else made)[a].at[(*idx, *([ALL] * (4 - len(idx))), cols)], dst)]

    def pos(i, level, off):
        a = UNITS[i][1]
        dim = UNITS[i][4][level] if level < 2 else LASTDIM[a]
        off %= SIZE[dim]
        if level < 2:
            return spots[dim][off]
        return windows[off] if a == "d" else pl.ds(spots[dim][off], 1)

    jobs = {k: n for n, k in enumerate(jobs_of(1) + jobs_of(0))}

    def landing(i, off):
        return region(S["loc_" + UNITS[i][1]], i, 0, pos(i, 0, off))

    def exchange(layer):
        for i, off in jobs_of(layer):
            n = jobs[i, off]
            for src, dst in pairs(i, off, 0, landing(i, off)):
                remote_copy(src, dst, S["ds"].at[n], S["dr"].at[n], sib).start()

    def exchanged(i, off):
        ref = landing(i, off)
        return remote_copy(ref, ref, S["ds"].at[jobs[i, off]], S["dr"].at[jobs[i, off]], sib)
    exchange(1)
    sib_waited = set()

    def wait_terms(i, off):
        off %= SIZE[UNITS[i][4][0]]
        n = SIZE[UNITS[i][4][0]]
        off = off - n if off > n // 2 else off
        if (i, off) not in sib_waited:
            sib_waited.add((i, off))
            exchanged(i, off).wait_recv()

    uses = {a: [] for a in "ugd"}
    for events in steps:
        for kind, level, key, s, k in events:
            if level == 0:
                h = SIZE[UNITS[key][4][0]] // 2
                if kind == "start" or k < h:
                    uses[UNITS[key][1]].append((key, h if kind == "start" else s * (h - k)))
    nth = {a: 0 for a in "ugd"}
    fetched = {a: 0 for a in "ugd"}

    def stage(a, n):
        i = uses[a][n][0]
        return S["stage_" + a].at[n % NB, :, :, :, pl.ds(0, UNITS[i][3])]

    layers = {1}

    def fetch_ahead(a):
        while fetched[a] < min(len(uses[a]), nth[a] + NB):
            n = fetched[a]
            i, off = uses[a][n]
            if UNITS[i][0] not in layers:
                return
            for src, dst in pairs(i, off, 1, stage(a, n)):
                pltpu.make_async_copy(src, dst, S["stsem_" + a].at[n % NB]).start()
            fetched[a] += 1

    own_fetched = set()

    sent = {}

    def own_buffer(i):
        return S["slot0_%d" % i].at[0, 0]

    def fetch_own(i):
        if i not in own_fetched and i in sent:
            sent[i]().wait_send()
            own_fetched.add(i)
            for src, dst in pairs(i, 0, 1, own_buffer(i)):
                pltpu.make_async_copy(src, dst, S["ownsem"].at[i]).start()

    def operands(level, i, off):
        _, a, _, _, o = UNITS[i]
        v = pos(i, level, off)
        here = region(S["loc_" + a], i, level, v)
        if level == 0:
            wait_terms(i, off)
            n = nth[a]
            assert uses[a][n] == (i, off)
            assert fetched[a] > n
            buf = stage(a, n)
            pltpu.make_async_copy(buf, buf, S["stsem_" + a].at[n % NB]).wait()
            nth[a] += 1
            return [buf, here]
        h = SIZE[o[0]] // 2
        first = [own_buffer(i)] + [S["slot0_%d" % i].at[d, h - 1] for d in (0, 1)]
        if level == 1:
            return [here] + [f.at[v] for f in first]
        w = pos(i, 1, 0)
        return [here] + [f.at[w, v] for f in first] + [S["slot1_%d" % i].at[d, 1, v] for d in (0, 1)]

    def half(ref, which, level, a):
        if level == 2 and TALL[a] == 1:
            return ref.at[..., pl.ds(896, 768) if which else pl.ds(0, 896)]
        n = ref.shape[0] // 2
        return ref.at[pl.ds(n * which, n)]

    def parts(key):
        r = []
        for i, u in enumerate(UNITS):
            if u[:2] == key:
                for lo, hi in ((0, 896), (896, 1664)):
                    a, b = max(lo, u[2]), min(hi, u[2] + u[3])
                    if a < b:
                        r.append((i, pl.ds(a - u[2], b - a), pl.ds(a, b - a), lo > 0))
        return r

    def cut(ref, cs):
        return ref.at[..., cs]

    def event(ev):
        kind, level, key, s, k = ev
        l, a = UNITS[key][:2] if level < 2 else key
        tag = "%d" % key if level < 2 else "%d%s" % key
        dim = UNITS[key][4][level] if level < 2 else LASTDIM[a]
        h = SIZE[dim] // 2
        if kind == "end":
            finish(l, a)
            return
        slot, rsem, ssem = (S["%s%d_%s" % (n, level, tag)] for n in ("slot", "r", "s"))

        def send(src, d, k):
            dst = lambda: slot.at[d, k] if k else half(slot.at[d, 0], d, level, a)
            remote(lambda: remote_copy(src(), dst(), ssem.at[d, k], rsem.at[d, k], near[dim, 1 - 2 * d]))

        if kind == "start":
            if level == 1:
                wait_terms(key, 0)
                fetch_own(key)
                assert key in own_fetched
                pltpu.make_async_copy(own_buffer(key), own_buffer(key), S["ownsem"].at[key]).wait()
            dst = (lambda: S["first_" + tag]) if level == 2 else (lambda: region(S["loc_" + a], key, level, pos(key, level, h)))
            if level < 2:
                addsum(dst(), operands(level, key, h))
            else:
                for i, uc, sc, _ in parts(key):
                    addsum(cut(dst(), sc), [cut(o, uc) for o in operands(level, i, h)])
            for d in (0, 1):
                send(lambda d=d: half(dst(), d, level, a), d, 0)
            if level == 0:
                fetch_own(key)
                fetch_ahead(a)
            return
        d = 0 if s > 0 else 1
        block = slot.at[d, k - 1]
        got = half(block, d, level, a) if k == 1 else block
        remote_copy(got, got, ssem.at[d, k - 1], rsem.at[d, k - 1], sib).wait_recv()
        if k == h:
            if level == 0:
                fetch_own(key)
            return
        off = s * (h - k)
        if level < 2:
            ops = operands(level, key, off)
            if k > 1:
                addsum(block, [block] + ops)
            else:
                for w in (0, 1):
                    hm = half(block, w, level, a)
                    addsum(hm, ([hm] if w == d else []) + [half(r, w, level, a) for r in ops])
        else:
            for i, uc, sc, w in parts(key):
                ops = [cut(o, uc) for o in operands(level, i, off)]
                m = cut(block, sc)
                if k > 1:
                    addsum(m, [m] + ops)
                elif TALL[a] == 1:
                    addsum(m, ([m] if w == (d == 1) else []) + ops)
                else:
                    for w in (0, 1):
                        hm = half(m, w, level, a)
                        addsum(hm, ([hm] if w == d else []) + [half(r, w, level, a) for r in ops])
        send(lambda: slot.at[d, k - 1], d, k)
        if (level, d, k) == (0, 0, 1):
            sent[key] = pend.pop()
        if level == 0:
            fetch_ahead(a)

    def finish(l, a):
        h = SIZE[LASTDIM[a]] // 2
        for i, uc, sc, _ in parts((l, a)):
            ops = [cut(o, uc) for o in operands(2, i, 0)] + [cut(S["slot2_%d%s" % (l, a)].at[d, h - 1], sc) for d in (0, 1)]
            addsum(cut(S["red_" + a].at[l], sc), ops)

    for a in "ugd":
        fetch_ahead(a)
    first = 0
    for n, events in zip(TASKS, steps, strict=False):
        for ev in events:
            event(ev)
        if not first:
            for cp in whole:
                cp.wait()

        def task(j, _):
            p = lax.rem(j, 2)
            for cp in inputs(j, p):
                cp.wait()

            @pl.when(j < 12)
            def _():
                for cp in inputs(j + 1, 1 - p):
                    cp.start()

            @pl.when(j >= 2)
            def _():
                for cp in outputs_done(p):
                    cp.wait()
            dh = dot(S["dh"][...], S["wd"][p], NT)
            S["res_d"][p] = dot(S["ht"][p], S["dh"][...]).reshape(32, 8, 1024).astype(BF)
            _, dgate, dup = silu_back(S["gate"][p], S["up"][p], dh.astype(BF).astype(F32))
            S["res_u"][p] = dot(S["at"][...], dup).reshape(4, 4, 8, 8, 256).astype(BF)
            S["res_g"][p] = dot(S["at"][...], dgate).reshape(4, 4, 8, 8, 256).astype(BF)
            for cp in outputs(j, p):
                cp.start()
            return 0
        lax.fori_loop(first, first + n, task, 0)
        first += n
    for p in (1, 0):
        for cp in outputs_done(p):
            cp.wait()
    exchange(0)
    layers.add(0)
    for a in "ugd":
        fetch_ahead(a)
    for ev in steps[-1]:
        event(ev)
    for i, off in jobs:
        exchanged(i, off).wait_send()
        wait_terms(i, off)

    total = jnp.zeros((8, 128), F32)
    for a in "ugd":
        for l in (0, 1):
            for t in range(TALL[a]):
                for q in range(WIDTH[a] // 128):
                    g = S["red_" + a][l, t, :, q * 128:q * 128 + 128].astype(F32)
                    if a == "d":
                        row = lax.broadcasted_iota(jnp.int32, (8, 128), 0) + 8 * t
                        g = jnp.where((row >= 2 * zz) & (row < 2 * zz + 26), g, 0.0)
                    total = total + g * g
    total = jnp.sum(total, axis=0, keepdims=True)
    for r, (buf, ds) in enumerate(((S["ar_z"], [(0, 0, q // 2, q % 2) for q in range(16)]), (S["ar_p"], [(q // 4, q % 4, 0, 0) for q in range(16)]))):
        buf[0] = total
        cps = []
        for q in range(1, 16):
            dx, dy, dz, dc = ds[q]
            to = device({"x": lax.rem(at["x"] + dx, 4), "y": lax.rem(at["y"] + dy, 4), "z": lax.rem(at["z"] + dz, 8), "c": lax.rem(c + dc, 2)})
            cps.append(remote(lambda q=q, to=to: remote_copy(buf.at[0], buf.at[q], S["arsem"].at[2 * r, q], S["arsem"].at[2 * r + 1, q], to)))
        for cp in cps:
            cp.wait_recv()
            cp.wait_send()
            pend.pop()
        total = buf[0]
        for q in range(1, 16):
            total = total + buf[q]
    mean = jnp.sum(total, axis=1, keepdims=True) / COUNT
    factor = jnp.minimum(1.0, 0.5 * lax.rsqrt(mean + 1e-30))
    for cp in moment_copies:
        cp.wait_recv() if cp.is_remote else cp.wait()

    def adamw(w, m, v, g):
        g = g * factor
        m = 0.9 * m + 0.1 * g
        v = 0.95 * v + 0.05 * g * g
        step = m * lax.rsqrt(v + 1e-8) + 0.1 * w
        return (w - 0.02 * step).astype(BF), m, v

    for a in "ug":
        mv, red, wv = S["mv_" + a], S["red_" + a], S["w_" + a]

        def body(q, _, mv=mv, red=red, wv=wv, a=a):
            cs = pl.ds(pl.multiple_of(q * 128, 128), 128)
            for l in (0, 1):
                m, v = (jnp.concatenate([mv[e, 0, l, :, cs], mv[e, 1, l, :, cs]], axis=0) for e in (0, 1))
                n, m, v = adamw(wv[l, 0, :, cs].astype(F32), m, v, red[l, 0, :, cs].astype(F32))
                wv[l, 0, :, cs] = n
                for e, t in enumerate((m, v)):
                    for s in (0, 1):
                        mv[e, s, l, :, cs] = t[4 * s:4 * s + 4]
            return 0
        lax.fori_loop(0, 13, body, 0)
    row = lax.broadcasted_iota(jnp.int32, (32, 32), 0)
    column = lax.broadcasted_iota(jnp.int32, (32, 32), 1)
    pick = (column == 2 * zz + 13 * (row >> 4) + (row & 15)) & ((row & 15) < 13)
    pick = jnp.where(pick, 1.0, 0.0).astype(BF)
    for l in (0, 1):
        gd, wd = (jnp.dot(pick, S[n][l].reshape(32, 512), preferred_element_type=F32) for n in ("red_d", "w_d"))
        for s in (0, 1):
            rows = slice(16 * s, 16 * s + 16)
            n, m, v = adamw(wd[rows], S["mv_d"][0, s, l], S["mv_d"][1, s, l], gd[rows])
            S["new_d"][l, s] = n
            S["mv_d"][0, s, l] = m
            S["mv_d"][1, s, l] = v
    ends = []
    for j, a in enumerate("ugd"):
        cp = pltpu.make_async_copy(S["new_d"] if a == "d" else S["w_" + a].at[:, 0], new[a], S["newsem"].at[j])
        cp.start()
        ends.append(cp.wait)
        for q in (0, 1):
            out = new_moments[a][q].at[:, :, halfcols(a, 1)]
            cp = remote_copy(S["mv_" + a].at[q, 1 - c], out, S["finsem"].at[j, q, 0], S["finsem"].at[j, q, 1], sib)
            cp.start()
            back = remote_copy(S["mv_" + a].at[q, 1 - c], new_moments[a][q].at[:, :, halfcols(a, 0)], S["finsem"].at[j, q, 0], S["finsem"].at[j, q, 1], sib)
            ends += [cp.wait_send, back.wait_recv]
            cp = pltpu.make_async_copy(S["mv_" + a].at[q, c], out, S["finsem"].at[j, q, 2])
            cp.start()
            ends.append(cp.wait)
    for wait in ends:
        wait()
    for make in pend:
        make().wait_send()


def reduce_scatter(grads, acts, weights, w_down, m, v):
    args = [g.reshape(4, 4, -1, 8, g.shape[-1]) for g in grads] + list(acts)
    args += [w.reshape(2, 4, 4, -1, 8, w.shape[-1]) for w in weights] + [w_down, *m, *v]
    sh = rs_scratch()
    any_ = pl.BlockSpec(memory_space=pl.ANY)
    outs = [jax.ShapeDtypeStruct(s, BF) for s in ((2, 8, 1664), (2, 8, 1664), (2, 2, 16, 512))] + [jax.ShapeDtypeStruct(t.shape, F32) for t in (*m, *v)]
    outs += [jax.ShapeDtypeStruct(s, BF) for s in ((4, 4, 8, 8, 3328), (4, 4, 8, 8, 3328), (4, 104, 8, 1024))]
    outs = pl.pallas_call(
        functools.partial(rs_kernel, list(sh)), out_shape=outs, in_specs=[any_] * 18, out_specs=[any_] * 12, scratch_shapes=list(sh.values()), name="reduce_scatter",
        compiler_params=pltpu.CompilerParams(collective_id=0, has_side_effects=True, vmem_limit_bytes=VMEM_BYTES))(*args)
    return outs[:3], outs[3:6], outs[6:9]


def plan_ag():
    RATE, LAT = 46.0e3, 2.9
    free, heap, order, seq, got, now = {}, [], [], [0], {}, 1.0

    def push(t, ev):
        seq[0] += 1
        heapq.heappush(heap, (t, seq[0], ev))

    def send(t, link, nbytes):
        free[link] = max(free.get(link, 0.0), t) + nbytes / RATE
        return free[link] + LAT
    ring = {(2, a): (LASTDIM[a], {"u": 8 * 1664, "g": 8 * 1664, "d": 32 * 512}[a] * 4) for a in "ugd"}
    for i, (_, a, _, cols, o) in enumerate(UNITS):
        ring[1, i] = (o[1], DEPTH[a] * 8 * cols * 2)
        ring[0, i] = (o[0], 4 * DEPTH[a] * 8 * cols * 2)
    for a in "gdu":
        push(1.0, ("start", 2, a, 0, 0))
    while heap:
        t, _, ev = heapq.heappop(heap)
        kind, level, key, s, k = ev
        dim, nbytes = ring[level, key]
        h = SIZE[dim] // 2
        now = max(now, t) + 0.1
        order.append(ev)
        if kind == "start":
            for s in (1, -1):
                push(send(now, (dim, s), nbytes), ("step", level, key, s, 1))
            continue
        if k < h:
            push(send(now, (dim, s), nbytes if k < h - 1 else nbytes // 2), ("step", level, key, s, k + 1))
            continue
        got[level, key] = got.get((level, key), 0) + 1
        if got[level, key] < 2:
            continue
        if level == 2:
            for i, u in enumerate(UNITS):
                if u[1] == key:
                    push(now + (1.0 if key == "d" else 0), ("start", 1, i, 0, 0))
        elif level == 1:
            push(now, ("start", 0, key, 0, 0))
    return order, now, free


def ag_scratch():
    sem = pltpu.SemaphoreType.DMA
    sh = {"pc": pltpu.VMEM((8, 2, 2, 16, 512), BF), "asm": pltpu.VMEM((2, 26, 8, 512), BF), "loc": sem((4,)), "sr": sem((128,)), "ss": sem((128,))}
    for n in "rs":
        for a in "ugd":
            sh["%s2_%s" % (n, a)] = sem((2, SIZE[LASTDIM[a]] // 2))
        for i, u in enumerate(UNITS):
            for lv in (0, 1):
                sh["%s%d_%d" % (n, lv, i)] = sem((2, SIZE[u[4][lv]] // 2))
    return sh


def ag_kernel(names, *refs):
    own = {a: refs[j] for j, a in enumerate("ugd")}
    out = {a: refs[3 + j] for j, a in enumerate("ugd")}
    S = dict(zip(names, refs[6:], strict=True))
    at = coords()
    c, x, y, z = at["c"], at["x"], at["y"], at["z"]
    sib = device({**at, "c": 1 - c})
    order, _, _ = plan_ag()
    spots, near = places(at)
    peers = [sib, *near.values()]
    bar = pltpu.get_barrier_semaphore()
    for p in peers:
        pl.semaphore_signal(bar, inc=1, device_id=p, device_id_type=MESH)

    def hc(a, col=0, n=None):
        return pl.ds(pl.multiple_of(c * WIDTH[a] + col, 128), WIDTH[a] if n is None else n)
    local = [pltpu.make_async_copy(own["u"], out["u"].at[:, x, y, z, :, hc("u")], S["loc"].at[0]),
             pltpu.make_async_copy(own["g"], out["g"].at[:, x, y, z, :, hc("g")], S["loc"].at[1]),
             pltpu.make_async_copy(own["d"], S["pc"].at[z], S["loc"].at[2])]
    for cp in local:
        cp.start()
    pl.semaphore_wait(bar, len(peers))
    for cp in local:
        cp.wait()
    pend, twin = [], []

    def remote(src, ss, rs, to):
        cp = remote_copy(src, src, ss, rs, to)
        cp.start()
        pend.append(cp)

    def to_sibling(ref):
        n = len(twin)
        remote(ref, S["ss"].at[n], S["sr"].at[n], sib)
        twin.append(ref)

    def region(level, key, v):
        if level == 2:
            if key == "d":
                return S["pc"].at[v]
            return out["u"].at[:, x, v, z, :, hc("u")] if key == "u" else out["g"].at[:, x, y, v, :, hc("g")]
        l, a, col, n, o = UNITS[key]
        idx = view(a, o, at, level, v)
        return out[a].at[(l, *idx, *([ALL] * (4 - len(idx))), hc(a, col, n))]

    def half(ref, which):
        n = ref.shape[0] // 2
        return ref.at[pl.ds(n * which, n)]

    got = {}
    for kind, level, key, s, k in order:
        dim = UNITS[key][4][level] if level < 2 else LASTDIM[key]
        n = SIZE[dim]
        h = n // 2
        rsem, ssem = S["r%d_%s" % (level, key)], S["s%d_%s" % (level, key)]

        def send(src, d, k, dim=dim, rsem=rsem, ssem=ssem):
            remote(src, ssem.at[d, k], rsem.at[d, k], near[dim, 1 - 2 * d])

        if kind == "start":
            for d in (0, 1):
                send(region(level, key, at[dim]), d, 0)
            continue
        d = 0 if s > 0 else 1
        block = region(level, key, spots[dim][-s * k % n])
        if k == h:
            block = half(block, d)
        remote_copy(block, block, ssem.at[d, k - 1], rsem.at[d, k - 1], sib).wait_recv()
        if k < h - 1:
            send(block, d, k)
        elif k == h - 1:
            send(half(block, d), d, k)
        if level < 2:
            to_sibling(block)
        if k == h:
            got[level, key] = got.get((level, key), 0) + 1
            if level == 2 and got[level, key] == 2:
                if key == "d":
                    q = lax.broadcasted_iota(jnp.int32, (208, 256), 1)
                    r = lax.broadcasted_iota(jnp.int32, (208, 256), 0)
                    e = q & 15
                    pick = (r == 26 * (q >> 5) + 13 * ((q >> 4) & 1) + e) & (e < 13)
                    pick = jnp.where(pick, 1.0, 0.0).astype(BF)
                    for l in (0, 1):
                        rows = jnp.dot(pick, S["pc"][:, l].reshape(256, 512), preferred_element_type=F32)
                        S["asm"][l] = rows.reshape(26, 8, 512).astype(BF)
                    cp = pltpu.make_async_copy(S["asm"], out["d"].at[:, x, y, :, :, hc("d")], S["loc"].at[3])
                    cp.start()
                    cp.wait()
                idx = (ALL, x, ALL, z, ALL) if key == "u" else (ALL, x, y, ALL, ALL)
                to_sibling(out[key].at[(*idx, hc(key))])
    for n, ref in enumerate(twin):
        remote_copy(ref, ref, S["ss"].at[n], S["sr"].at[n], sib).wait_recv()
    for cp in pend:
        cp.wait_send()


def all_gather(u, g, d):
    sh = ag_scratch()
    any_ = pl.BlockSpec(memory_space=pl.ANY)
    outs = [jax.ShapeDtypeStruct((2, 4, 4, TILES[a], 8, 2 * WIDTH[a]), BF) for a in "ugd"]
    return pl.pallas_call(
        functools.partial(ag_kernel, list(sh)), out_shape=outs, in_specs=[any_] * 3, out_specs=[any_] * 3, scratch_shapes=list(sh.values()), name="all_gather",
        compiler_params=pltpu.CompilerParams(collective_id=1, has_side_effects=True, vmem_limit_bytes=AG_VMEM))(u, g, d)


def solution(mesh):
    def step(x, dy, w_gate, w_up, w_down, *moments):
        x, dy = x[0], dy[0]
        gate0, up0, hid0, h1, a0 = layer0(x, w_gate, w_up, w_down)
        down1, gate1, up1, dh1 = layer1(h1, dy, w_gate, w_up, w_down)
        m, v = moments[:3], moments[3:]
        order = lambda t: (t[1], t[0], t[2])
        pad = lambda t: (*t[:2], jnp.pad(t[2], ((0, 0), (0, 3), (0, 0))))
        acts = (dh1, a0, gate0, up0, hid0)
        new, m, v = reduce_scatter((up1, gate1, down1), acts, order((w_gate, w_up, w_down)), w_down, pad(order(m)), pad(order(v)))
        u, g, d = all_gather(*new)
        w = (g.reshape(w_gate.shape), u.reshape(w_up.shape), d.reshape(w_down.shape))
        cut = lambda t: (t[1], t[0], t[2][:, :13])
        return (*w, *cut(m), *cut(v))

    data, whole, rows = P(("rep", "dp"), None, None), P(), P(None, "dp", None)
    out = P("rep", None, None)
    return jax.shard_map(step, mesh=mesh, in_specs=(data, data) + (whole,) * 3 + (rows,) * 6, out_specs=(out,) * 3 + (P("rep", "dp", None),) * 6, check_vma=False)
```

```python
import functools
import heapq

import jax
import jax.numpy as jnp
from jax import lax
from jax.experimental import pallas as pl
from jax.experimental.pallas import tpu as pltpu
from jax.sharding import PartitionSpec as P

MESH = pl.DeviceIdType.MESH
BF, F32 = jnp.bfloat16, jnp.float32
SIZE = {"x": 4, "y": 4, "z": 8}
VMEM_BYTES = 67043328
AG_VMEM = 4 * 2**20
ALL = slice(None)


def coords():
    i = lax.axis_index("dp")
    return {"x": i // 64, "y": lax.rem(i // 16, 4), "z": lax.rem(i // 2, 8), "c": lax.rem(i, 2)}


def device(at):
    return {"dp": ((at["x"] * 4 + at["y"]) * 8 + at["z"]) * 2 + at["c"]}


def places(at):
    spots = {d: [at[d]] + [lax.rem(at[d] + k, n) for k in range(1, n)] for d, n in SIZE.items()}
    return spots, {(d, s): device({**at, d: spots[d][s]}) for d in SIZE for s in (1, -1)}


UNITS = [
    (1, "d", 0, 256, "xyz"), (1, "d", 256, 256, "yxz"), (1, "u", 0, 896, "zxy"), (1, "u", 896, 768, "zxy"), (1, "g", 0, 896, "xyz"), (1, "g", 896, 768, "yxz"),
    (0, "d", 0, 256, "xyz"), (0, "d", 256, 256, "yxz"), (0, "u", 0, 896, "zxy"), (0, "u", 896, 768, "zxy"), (0, "g", 0, 896, "yxz"), (0, "g", 896, 768, "xyz"),
]
DEPTH = {"u": 4, "g": 8, "d": 26}
TILES = {"u": 8, "g": 8, "d": 26}
WIDTH = {"u": 1664, "g": 1664, "d": 512}
TALL = {"u": 1, "g": 1, "d": 4}
LASTDIM = {"u": "y", "g": "z", "d": "z"}
MOMENTS = {"u": (2, 4), "g": (2, 4), "d": (13, 2)}
COUNT = 2 * 3 * 1024 * 3328
NB = 2


def view(a, order, at, level, v):
    if level == 0:
        return {"z": (ALL, ALL, v), "x": (v,), "y": (ALL, v)}[order[0]]
    if level == 1:
        return {"zxy": (v, ALL, at["z"]), "xyz": (at["x"], v), "yxz": (v, at["y"])}[order]
    return (at["x"], v, at["z"]) if a == "u" else (at["x"], at["y"], v)


def block_shape(i, level):
    _, a, _, cols, _ = UNITS[i]
    return ((4, DEPTH[a], 8, cols), (DEPTH[a], 8, cols))[level]


def remote_copy(src, dst, ss, rs, to):
    return pltpu.make_async_remote_copy(src_ref=src, dst_ref=dst, send_sem=ss, recv_sem=rs, device_id=to, device_id_type=MESH)


T = 1024
B = 256
N = 3328 // B
NT = (((1,), (1,)), ((), ()))


def dot(a, b, dims=(((1,), (0,)), ((), ()))):
    return lax.dot_general(a, b, dims, preferred_element_type=F32)


def norm_scale(wide):
    return lax.rsqrt(jnp.mean(wide**2, -1, keepdims=True) + 1e-6)


def rowwise(n, body, step=128):
    def one(i, _):
        body(pl.ds(pl.multiple_of(i * step, step), step))
        return 0
    lax.fori_loop(0, n // step, one, 0)


def silu_back(g, u, dh):
    s = jax.nn.sigmoid(g)
    silu = g * s
    return silu, (dh * u * (s + silu * (1.0 - s))).astype(BF), (dh * silu).astype(BF)


def norm_into(h, a):
    def norm(rows):
        wide = h[rows].astype(F32)
        a[rows] = (wide * norm_scale(wide)).astype(BF)
    rowwise(T, norm)


def pipelined(chunk, first, second):
    held = None
    for m in range(0, T, chunk):
        rows = slice(m, m + chunk)
        now = first(rows)
        if held is not None:
            second(*held)
        held = rows, now
    second(*held)


def fwd0(C, tr, x, wg, wu, wd, gate, up, ht, h1, at, a, hid):
    j = pl.program_id(0)

    @pl.when(j == 0)
    def _():
        norm_into(x, a)
        at[...] = a[...].T if tr else a[...]

    @pl.when(j < N)
    def _():
        def first(rows):
            return dot(a[rows], wg[...]), dot(a[rows], wu[...])

        def second(rows, gu):
            g, u = gu
            gate[rows] = g
            up[rows] = u
            v = (g * jax.nn.sigmoid(g) * u).astype(BF)
            hid[j, rows] = v
            if tr:
                ht[:, rows] = v.T
            else:
                ht[rows] = v
        pipelined(C, first, second)

    @pl.when(j >= N)
    def _():
        def first(rows):
            return sum(dot(hid[i, rows], wd[i * B:i * B + B]) for i in range(N))

        def second(rows, y):
            n = pl.ds(pl.multiple_of((j - N) * B, B), B)
            h1[rows] = (x[rows, n].astype(F32) + y.astype(BF).astype(F32)).astype(BF)
        pipelined(C, first, second)


def layer0(x, w_gate, w_up, w_down, C=512, tr=True):
    whole = pl.BlockSpec((T, T), lambda j: (0, 0))
    cap = lambda j: jnp.minimum(j, N - 1)
    cols = pl.BlockSpec((T, B), lambda j: (0, cap(j)))
    wcols = pl.BlockSpec((None, T, B), lambda j: (0, 0, cap(j)))
    late = lambda j: jnp.maximum(j - N, 0)
    wrows = pl.BlockSpec((None, 3328, B), lambda j: (0, 0, late(j)))
    rows = pl.BlockSpec((B, T), lambda j: (cap(j), 0)) if tr else cols
    o = jax.ShapeDtypeStruct
    blk = pl.BlockSpec((None, T, B), lambda j: (cap(j), 0, 0))
    return pl.pallas_call(functools.partial(fwd0, C, tr), grid=(N + 4,), in_specs=[whole, wcols, wcols, wrows],
        out_specs=[blk, blk, rows, pl.BlockSpec((T, B), lambda j: (0, late(j))), whole],
        out_shape=[o((N, T, B), F32)] * 2 + [o((3328, T) if tr else (T, 3328), BF), o((T, T), BF), o((T, T), BF)],
        scratch_shapes=[pltpu.VMEM((T, T), BF), pltpu.VMEM((N, T, B), BF)], name="layer0",
        compiler_params=pltpu.CompilerParams(vmem_limit_bytes=VMEM_BYTES))(x, w_gate, w_up, w_down)


def both1(h, dy, wg, wu, wd, wg2, wu2, dwd, dwg, dwu, dh1, a, at, gs, us, hta, htb, acc):
    j = pl.program_id(0)

    @pl.when(j == 0)
    def _():
        norm_into(h, a)
        at[...] = a[...].T

    def now():
        return dot(a[...], wg[...]), dot(a[...], wu[...]), dot(dy[...], wd[...], NT)

    def before(ht):
        dwd[...] = dot(ht[...], dy[...]).astype(BF)
        dwg[...] = dot(at[...], gs[j - 1]).astype(BF)
        dwu[...] = dot(at[...], us[j - 1]).astype(BF)

    def then(g, u, dh, ht):
        silu, dgate, dup = silu_back(g, u, dh.astype(BF).astype(F32))
        gs[j] = dgate
        us[j] = dup
        ht[...] = (silu * u).astype(BF).T

    @pl.when(j == 0)
    def _():
        then(*now(), hta)

    for p, (mine, last) in enumerate(((hta, htb), (htb, hta))):
        @pl.when((j > 0) & (j < N) & (lax.rem(j, 2) == p))
        def _():
            x = now()
            before(last)
            then(*x, mine)

    @pl.when(j == N)
    def _():
        before(hta)

    @pl.when(j >= N)
    def _():
        y = sum(dot(gs[i], wg2[:, i * B:i * B + B], NT) + dot(us[i], wu2[:, i * B:i * B + B], NT) for i in range(N))
        acc[:, pl.ds(pl.multiple_of((j - N) * B, B), B)] = y

    @pl.when(j == N + 3)
    def _():
        def back(rows):
            wide = h[rows].astype(F32)
            scale = norm_scale(wide)
            d = acc[rows].astype(BF).astype(F32)
            d = d * scale - wide * (scale * scale * scale * jnp.mean(d * wide, -1, keepdims=True))
            dh1[rows] = (dy[rows].astype(F32) + d.astype(BF).astype(F32)).astype(BF)
        rowwise(T, back)


def layer1(h, dy, w_gate, w_up, w_down):
    cap = lambda j: jnp.minimum(j, N - 1)
    prev = lambda j: jnp.clip(j - 1, 0, N - 1)
    late = lambda j: jnp.maximum(j - N, 0)
    whole = pl.BlockSpec((T, T), lambda j: (0, 0))
    cols = pl.BlockSpec((T, B), lambda j: (0, prev(j)))
    wcols = pl.BlockSpec((None, T, B), lambda j: (1, 0, cap(j)))
    wrows = pl.BlockSpec((None, B, T), lambda j: (1, cap(j), 0))
    wtall = pl.BlockSpec((None, B, 3328), lambda j: (1, late(j), 0))
    rows = pl.BlockSpec((B, T), lambda j: (prev(j), 0))
    o = jax.ShapeDtypeStruct
    return pl.pallas_call(both1, grid=(N + 4,), in_specs=[whole, whole, wcols, wcols, wrows, wtall, wtall], out_specs=[rows, cols, cols, whole],
        out_shape=[o((3328, T), BF)] + [o((T, 3328), BF)] * 2 + [o((T, T), BF)],
        scratch_shapes=[pltpu.VMEM((T, T), BF)] * 2 + [pltpu.VMEM((N, T, B), BF)] * 2 + [pltpu.VMEM((B, T), BF)] * 2 + [pltpu.VMEM((T, T), F32)], name="layer1",
        compiler_params=pltpu.CompilerParams(vmem_limit_bytes=VMEM_BYTES))(h, dy, w_gate, w_up, w_down, w_gate, w_up)


TASKS = (2, 3, 4, 4)


def jobs_of(layer):
    rank = {}
    for i, u in enumerate(UNITS):
        if u[0] == layer:
            n = SIZE[u[4][0]]
            h = n // 2
            for at, off in enumerate([h] + [s * (h - k) for k in range(1, h) for s in (1, -1)] + [0]):
                rank[i, off] = (at / n, i)
    return sorted(rank, key=rank.get)


def plan():
    RATE, LAT, TASK, DRATE, DLAT = 46.0e3, 3.0, 2.7, 600.0e3, 2.0
    free, heap, seq = {}, [], [0]

    def send(t, link, nbytes):
        free[link] = max(free.get(link, 0.0), t) + nbytes / RATE
        return free[link] + LAT

    def push(t, ev):
        seq[0] += 1
        heapq.heappush(heap, (t, seq[0], ev))
    ring = {}
    for i, (l, a, _, cols, o) in enumerate(UNITS):
        ring[0, i] = (o[0], 4 * DEPTH[a] * 8 * cols * 2)
        ring[1, i] = (o[1], DEPTH[a] * 8 * cols * 2)
        ring[2, (l, a)] = (LASTDIM[a], TALL[a] * 8 * WIDTH[a] * 2)
    arrive, got, steps, now = {}, {}, [], 2.0

    def exchange(layer, t):
        for i, off in jobs_of(layer):
            t += ring[0, i][1] / DRATE
            arrive[i, off] = t + DLAT
            if off == SIZE[UNITS[i][4][0]] // 2:
                push(arrive[i, off], ("start", 0, i, 0, 0))

    def run(until):
        nonlocal now
        taken = []
        while heap and heap[0][0] <= until:
            t, _, ev = heapq.heappop(heap)
            kind, level, key, s, k = ev
            dim, nbytes = ring[level, key]
            h = SIZE[dim] // 2
            if level == 0 and kind == "step" and k < h and arrive[key, s * (h - k)] > t:
                push(arrive[key, s * (h - k)], ev)
                continue
            now = max(now, t)
            taken.append(ev)
            cost = 0.15 + nbytes * (4 + 2 * level) / 7.0e6
            if kind == "end":
                continue
            if kind == "start":
                now += cost
                for s in (1, -1):
                    push(send(now, (dim, s), nbytes // 2), ("step", level, key, s, 1))
            elif k < h:
                now += cost
                push(send(now, (dim, s), nbytes), ("step", level, key, s, k + 1))
            else:
                got[level, key] = got.get((level, key), 0) + 1
                if got[level, key] < 2:
                    continue
                if level == 0:
                    push(now, ("start", 1, key, 0, 0))
                elif level == 1:
                    ka = UNITS[key][:2]
                    if all(got.get((1, i)) == 2 for i, u in enumerate(UNITS) if u[:2] == ka):
                        push(now, ("start", 2, ka, 0, 0))
                else:
                    push(now, ("end", 2, key, 0, 0))
        return taken
    exchange(1, now)
    now = max(now, FIRST)
    for n in TASKS:
        steps.append(run(now))
        now += n * TASK
    exchange(0, now)
    steps.append(run(float("inf")))
    return steps, now, free


FIRST = 1.0


def addsum(dst, srcs):
    def add(*at):
        acc = srcs[0][at].astype(F32)
        for s in srcs[1:]:
            acc = acc + s[at].astype(F32)
        dst[at] = acc.astype(BF)

    if len(dst.shape) == 4:

        def body(i, _):
            add(i)
            return 0
        lax.fori_loop(0, dst.shape[0], body, 0)
    else:
        add(...)


def rs_scratch():
    sh = {}
    sem = pltpu.SemaphoreType.DMA
    for a in "ugd":
        sh["loc_" + a] = pltpu.VMEM((2, 4, 4, TILES[a], 8, WIDTH[a]), BF)
        sh["stage_" + a] = pltpu.VMEM((NB, 4, DEPTH[a], 8, max(u[3] for u in UNITS if u[1] == a)), BF)
        sh["stsem_" + a] = sem((NB,))
        sh["red_" + a] = pltpu.VMEM((2, TALL[a], 8, WIDTH[a]), BF)
        sh["mv_" + a] = pltpu.VMEM((2, 2, *MOMENTS[a], WIDTH[a]), F32)
        sh["w_" + a] = pltpu.VMEM((2, TALL[a], 8, WIDTH[a]), BF)
        h = SIZE[LASTDIM[a]] // 2
        for l in (0, 1):
            sh["slot2_%d%s" % (l, a)] = pltpu.VMEM((2, h, TALL[a], 8, WIDTH[a]), BF)
            sh["first_%d%s" % (l, a)] = pltpu.VMEM((TALL[a], 8, WIDTH[a]), BF)
            for n in "rs":
                sh["%s2_%d%s" % (n, l, a)] = sem((2, h))
    sh["new_d"] = pltpu.VMEM((2, 2, 16, 512), BF)
    sh["wide_d"] = pltpu.VMEM((2, 2, 16, 512), F32)
    for i, u in enumerate(UNITS):
        h = SIZE[u[4][0]] // 2
        sh["slot0_%d" % i] = pltpu.VMEM((2, h) + block_shape(i, 0), BF)
        sh["slot1_%d" % i] = pltpu.VMEM((2, 2) + block_shape(i, 1), BF)
        for n in "rs":
            sh["%s0_%d" % (n, i)] = sem((2, h))
            sh["%s1_%d" % (n, i)] = sem((2, 2))
    sh["ownsem"] = sem((len(UNITS),))
    sh["dh"] = pltpu.VMEM((1024, 1024), BF)
    sh["at"] = pltpu.VMEM((1024, 1024), BF)
    sh["gate"] = pltpu.VMEM((2, 1024, 256), F32)
    sh["up"] = pltpu.VMEM((2, 1024, 256), F32)
    sh["wd"] = pltpu.VMEM((2, 256, 1024), BF)
    sh["ht"] = pltpu.VMEM((2, 256, 1024), BF)
    sh["res_u"] = pltpu.VMEM((2, 4, 4, 8, 8, 256), BF)
    sh["res_g"] = pltpu.VMEM((2, 4, 4, 8, 8, 256), BF)
    sh["res_d"] = pltpu.VMEM((2, 32, 8, 1024), BF)
    sh["insem"] = sem((4, 2))
    sh["outsem"] = sem((3, 2))
    sh["wholesem"] = sem((2,))
    sh["dr"] = sem((64,))
    sh["ds"] = sem((64,))
    sh["ar_z"] = pltpu.VMEM((16, 1, 128), F32)
    sh["ar_p"] = pltpu.VMEM((16, 1, 128), F32)
    sh["arsem"] = sem((4, 16))
    sh["mvsem"] = sem((3, 2, 3))
    sh["wsem"] = sem((3,))
    sh["finsem"] = sem((3, 2, 3))
    sh["newsem"] = sem((3,))
    return sh


def rs_kernel(names, *refs):
    given = {a: refs[j] for j, a in enumerate("ugd")}
    acts = dict(zip(("dh", "at", "gate", "up", "ht"), refs[3:8], strict=True))
    weights = {a: refs[8 + j] for j, a in enumerate("ugd")}
    w_down = refs[11]
    moments = {a: (refs[12 + j], refs[15 + j]) for j, a in enumerate("ugd")}
    new = {a: refs[18 + j] for j, a in enumerate("ugd")}
    new_moments = {a: (refs[21 + j], refs[24 + j]) for j, a in enumerate("ugd")}
    made = {a: refs[27 + j] for j, a in enumerate("ugd")}
    S = dict(zip(names, refs[30:], strict=True))
    at = coords()
    c, x = at["c"], at["x"]
    sib = device({**at, "c": 1 - c})
    steps, _, _ = plan()
    spots, near = places(at)
    windows = [pl.ds(13 * lax.div(v, 4) + 3 * lax.rem(v, 4), 4) for v in spots["z"]]
    zz = lax.rem(at["z"], 4)

    peers = [device({**at, "z": lax.rem(at["z"] + dz, 8), "c": lax.rem(c + dc, 2)}) for dz in range(8) for dc in range(2)][1:]
    peers += [device({**at, "x": lax.rem(at["x"] + dx, 4), "y": lax.rem(at["y"] + dy, 4)}) for dx in range(4) for dy in range(4)][1:]
    bar = pltpu.get_barrier_semaphore()
    for p in peers:
        pl.semaphore_signal(bar, inc=1, device_id=p, device_id_type=MESH)

    def halfcols(a, which):
        w = WIDTH[a]
        return pl.ds(pl.multiple_of((c if which else 1 - c) * w, 128), w)

    def inputs(j, p):
        rows = pl.ds(pl.multiple_of(j * 256, 256), 256)
        pairs = ((acts["gate"].at[j], S["gate"]), (acts["up"].at[j], S["up"]), (w_down.at[0, rows], S["wd"]), (acts["ht"].at[rows], S["ht"]))
        return [pltpu.make_async_copy(src, dst.at[p], S["insem"].at[n, p]) for n, (src, dst) in enumerate(pairs)]

    def outputs(j, p):
        cols = pl.ds(pl.multiple_of(j * 256, 256), 256)
        pairs = [(S["res_" + a].at[p], made[a].at[:, :, :, :, cols], n) for n, a in enumerate("ug")]
        for q in range(4):
            tile = j * 32 + 8 * q
            pairs.append((S["res_d"].at[p, pl.ds(8 * q, 8)], made["d"].at[lax.div(tile, 104), pl.ds(lax.rem(tile, 104), 8)], 2))
        return [pltpu.make_async_copy(src, dst, S["outsem"].at[n, p]) for src, dst, n in pairs]

    def outputs_done(p):
        return [pltpu.make_async_copy(S["res_" + a].at[p], S["res_" + a].at[p], S["outsem"].at[n, p]) for n, a in enumerate("ugd")]
    whole = [pltpu.make_async_copy(acts[n], S[n], S["wholesem"].at[k]) for k, n in enumerate(("dh", "at"))]
    for cp in [*inputs(0, 0), *whole]:
        cp.start()

    moment_copies = []
    for j, a in enumerate("ugd"):
        for q in (0, 1):
            ref = moments[a][q]
            moment_copies.append(pltpu.make_async_copy(ref.at[:, :, halfcols(a, 1)], S["mv_" + a].at[q, c], S["mvsem"].at[j, q, 2]))
        tile = windows[0] if a == "d" else pl.ds(at["z"], 1)
        moment_copies.append(pltpu.make_async_copy(weights[a].at[:, at["x"], at["y"], tile, :, halfcols(a, 1)], S["w_" + a], S["wsem"].at[j]))
    for cp in moment_copies:
        cp.start()
    pl.semaphore_wait(bar, len(peers))
    pend = []

    def remote(make):
        cp = make()
        cp.start()
        pend.append(make)
        return cp
    for j, a in enumerate("ugd"):
        for q in (0, 1):
            moment_copies.append(remote(lambda j=j, a=a, q=q: remote_copy(
                moments[a][q].at[:, :, halfcols(a, 0)], S["mv_" + a].at[q, c], S["mvsem"].at[j, q, 0], S["mvsem"].at[j, q, 1], sib)))

    def region(ref, i, level, v):
        l, a, col, n, o = UNITS[i]
        idx = view(a, o, at, level, v)
        return ref.at[(l, *idx, *([ALL] * (4 - len(idx))), pl.ds(col, n))]

    def pairs(i, off, which, dst):
        l, a, col, n, o = UNITS[i]
        cols = pl.ds(pl.multiple_of((c if which else 1 - c) * WIDTH[a] + col, 128), n)
        v = pos(i, 0, off)
        if a == "d" and not l:
            if o[0] == "x":
                return [(made["d"].at[v, pl.ds(26 * q, 26), :, cols], dst.at[q]) for q in range(4)]
            return [(made["d"].at[:, pl.ds(26 * v, 26), :, cols], dst)]
        idx = view(a, o, at, 0, v)
        return [((given if l else made)[a].at[(*idx, *([ALL] * (4 - len(idx))), cols)], dst)]

    def pos(i, level, off):
        a = UNITS[i][1]
        dim = UNITS[i][4][level] if level < 2 else LASTDIM[a]
        off %= SIZE[dim]
        if level < 2:
            return spots[dim][off]
        return windows[off] if a == "d" else pl.ds(spots[dim][off], 1)

    jobs = {k: n for n, k in enumerate(jobs_of(1) + jobs_of(0))}

    def landing(i, off):
        return region(S["loc_" + UNITS[i][1]], i, 0, pos(i, 0, off))

    def exchange(layer):
        for i, off in jobs_of(layer):
            n = jobs[i, off]
            for src, dst in pairs(i, off, 0, landing(i, off)):
                remote_copy(src, dst, S["ds"].at[n], S["dr"].at[n], sib).start()

    def exchanged(i, off):
        ref = landing(i, off)
        return remote_copy(ref, ref, S["ds"].at[jobs[i, off]], S["dr"].at[jobs[i, off]], sib)
    exchange(1)
    sib_waited = set()

    def wait_terms(i, off):
        off %= SIZE[UNITS[i][4][0]]
        n = SIZE[UNITS[i][4][0]]
        off = off - n if off > n // 2 else off
        if (i, off) not in sib_waited:
            sib_waited.add((i, off))
            exchanged(i, off).wait_recv()

    uses = {a: [] for a in "ugd"}
    for events in steps:
        for kind, level, key, s, k in events:
            if level == 0:
                h = SIZE[UNITS[key][4][0]] // 2
                if kind == "start" or k < h:
                    uses[UNITS[key][1]].append((key, h if kind == "start" else s * (h - k)))
    nth = {a: 0 for a in "ugd"}
    fetched = {a: 0 for a in "ugd"}

    def stage(a, n):
        i = uses[a][n][0]
        return S["stage_" + a].at[n % NB, :, :, :, pl.ds(0, UNITS[i][3])]

    layers = {1}

    def fetch_ahead(a):
        while fetched[a] < min(len(uses[a]), nth[a] + NB):
            n = fetched[a]
            i, off = uses[a][n]
            if UNITS[i][0] not in layers:
                return
            for src, dst in pairs(i, off, 1, stage(a, n)):
                pltpu.make_async_copy(src, dst, S["stsem_" + a].at[n % NB]).start()
            fetched[a] += 1

    own_fetched = set()

    sent = {}

    def own_buffer(i):
        return S["slot0_%d" % i].at[0, 0]

    def fetch_own(i):
        if i not in own_fetched and i in sent:
            sent[i]().wait_send()
            own_fetched.add(i)
            for src, dst in pairs(i, 0, 1, own_buffer(i)):
                pltpu.make_async_copy(src, dst, S["ownsem"].at[i]).start()

    def operands(level, i, off):
        _, a, _, _, o = UNITS[i]
        v = pos(i, level, off)
        here = region(S["loc_" + a], i, level, v)
        if level == 0:
            wait_terms(i, off)
            n = nth[a]
            assert uses[a][n] == (i, off)
            assert fetched[a] > n
            buf = stage(a, n)
            pltpu.make_async_copy(buf, buf, S["stsem_" + a].at[n % NB]).wait()
            nth[a] += 1
            return [buf, here]
        h = SIZE[o[0]] // 2
        first = [own_buffer(i)] + [S["slot0_%d" % i].at[d, h - 1] for d in (0, 1)]
        if level == 1:
            return [here] + [f.at[v] for f in first]
        w = pos(i, 1, 0)
        return [here] + [f.at[w, v] for f in first] + [S["slot1_%d" % i].at[d, 1, v] for d in (0, 1)]

    def half(ref, which, level, a):
        if level == 2 and TALL[a] == 1:
            return ref.at[..., pl.ds(896, 768) if which else pl.ds(0, 896)]
        n = ref.shape[0] // 2
        return ref.at[pl.ds(n * which, n)]

    def parts(key):
        r = []
        for i, u in enumerate(UNITS):
            if u[:2] == key:
                for lo, hi in ((0, 896), (896, 1664)):
                    a, b = max(lo, u[2]), min(hi, u[2] + u[3])
                    if a < b:
                        r.append((i, pl.ds(a - u[2], b - a), pl.ds(a, b - a), lo > 0))
        return r

    def cut(ref, cs):
        return ref.at[..., cs]

    def event(ev):
        kind, level, key, s, k = ev
        l, a = UNITS[key][:2] if level < 2 else key
        tag = "%d" % key if level < 2 else "%d%s" % key
        dim = UNITS[key][4][level] if level < 2 else LASTDIM[a]
        h = SIZE[dim] // 2
        if kind == "end":
            finish(l, a)
            return
        slot, rsem, ssem = (S["%s%d_%s" % (n, level, tag)] for n in ("slot", "r", "s"))

        def send(src, d, k):
            dst = lambda: slot.at[d, k] if k else half(slot.at[d, 0], d, level, a)
            remote(lambda: remote_copy(src(), dst(), ssem.at[d, k], rsem.at[d, k], near[dim, 1 - 2 * d]))

        if kind == "start":
            if level == 1:
                wait_terms(key, 0)
                fetch_own(key)
                assert key in own_fetched
                pltpu.make_async_copy(own_buffer(key), own_buffer(key), S["ownsem"].at[key]).wait()
            dst = (lambda: S["first_" + tag]) if level == 2 else (lambda: region(S["loc_" + a], key, level, pos(key, level, h)))
            if level < 2:
                addsum(dst(), operands(level, key, h))
            else:
                for i, uc, sc, _ in parts(key):
                    addsum(cut(dst(), sc), [cut(o, uc) for o in operands(level, i, h)])
            for d in (0, 1):
                send(lambda d=d: half(dst(), d, level, a), d, 0)
            if level == 0:
                fetch_own(key)
                fetch_ahead(a)
            return
        d = 0 if s > 0 else 1
        block = slot.at[d, k - 1]
        got = half(block, d, level, a) if k == 1 else block
        remote_copy(got, got, ssem.at[d, k - 1], rsem.at[d, k - 1], sib).wait_recv()
        if k == h:
            if level == 0:
                fetch_own(key)
            return
        off = s * (h - k)
        if level < 2:
            ops = operands(level, key, off)
            if k > 1:
                addsum(block, [block] + ops)
            else:
                for w in (0, 1):
                    hm = half(block, w, level, a)
                    addsum(hm, ([hm] if w == d else []) + [half(r, w, level, a) for r in ops])
        else:
            for i, uc, sc, w in parts(key):
                ops = [cut(o, uc) for o in operands(level, i, off)]
                m = cut(block, sc)
                if k > 1:
                    addsum(m, [m] + ops)
                elif TALL[a] == 1:
                    addsum(m, ([m] if w == (d == 1) else []) + ops)
                else:
                    for w in (0, 1):
                        hm = half(m, w, level, a)
                        addsum(hm, ([hm] if w == d else []) + [half(r, w, level, a) for r in ops])
        send(lambda: slot.at[d, k - 1], d, k)
        if (level, d, k) == (0, 0, 1):
            sent[key] = pend.pop()
        if level == 0:
            fetch_ahead(a)

    def finish(l, a):
        h = SIZE[LASTDIM[a]] // 2
        for i, uc, sc, _ in parts((l, a)):
            ops = [cut(o, uc) for o in operands(2, i, 0)] + [cut(S["slot2_%d%s" % (l, a)].at[d, h - 1], sc) for d in (0, 1)]
            addsum(cut(S["red_" + a].at[l], sc), ops)

    for a in "ugd":
        fetch_ahead(a)
    first = 0
    for n, events in zip(TASKS, steps, strict=False):
        for ev in events:
            event(ev)
        if not first:
            for cp in whole:
                cp.wait()

        def task(j, _):
            p = lax.rem(j, 2)
            for cp in inputs(j, p):
                cp.wait()

            @pl.when(j < 12)
            def _():
                for cp in inputs(j + 1, 1 - p):
                    cp.start()

            @pl.when(j >= 2)
            def _():
                for cp in outputs_done(p):
                    cp.wait()
            dh = dot(S["dh"][...], S["wd"][p], NT)
            S["res_d"][p] = dot(S["ht"][p], S["dh"][...]).reshape(32, 8, 1024).astype(BF)
            _, dgate, dup = silu_back(S["gate"][p], S["up"][p], dh.astype(BF).astype(F32))
            S["res_u"][p] = dot(S["at"][...], dup).reshape(4, 4, 8, 8, 256).astype(BF)
            S["res_g"][p] = dot(S["at"][...], dgate).reshape(4, 4, 8, 8, 256).astype(BF)
            for cp in outputs(j, p):
                cp.start()
            return 0
        lax.fori_loop(first, first + n, task, 0)
        first += n
    for p in (1, 0):
        for cp in outputs_done(p):
            cp.wait()
    exchange(0)
    layers.add(0)
    for a in "ugd":
        fetch_ahead(a)
    for ev in steps[-1]:
        event(ev)
    for i, off in jobs:
        exchanged(i, off).wait_send()
        wait_terms(i, off)

    total = jnp.zeros((8, 128), F32)
    for a in "ugd":
        for l in (0, 1):
            for t in range(TALL[a]):
                for q in range(WIDTH[a] // 128):
                    g = S["red_" + a][l, t, :, q * 128:q * 128 + 128].astype(F32)
                    if a == "d":
                        row = lax.broadcasted_iota(jnp.int32, (8, 128), 0) + 8 * t
                        g = jnp.where((row >= 2 * zz) & (row < 2 * zz + 26), g, 0.0)
                    total = total + g * g
    total = jnp.sum(total, axis=0, keepdims=True)
    for r, (buf, ds) in enumerate(((S["ar_z"], [(0, 0, q // 2, q % 2) for q in range(16)]), (S["ar_p"], [(q // 4, q % 4, 0, 0) for q in range(16)]))):
        buf[0] = total
        cps = []
        for q in range(1, 16):
            dx, dy, dz, dc = ds[q]
            to = device({"x": lax.rem(at["x"] + dx, 4), "y": lax.rem(at["y"] + dy, 4), "z": lax.rem(at["z"] + dz, 8), "c": lax.rem(c + dc, 2)})
            cps.append(remote(lambda q=q, to=to: remote_copy(buf.at[0], buf.at[q], S["arsem"].at[2 * r, q], S["arsem"].at[2 * r + 1, q], to)))
        for cp in cps:
            cp.wait_recv()
            cp.wait_send()
            pend.pop()
        total = buf[0]
        for q in range(1, 16):
            total = total + buf[q]
    mean = jnp.sum(total, axis=1, keepdims=True) / COUNT
    factor = jnp.minimum(1.0, 0.5 * lax.rsqrt(mean + 1e-30))
    for cp in moment_copies:
        cp.wait_recv() if cp.is_remote else cp.wait()

    def adamw(w, m, v, g):
        g = g * factor
        m = 0.9 * m + 0.1 * g
        v = 0.95 * v + 0.05 * g * g
        step = m * lax.rsqrt(v + 1e-8) + 0.1 * w
        return (w - 0.02 * step).astype(BF), m, v

    for a in "ug":
        mv, red, wv = S["mv_" + a], S["red_" + a], S["w_" + a]

        def body(q, _, mv=mv, red=red, wv=wv, a=a):
            cs = pl.ds(pl.multiple_of(q * 128, 128), 128)
            for l in (0, 1):
                m, v = (jnp.concatenate([mv[e, 0, l, :, cs], mv[e, 1, l, :, cs]], axis=0) for e in (0, 1))
                n, m, v = adamw(wv[l, 0, :, cs].astype(F32), m, v, red[l, 0, :, cs].astype(F32))
                wv[l, 0, :, cs] = n
                for e, t in enumerate((m, v)):
                    for s in (0, 1):
                        mv[e, s, l, :, cs] = t[4 * s:4 * s + 4]
            return 0
        lax.fori_loop(0, 13, body, 0)
    row = lax.broadcasted_iota(jnp.int32, (32, 32), 0)
    column = lax.broadcasted_iota(jnp.int32, (32, 32), 1)
    pick = (column == 2 * zz + 13 * (row >> 4) + (row & 15)) & ((row & 15) < 13)
    pick = jnp.where(pick, 1.0, 0.0).astype(BF)
    S["wide_d"][...] = jnp.zeros((2, 2, 16, 512), F32)
    for l in (0, 1):
        gd, wd = (jnp.dot(pick, S[n][l].reshape(32, 512), preferred_element_type=F32) for n in ("red_d", "w_d"))
        for s in (0, 1):
            rows = slice(16 * s, 16 * s + 13)
            n, m, v = adamw(wd[rows], S["mv_d"][0, s, :, l], S["mv_d"][1, s, :, l], gd[rows])
            S["wide_d"][l, s, 0:13] = n.astype(F32)
            S["new_d"][l, s] = S["wide_d"][l, s].astype(BF)
            S["mv_d"][0, s, :, l] = m
            S["mv_d"][1, s, :, l] = v
    ends = []
    for j, a in enumerate("ugd"):
        cp = pltpu.make_async_copy(S["new_d"] if a == "d" else S["w_" + a].at[:, 0], new[a], S["newsem"].at[j])
        cp.start()
        ends.append(cp.wait)
        for q in (0, 1):
            out = new_moments[a][q].at[:, :, halfcols(a, 1)]
            cp = remote_copy(S["mv_" + a].at[q, 1 - c], out, S["finsem"].at[j, q, 0], S["finsem"].at[j, q, 1], sib)
            cp.start()
            back = remote_copy(S["mv_" + a].at[q, 1 - c], new_moments[a][q].at[:, :, halfcols(a, 0)], S["finsem"].at[j, q, 0], S["finsem"].at[j, q, 1], sib)
            ends += [cp.wait_send, back.wait_recv]
            cp = pltpu.make_async_copy(S["mv_" + a].at[q, c], out, S["finsem"].at[j, q, 2])
            cp.start()
            ends.append(cp.wait)
    for wait in ends:
        wait()
    for make in pend:
        make().wait_send()


def reduce_scatter(grads, acts, weights, w_down, m, v):
    args = [g.reshape(4, 4, -1, 8, g.shape[-1]) for g in grads] + list(acts)
    args += [w.reshape(2, 4, 4, -1, 8, w.shape[-1]) for w in weights] + [w_down, *m, *v]
    sh = rs_scratch()
    any_ = pl.BlockSpec(memory_space=pl.ANY)
    outs = [jax.ShapeDtypeStruct(s, BF) for s in ((2, 8, 1664), (2, 8, 1664), (2, 2, 16, 512))] + [jax.ShapeDtypeStruct(t.shape, F32) for t in (*m, *v)]
    outs += [jax.ShapeDtypeStruct(s, BF) for s in ((4, 4, 8, 8, 3328), (4, 4, 8, 8, 3328), (4, 104, 8, 1024))]
    outs = pl.pallas_call(
        functools.partial(rs_kernel, list(sh)), out_shape=outs, in_specs=[any_] * 18, out_specs=[any_] * 12, scratch_shapes=list(sh.values()), name="reduce_scatter",
        compiler_params=pltpu.CompilerParams(collective_id=0, has_side_effects=True, vmem_limit_bytes=VMEM_BYTES))(*args)
    return outs[:3], outs[3:6], outs[6:9]


def plan_ag():
    RATE, LAT = 46.0e3, 2.9
    free, heap, order, seq, got, now = {}, [], [], [0], {}, 1.0

    def push(t, ev):
        seq[0] += 1
        heapq.heappush(heap, (t, seq[0], ev))

    def send(t, link, nbytes):
        free[link] = max(free.get(link, 0.0), t) + nbytes / RATE
        return free[link] + LAT
    ring = {(2, a): (LASTDIM[a], {"u": 8 * 1664, "g": 8 * 1664, "d": 32 * 512}[a] * 4) for a in "ugd"}
    for i, (_, a, _, cols, o) in enumerate(UNITS):
        ring[1, i] = (o[1], DEPTH[a] * 8 * cols * 2)
        ring[0, i] = (o[0], 4 * DEPTH[a] * 8 * cols * 2)
    for a in "gdu":
        push(1.0, ("start", 2, a, 0, 0))
    while heap:
        t, _, ev = heapq.heappop(heap)
        kind, level, key, s, k = ev
        dim, nbytes = ring[level, key]
        h = SIZE[dim] // 2
        now = max(now, t) + 0.1
        order.append(ev)
        if kind == "start":
            for s in (1, -1):
                push(send(now, (dim, s), nbytes), ("step", level, key, s, 1))
            continue
        if k < h:
            push(send(now, (dim, s), nbytes if k < h - 1 else nbytes // 2), ("step", level, key, s, k + 1))
            continue
        got[level, key] = got.get((level, key), 0) + 1
        if got[level, key] < 2:
            continue
        if level == 2:
            for i, u in enumerate(UNITS):
                if u[1] == key:
                    push(now + (1.0 if key == "d" else 0), ("start", 1, i, 0, 0))
        elif level == 1:
            push(now, ("start", 0, key, 0, 0))
    return order, now, free


def ag_scratch():
    sem = pltpu.SemaphoreType.DMA
    sh = {"pc": pltpu.VMEM((8, 2, 2, 16, 512), BF), "asm": pltpu.VMEM((2, 26, 8, 512), BF), "loc": sem((4,)), "sr": sem((128,)), "ss": sem((128,))}
    for n in "rs":
        for a in "ugd":
            sh["%s2_%s" % (n, a)] = sem((2, SIZE[LASTDIM[a]] // 2))
        for i, u in enumerate(UNITS):
            for lv in (0, 1):
                sh["%s%d_%d" % (n, lv, i)] = sem((2, SIZE[u[4][lv]] // 2))
    return sh


def ag_kernel(names, *refs):
    own = {a: refs[j] for j, a in enumerate("ugd")}
    out = {a: refs[3 + j] for j, a in enumerate("ugd")}
    S = dict(zip(names, refs[6:], strict=True))
    at = coords()
    c, x, y, z = at["c"], at["x"], at["y"], at["z"]
    sib = device({**at, "c": 1 - c})
    order, _, _ = plan_ag()
    spots, near = places(at)
    peers = [sib, *near.values()]
    bar = pltpu.get_barrier_semaphore()
    for p in peers:
        pl.semaphore_signal(bar, inc=1, device_id=p, device_id_type=MESH)

    def hc(a, col=0, n=None):
        return pl.ds(pl.multiple_of(c * WIDTH[a] + col, 128), WIDTH[a] if n is None else n)
    local = [pltpu.make_async_copy(own["u"], out["u"].at[:, x, y, z, :, hc("u")], S["loc"].at[0]),
             pltpu.make_async_copy(own["g"], out["g"].at[:, x, y, z, :, hc("g")], S["loc"].at[1]),
             pltpu.make_async_copy(own["d"], S["pc"].at[z], S["loc"].at[2])]
    for cp in local:
        cp.start()
    pl.semaphore_wait(bar, len(peers))
    for cp in local:
        cp.wait()
    pend, twin = [], []

    def remote(src, ss, rs, to):
        cp = remote_copy(src, src, ss, rs, to)
        cp.start()
        pend.append(cp)

    def to_sibling(ref):
        n = len(twin)
        remote(ref, S["ss"].at[n], S["sr"].at[n], sib)
        twin.append(ref)

    def region(level, key, v):
        if level == 2:
            if key == "d":
                return S["pc"].at[v]
            return out["u"].at[:, x, v, z, :, hc("u")] if key == "u" else out["g"].at[:, x, y, v, :, hc("g")]
        l, a, col, n, o = UNITS[key]
        idx = view(a, o, at, level, v)
        return out[a].at[(l, *idx, *([ALL] * (4 - len(idx))), hc(a, col, n))]

    def half(ref, which):
        n = ref.shape[0] // 2
        return ref.at[pl.ds(n * which, n)]

    got = {}
    for kind, level, key, s, k in order:
        dim = UNITS[key][4][level] if level < 2 else LASTDIM[key]
        n = SIZE[dim]
        h = n // 2
        rsem, ssem = S["r%d_%s" % (level, key)], S["s%d_%s" % (level, key)]

        def send(src, d, k, dim=dim, rsem=rsem, ssem=ssem):
            remote(src, ssem.at[d, k], rsem.at[d, k], near[dim, 1 - 2 * d])

        if kind == "start":
            for d in (0, 1):
                send(region(level, key, at[dim]), d, 0)
            continue
        d = 0 if s > 0 else 1
        block = region(level, key, spots[dim][-s * k % n])
        if k == h:
            block = half(block, d)
        remote_copy(block, block, ssem.at[d, k - 1], rsem.at[d, k - 1], sib).wait_recv()
        if k < h - 1:
            send(block, d, k)
        elif k == h - 1:
            send(half(block, d), d, k)
        if level < 2:
            to_sibling(block)
        if k == h:
            got[level, key] = got.get((level, key), 0) + 1
            if level == 2 and got[level, key] == 2:
                if key == "d":
                    q = lax.broadcasted_iota(jnp.int32, (208, 256), 1)
                    r = lax.broadcasted_iota(jnp.int32, (208, 256), 0)
                    e = q & 15
                    pick = (r == 26 * (q >> 5) + 13 * ((q >> 4) & 1) + e) & (e < 13)
                    pick = jnp.where(pick, 1.0, 0.0).astype(BF)
                    for l in (0, 1):
                        rows = jnp.dot(pick, S["pc"][:, l].reshape(256, 512), preferred_element_type=F32)
                        S["asm"][l] = rows.reshape(26, 8, 512).astype(BF)
                    cp = pltpu.make_async_copy(S["asm"], out["d"].at[:, x, y, :, :, hc("d")], S["loc"].at[3])
                    cp.start()
                    cp.wait()
                idx = (ALL, x, ALL, z, ALL) if key == "u" else (ALL, x, y, ALL, ALL)
                to_sibling(out[key].at[(*idx, hc(key))])
    for n, ref in enumerate(twin):
        remote_copy(ref, ref, S["ss"].at[n], S["sr"].at[n], sib).wait_recv()
    for cp in pend:
        cp.wait_send()


def all_gather(u, g, d):
    sh = ag_scratch()
    any_ = pl.BlockSpec(memory_space=pl.ANY)
    outs = [jax.ShapeDtypeStruct((2, 4, 4, TILES[a], 8, 2 * WIDTH[a]), BF) for a in "ugd"]
    return pl.pallas_call(
        functools.partial(ag_kernel, list(sh)), out_shape=outs, in_specs=[pl.BlockSpec(memory_space=pltpu.HBM)] * 3, out_specs=[any_] * 3, scratch_shapes=list(sh.values()), name="all_gather",
        compiler_params=pltpu.CompilerParams(collective_id=1, has_side_effects=True, vmem_limit_bytes=AG_VMEM))(u, g, d)


def settle_kernel(*refs):
    ins, outs, sem = refs[:3], refs[3:6], refs[6]
    copies = [pltpu.make_async_copy(ins[n].at[l, x], outs[n].at[l, x], sem.at[n, l, x]) for l in (0, 1) for x in range(4) for n in range(3)]
    for cp in copies:
        cp.start()
    for cp in copies:
        cp.wait()


def settle(*gathered):
    any_ = pl.BlockSpec(memory_space=pl.ANY)
    return pl.pallas_call(
        settle_kernel, out_shape=[jax.ShapeDtypeStruct(t.shape, t.dtype) for t in gathered], in_specs=[any_] * 3, out_specs=[pl.BlockSpec(memory_space=pltpu.HBM)] * 3,
        scratch_shapes=[pltpu.SemaphoreType.DMA((3, 2, 4))], name="settle", compiler_params=pltpu.CompilerParams(vmem_limit_bytes=2**20))(*gathered)


def solution(mesh):
    def step(x, dy, w_gate, w_up, w_down, *moments):
        x, dy = x[0], dy[0]
        gate0, up0, hid0, h1, a0 = layer0(x, w_gate, w_up, w_down)
        down1, gate1, up1, dh1 = layer1(h1, dy, w_gate, w_up, w_down)
        m, v = moments[:3], moments[3:]
        order = lambda t: (t[1], t[0], t[2])
        turned = lambda t: (*t[:2], t[2].transpose(1, 0, 2))
        acts = (dh1, a0, gate0, up0, hid0)
        new, m, v = reduce_scatter((up1, gate1, down1), acts, order((w_gate, w_up, w_down)), w_down, turned(order(m)), turned(order(v)))
        u, g, d = settle(*all_gather(*new))
        w = (g.reshape(w_gate.shape), u.reshape(w_up.shape), d.reshape(w_down.shape))
        return (*w, *order(turned(m)), *order(turned(v)))

    data, whole, rows = P(("rep", "dp"), None, None), P(), P(None, "dp", None)
    out = P("rep", None, None)
    return jax.shard_map(step, mesh=mesh, in_specs=(data, data) + (whole,) * 3 + (rows,) * 6, out_specs=(out,) * 3 + (P("rep", "dp", None),) * 6, check_vma=False)
```

```python
import functools
import heapq

import jax
import jax.numpy as jnp
from jax import lax
from jax.experimental import pallas as pl
from jax.experimental.pallas import tpu as pltpu
from jax.sharding import PartitionSpec as P

MESH = pl.DeviceIdType.MESH
BF, F32 = jnp.bfloat16, jnp.float32
SIZE = {"x": 4, "y": 4, "z": 8}
VMEM_BYTES = 67043328
AG_VMEM = 4 * 2**20
ALL = slice(None)


def coords():
    i = lax.axis_index("dp")
    return {"x": i // 64, "y": lax.rem(i // 16, 4), "z": lax.rem(i // 2, 8), "c": lax.rem(i, 2)}


def device(at):
    return {"dp": ((at["x"] * 4 + at["y"]) * 8 + at["z"]) * 2 + at["c"]}


def places(at):
    spots = {d: [at[d]] + [lax.rem(at[d] + k, n) for k in range(1, n)] for d, n in SIZE.items()}
    return spots, {(d, s): device({**at, d: spots[d][s]}) for d in SIZE for s in (1, -1)}


UNITS = [
    (1, "d", 0, 256, "xyz"), (1, "d", 256, 256, "yxz"), (1, "u", 0, 896, "zxy"), (1, "u", 896, 768, "zxy"), (1, "g", 0, 896, "xyz"), (1, "g", 896, 768, "yxz"),
    (0, "d", 0, 256, "xyz"), (0, "d", 256, 256, "yxz"), (0, "u", 0, 896, "zxy"), (0, "u", 896, 768, "zxy"), (0, "g", 0, 896, "yxz"), (0, "g", 896, 768, "xyz"),
]
DEPTH = {"u": 4, "g": 8, "d": 26}
TILES = {"u": 8, "g": 8, "d": 26}
WIDTH = {"u": 1664, "g": 1664, "d": 512}
TALL = {"u": 1, "g": 1, "d": 4}
LASTDIM = {"u": "y", "g": "z", "d": "z"}
MOMENTS = {"u": (2, 4), "g": (2, 4), "d": (13, 2)}
COUNT = 2 * 3 * 1024 * 3328
NB = 2


def view(a, order, at, level, v):
    if level == 0:
        return {"z": (ALL, ALL, v), "x": (v,), "y": (ALL, v)}[order[0]]
    if level == 1:
        return {"zxy": (v, ALL, at["z"]), "xyz": (at["x"], v), "yxz": (v, at["y"])}[order]
    return (at["x"], v, at["z"]) if a == "u" else (at["x"], at["y"], v)


def block_shape(i, level):
    _, a, _, cols, _ = UNITS[i]
    return ((4, DEPTH[a], 8, cols), (DEPTH[a], 8, cols))[level]


def remote_copy(src, dst, ss, rs, to):
    return pltpu.make_async_remote_copy(src_ref=src, dst_ref=dst, send_sem=ss, recv_sem=rs, device_id=to, device_id_type=MESH)


T = 1024
B = 256
N = 3328 // B
NT = (((1,), (1,)), ((), ()))


def dot(a, b, dims=(((1,), (0,)), ((), ()))):
    return lax.dot_general(a, b, dims, preferred_element_type=F32)


def norm_scale(wide):
    return lax.rsqrt(jnp.mean(wide**2, -1, keepdims=True) + 1e-6)


def rowwise(n, body, step=128):
    def one(i, _):
        body(pl.ds(pl.multiple_of(i * step, step), step))
        return 0
    lax.fori_loop(0, n // step, one, 0)


def silu_back(g, u, dh):
    s = jax.nn.sigmoid(g)
    silu = g * s
    return silu, (dh * u * (s + silu * (1.0 - s))).astype(BF), (dh * silu).astype(BF)


def norm_into(h, a):
    def norm(rows):
        wide = h[rows].astype(F32)
        a[rows] = (wide * norm_scale(wide)).astype(BF)
    rowwise(T, norm)


def pipelined(chunk, first, second):
    held = None
    for m in range(0, T, chunk):
        rows = slice(m, m + chunk)
        now = first(rows)
        if held is not None:
            second(*held)
        held = rows, now
    second(*held)


def fwd0(C, tr, x, wg, wu, wd, gate, up, ht, h1, at, a, hid):
    j = pl.program_id(0)

    @pl.when(j == 0)
    def _():
        norm_into(x, a)
        at[...] = a[...].T if tr else a[...]

    @pl.when(j < N)
    def _():
        def first(rows):
            return dot(a[rows], wg[...]), dot(a[rows], wu[...])

        def second(rows, gu):
            g, u = gu
            gate[rows] = g
            up[rows] = u
            v = (g * jax.nn.sigmoid(g) * u).astype(BF)
            hid[j, rows] = v
            if tr:
                ht[:, rows] = v.T
            else:
                ht[rows] = v
        pipelined(C, first, second)

    @pl.when(j >= N)
    def _():
        def first(rows):
            return sum(dot(hid[i, rows], wd[i * B:i * B + B]) for i in range(N))

        def second(rows, y):
            n = pl.ds(pl.multiple_of((j - N) * B, B), B)
            h1[rows] = (x[rows, n].astype(F32) + y.astype(BF).astype(F32)).astype(BF)
        pipelined(C, first, second)


def layer0(x, w_gate, w_up, w_down, C=512, tr=True):
    whole = pl.BlockSpec((T, T), lambda j: (0, 0))
    cap = lambda j: jnp.minimum(j, N - 1)
    cols = pl.BlockSpec((T, B), lambda j: (0, cap(j)))
    wcols = pl.BlockSpec((None, T, B), lambda j: (0, 0, cap(j)))
    late = lambda j: jnp.maximum(j - N, 0)
    wrows = pl.BlockSpec((None, 3328, B), lambda j: (0, 0, late(j)))
    rows = pl.BlockSpec((B, T), lambda j: (cap(j), 0)) if tr else cols
    o = jax.ShapeDtypeStruct
    blk = pl.BlockSpec((None, T, B), lambda j: (cap(j), 0, 0))
    return pl.pallas_call(functools.partial(fwd0, C, tr), grid=(N + 4,), in_specs=[whole, wcols, wcols, wrows],
        out_specs=[blk, blk, rows, pl.BlockSpec((T, B), lambda j: (0, late(j))), whole],
        out_shape=[o((N, T, B), F32)] * 2 + [o((3328, T) if tr else (T, 3328), BF), o((T, T), BF), o((T, T), BF)],
        scratch_shapes=[pltpu.VMEM((T, T), BF), pltpu.VMEM((N, T, B), BF)], name="layer0",
        compiler_params=pltpu.CompilerParams(vmem_limit_bytes=VMEM_BYTES))(x, w_gate, w_up, w_down)


def both1(h, dy, wg, wu, wd, wg2, wu2, dwd, dwg, dwu, dh1, a, at, gs, us, hta, htb, acc):
    j = pl.program_id(0)

    @pl.when(j == 0)
    def _():
        norm_into(h, a)
        at[...] = a[...].T

    def now():
        return dot(a[...], wg[...]), dot(a[...], wu[...]), dot(dy[...], wd[...], NT)

    def before(ht):
        dwd[...] = dot(ht[...], dy[...]).astype(BF)
        dwg[...] = dot(at[...], gs[j - 1]).astype(BF)
        dwu[...] = dot(at[...], us[j - 1]).astype(BF)

    def then(g, u, dh, ht):
        silu, dgate, dup = silu_back(g, u, dh.astype(BF).astype(F32))
        gs[j] = dgate
        us[j] = dup
        ht[...] = (silu * u).astype(BF).T

    @pl.when(j == 0)
    def _():
        then(*now(), hta)

    for p, (mine, last) in enumerate(((hta, htb), (htb, hta))):
        @pl.when((j > 0) & (j < N) & (lax.rem(j, 2) == p))
        def _():
            x = now()
            before(last)
            then(*x, mine)

    @pl.when(j == N)
    def _():
        before(hta)

    @pl.when(j >= N)
    def _():
        y = sum(dot(gs[i], wg2[:, i * B:i * B + B], NT) + dot(us[i], wu2[:, i * B:i * B + B], NT) for i in range(N))
        acc[:, pl.ds(pl.multiple_of((j - N) * B, B), B)] = y

    @pl.when(j == N + 3)
    def _():
        def back(rows):
            wide = h[rows].astype(F32)
            scale = norm_scale(wide)
            d = acc[rows].astype(BF).astype(F32)
            d = d * scale - wide * (scale * scale * scale * jnp.mean(d * wide, -1, keepdims=True))
            dh1[rows] = (dy[rows].astype(F32) + d.astype(BF).astype(F32)).astype(BF)
        rowwise(T, back)


def layer1(h, dy, w_gate, w_up, w_down):
    cap = lambda j: jnp.minimum(j, N - 1)
    prev = lambda j: jnp.clip(j - 1, 0, N - 1)
    late = lambda j: jnp.maximum(j - N, 0)
    whole = pl.BlockSpec((T, T), lambda j: (0, 0))
    cols = pl.BlockSpec((T, B), lambda j: (0, prev(j)))
    wcols = pl.BlockSpec((None, T, B), lambda j: (1, 0, cap(j)))
    wrows = pl.BlockSpec((None, B, T), lambda j: (1, cap(j), 0))
    wtall = pl.BlockSpec((None, B, 3328), lambda j: (1, late(j), 0))
    rows = pl.BlockSpec((B, T), lambda j: (prev(j), 0))
    o = jax.ShapeDtypeStruct
    return pl.pallas_call(both1, grid=(N + 4,), in_specs=[whole, whole, wcols, wcols, wrows, wtall, wtall], out_specs=[rows, cols, cols, whole],
        out_shape=[o((3328, T), BF)] + [o((T, 3328), BF)] * 2 + [o((T, T), BF)],
        scratch_shapes=[pltpu.VMEM((T, T), BF)] * 2 + [pltpu.VMEM((N, T, B), BF)] * 2 + [pltpu.VMEM((B, T), BF)] * 2 + [pltpu.VMEM((T, T), F32)], name="layer1",
        compiler_params=pltpu.CompilerParams(vmem_limit_bytes=VMEM_BYTES))(h, dy, w_gate, w_up, w_down, w_gate, w_up)


TASKS = (2, 3, 4, 4)


def jobs_of(layer):
    rank = {}
    for i, u in enumerate(UNITS):
        if u[0] == layer:
            n = SIZE[u[4][0]]
            h = n // 2
            for at, off in enumerate([h] + [s * (h - k) for k in range(1, h) for s in (1, -1)] + [0]):
                rank[i, off] = (at / n, i)
    return sorted(rank, key=rank.get)


def plan():
    RATE, LAT, TASK, DRATE, DLAT = 46.0e3, 3.0, 2.7, 600.0e3, 2.0
    free, heap, seq = {}, [], [0]

    def send(t, link, nbytes):
        free[link] = max(free.get(link, 0.0), t) + nbytes / RATE
        return free[link] + LAT

    def push(t, ev):
        seq[0] += 1
        heapq.heappush(heap, (t, seq[0], ev))
    ring = {}
    for i, (l, a, _, cols, o) in enumerate(UNITS):
        ring[0, i] = (o[0], 4 * DEPTH[a] * 8 * cols * 2)
        ring[1, i] = (o[1], DEPTH[a] * 8 * cols * 2)
        ring[2, (l, a)] = (LASTDIM[a], TALL[a] * 8 * WIDTH[a] * 2)
    arrive, got, steps, now = {}, {}, [], 2.0

    def exchange(layer, t):
        for i, off in jobs_of(layer):
            t += ring[0, i][1] / DRATE
            arrive[i, off] = t + DLAT
            if off == SIZE[UNITS[i][4][0]] // 2:
                push(arrive[i, off], ("start", 0, i, 0, 0))

    def run(until):
        nonlocal now
        taken = []
        while heap and heap[0][0] <= until:
            t, _, ev = heapq.heappop(heap)
            kind, level, key, s, k = ev
            dim, nbytes = ring[level, key]
            h = SIZE[dim] // 2
            if level == 0 and kind == "step" and k < h and arrive[key, s * (h - k)] > t:
                push(arrive[key, s * (h - k)], ev)
                continue
            now = max(now, t)
            taken.append(ev)
            cost = 0.15 + nbytes * (4 + 2 * level) / 7.0e6
            if kind == "end":
                continue
            if kind == "start":
                now += cost
                for s in (1, -1):
                    push(send(now, (dim, s), nbytes // 2), ("step", level, key, s, 1))
            elif k < h:
                now += cost
                push(send(now, (dim, s), nbytes), ("step", level, key, s, k + 1))
            else:
                got[level, key] = got.get((level, key), 0) + 1
                if got[level, key] < 2:
                    continue
                if level == 0:
                    push(now, ("start", 1, key, 0, 0))
                elif level == 1:
                    ka = UNITS[key][:2]
                    if all(got.get((1, i)) == 2 for i, u in enumerate(UNITS) if u[:2] == ka):
                        push(now, ("start", 2, ka, 0, 0))
                else:
                    push(now, ("end", 2, key, 0, 0))
        return taken
    exchange(1, now)
    now = max(now, FIRST)
    for n in TASKS:
        steps.append(run(now))
        now += n * TASK
    exchange(0, now)
    steps.append(run(float("inf")))
    return steps, now, free


FIRST = 1.0


def addsum(dst, srcs):
    def add(*at):
        acc = srcs[0][at].astype(F32)
        for s in srcs[1:]:
            acc = acc + s[at].astype(F32)
        dst[at] = acc.astype(BF)

    if len(dst.shape) == 4:

        def body(i, _):
            add(i)
            return 0
        lax.fori_loop(0, dst.shape[0], body, 0)
    else:
        add(...)


def rs_scratch():
    sh = {}
    sem = pltpu.SemaphoreType.DMA
    for a in "ugd":
        sh["loc_" + a] = pltpu.VMEM((2, 4, 4, TILES[a], 8, WIDTH[a]), BF)
        sh["stage_" + a] = pltpu.VMEM((NB, 4, DEPTH[a], 8, max(u[3] for u in UNITS if u[1] == a)), BF)
        sh["stsem_" + a] = sem((NB,))
        sh["red_" + a] = pltpu.VMEM((2, TALL[a], 8, WIDTH[a]), BF)
        sh["mv_" + a] = pltpu.VMEM((2, 2, *MOMENTS[a], WIDTH[a]), F32)
        sh["w_" + a] = pltpu.VMEM((2, TALL[a], 8, WIDTH[a]), BF)
        h = SIZE[LASTDIM[a]] // 2
        for l in (0, 1):
            sh["slot2_%d%s" % (l, a)] = pltpu.VMEM((2, h, TALL[a], 8, WIDTH[a]), BF)
            sh["first_%d%s" % (l, a)] = pltpu.VMEM((TALL[a], 8, WIDTH[a]), BF)
            for n in "rs":
                sh["%s2_%d%s" % (n, l, a)] = sem((2, h))
    sh["new_d"] = pltpu.VMEM((2, 2, 16, 512), BF)
    sh["wide_d"] = pltpu.VMEM((2, 2, 16, 512), F32)
    for i, u in enumerate(UNITS):
        h = SIZE[u[4][0]] // 2
        sh["slot0_%d" % i] = pltpu.VMEM((2, h) + block_shape(i, 0), BF)
        sh["slot1_%d" % i] = pltpu.VMEM((2, 2) + block_shape(i, 1), BF)
        for n in "rs":
            sh["%s0_%d" % (n, i)] = sem((2, h))
            sh["%s1_%d" % (n, i)] = sem((2, 2))
    sh["ownsem"] = sem((len(UNITS),))
    sh["dh"] = pltpu.VMEM((1024, 1024), BF)
    sh["at"] = pltpu.VMEM((1024, 1024), BF)
    sh["gate"] = pltpu.VMEM((2, 1024, 256), F32)
    sh["up"] = pltpu.VMEM((2, 1024, 256), F32)
    sh["wd"] = pltpu.VMEM((2, 256, 1024), BF)
    sh["ht"] = pltpu.VMEM((2, 256, 1024), BF)
    sh["res_u"] = pltpu.VMEM((2, 4, 4, 8, 8, 256), BF)
    sh["res_g"] = pltpu.VMEM((2, 4, 4, 8, 8, 256), BF)
    sh["res_d"] = pltpu.VMEM((2, 32, 8, 1024), BF)
    sh["insem"] = sem((4, 2))
    sh["outsem"] = sem((3, 2))
    sh["wholesem"] = sem((2,))
    sh["dr"] = sem((64,))
    sh["ds"] = sem((64,))
    sh["ar_z"] = pltpu.VMEM((16, 1, 128), F32)
    sh["ar_p"] = pltpu.VMEM((16, 1, 128), F32)
    sh["arsem"] = sem((4, 16))
    sh["mvsem"] = sem((3, 2, 3))
    sh["wsem"] = sem((3,))
    sh["finsem"] = sem((3, 2, 3))
    sh["newsem"] = sem((3,))
    return sh


def rs_kernel(names, *refs):
    given = {a: refs[j] for j, a in enumerate("ugd")}
    acts = dict(zip(("dh", "at", "gate", "up", "ht"), refs[3:8], strict=True))
    weights = {a: refs[8 + j] for j, a in enumerate("ugd")}
    w_down = refs[11]
    moments = {a: (refs[12 + j], refs[15 + j]) for j, a in enumerate("ugd")}
    new = {"u": refs[18].at[0], "g": refs[18].at[1], "d": refs[19]}
    new_moments = {a: (refs[20 + j], refs[23 + j]) for j, a in enumerate("ugd")}
    made = {a: refs[26 + j] for j, a in enumerate("ugd")}
    S = dict(zip(names, refs[29:], strict=True))
    at = coords()
    c, x = at["c"], at["x"]
    sib = device({**at, "c": 1 - c})
    steps, _, _ = plan()
    spots, near = places(at)
    windows = [pl.ds(13 * lax.div(v, 4) + 3 * lax.rem(v, 4), 4) for v in spots["z"]]
    zz = lax.rem(at["z"], 4)

    peers = [device({**at, "z": lax.rem(at["z"] + dz, 8), "c": lax.rem(c + dc, 2)}) for dz in range(8) for dc in range(2)][1:]
    peers += [device({**at, "x": lax.rem(at["x"] + dx, 4), "y": lax.rem(at["y"] + dy, 4)}) for dx in range(4) for dy in range(4)][1:]
    bar = pltpu.get_barrier_semaphore()
    for p in peers:
        pl.semaphore_signal(bar, inc=1, device_id=p, device_id_type=MESH)

    def halfcols(a, which):
        w = WIDTH[a]
        return pl.ds(pl.multiple_of((c if which else 1 - c) * w, 128), w)

    def inputs(j, p):
        rows = pl.ds(pl.multiple_of(j * 256, 256), 256)
        pairs = ((acts["gate"].at[j], S["gate"]), (acts["up"].at[j], S["up"]), (w_down.at[0, rows], S["wd"]), (acts["ht"].at[rows], S["ht"]))
        return [pltpu.make_async_copy(src, dst.at[p], S["insem"].at[n, p]) for n, (src, dst) in enumerate(pairs)]

    def outputs(j, p):
        cols = pl.ds(pl.multiple_of(j * 256, 256), 256)
        pairs = [(S["res_" + a].at[p], made[a].at[:, :, :, :, cols], n) for n, a in enumerate("ug")]
        for q in range(4):
            tile = j * 32 + 8 * q
            pairs.append((S["res_d"].at[p, pl.ds(8 * q, 8)], made["d"].at[lax.div(tile, 104), pl.ds(lax.rem(tile, 104), 8)], 2))
        return [pltpu.make_async_copy(src, dst, S["outsem"].at[n, p]) for src, dst, n in pairs]

    def outputs_done(p):
        return [pltpu.make_async_copy(S["res_" + a].at[p], S["res_" + a].at[p], S["outsem"].at[n, p]) for n, a in enumerate("ugd")]
    whole = [pltpu.make_async_copy(acts[n], S[n], S["wholesem"].at[k]) for k, n in enumerate(("dh", "at"))]
    for cp in [*inputs(0, 0), *whole]:
        cp.start()

    moment_copies = []
    for j, a in enumerate("ugd"):
        for q in (0, 1):
            ref = moments[a][q]
            moment_copies.append(pltpu.make_async_copy(ref.at[:, :, halfcols(a, 1)], S["mv_" + a].at[q, c], S["mvsem"].at[j, q, 2]))
        tile = windows[0] if a == "d" else pl.ds(at["z"], 1)
        moment_copies.append(pltpu.make_async_copy(weights[a].at[:, at["x"], at["y"], tile, :, halfcols(a, 1)], S["w_" + a], S["wsem"].at[j]))
    for cp in moment_copies:
        cp.start()
    pl.semaphore_wait(bar, len(peers))
    pend = []

    def remote(make):
        cp = make()
        cp.start()
        pend.append(make)
        return cp
    def region(ref, i, level, v):
        l, a, col, n, o = UNITS[i]
        idx = view(a, o, at, level, v)
        return ref.at[(l, *idx, *([ALL] * (4 - len(idx))), pl.ds(col, n))]

    def pairs(i, off, which, dst):
        l, a, col, n, o = UNITS[i]
        cols = pl.ds(pl.multiple_of((c if which else 1 - c) * WIDTH[a] + col, 128), n)
        v = pos(i, 0, off)
        if a == "d" and not l:
            if o[0] == "x":
                return [(made["d"].at[v, pl.ds(26 * q, 26), :, cols], dst.at[q]) for q in range(4)]
            return [(made["d"].at[:, pl.ds(26 * v, 26), :, cols], dst)]
        idx = view(a, o, at, 0, v)
        return [((given if l else made)[a].at[(*idx, *([ALL] * (4 - len(idx))), cols)], dst)]

    def pos(i, level, off):
        a = UNITS[i][1]
        dim = UNITS[i][4][level] if level < 2 else LASTDIM[a]
        off %= SIZE[dim]
        if level < 2:
            return spots[dim][off]
        return windows[off] if a == "d" else pl.ds(spots[dim][off], 1)

    jobs = {k: n for n, k in enumerate(jobs_of(1) + jobs_of(0))}

    def landing(i, off):
        return region(S["loc_" + UNITS[i][1]], i, 0, pos(i, 0, off))

    def exchange(layer):
        for i, off in jobs_of(layer):
            n = jobs[i, off]
            for src, dst in pairs(i, off, 0, landing(i, off)):
                remote_copy(src, dst, S["ds"].at[n], S["dr"].at[n], sib).start()

    def exchanged(i, off):
        ref = landing(i, off)
        return remote_copy(ref, ref, S["ds"].at[jobs[i, off]], S["dr"].at[jobs[i, off]], sib)
    exchange(1)
    for j, a in enumerate("ugd"):
        for q in (0, 1):
            moment_copies.append(remote(lambda j=j, a=a, q=q: remote_copy(
                moments[a][q].at[:, :, halfcols(a, 0)], S["mv_" + a].at[q, c], S["mvsem"].at[j, q, 0], S["mvsem"].at[j, q, 1], sib)))

    sib_waited = set()

    def wait_terms(i, off):
        off %= SIZE[UNITS[i][4][0]]
        n = SIZE[UNITS[i][4][0]]
        off = off - n if off > n // 2 else off
        if (i, off) not in sib_waited:
            sib_waited.add((i, off))
            exchanged(i, off).wait_recv()

    uses = {a: [] for a in "ugd"}
    for events in steps:
        for kind, level, key, s, k in events:
            if level == 0:
                h = SIZE[UNITS[key][4][0]] // 2
                if kind == "start" or k < h:
                    uses[UNITS[key][1]].append((key, h if kind == "start" else s * (h - k)))
    nth = {a: 0 for a in "ugd"}
    fetched = {a: 0 for a in "ugd"}

    def stage(a, n):
        i = uses[a][n][0]
        return S["stage_" + a].at[n % NB, :, :, :, pl.ds(0, UNITS[i][3])]

    layers = {1}

    def fetch_ahead(a):
        while fetched[a] < min(len(uses[a]), nth[a] + NB):
            n = fetched[a]
            i, off = uses[a][n]
            if UNITS[i][0] not in layers:
                return
            for src, dst in pairs(i, off, 1, stage(a, n)):
                pltpu.make_async_copy(src, dst, S["stsem_" + a].at[n % NB]).start()
            fetched[a] += 1

    own_fetched = set()

    sent = {}

    def own_buffer(i):
        return S["slot0_%d" % i].at[0, 0]

    def fetch_own(i):
        if i not in own_fetched and i in sent:
            sent[i]().wait_send()
            own_fetched.add(i)
            for src, dst in pairs(i, 0, 1, own_buffer(i)):
                pltpu.make_async_copy(src, dst, S["ownsem"].at[i]).start()

    def operands(level, i, off):
        _, a, _, _, o = UNITS[i]
        v = pos(i, level, off)
        here = region(S["loc_" + a], i, level, v)
        if level == 0:
            wait_terms(i, off)
            n = nth[a]
            assert uses[a][n] == (i, off)
            assert fetched[a] > n
            buf = stage(a, n)
            pltpu.make_async_copy(buf, buf, S["stsem_" + a].at[n % NB]).wait()
            nth[a] += 1
            return [buf, here]
        h = SIZE[o[0]] // 2
        first = [own_buffer(i)] + [S["slot0_%d" % i].at[d, h - 1] for d in (0, 1)]
        if level == 1:
            return [here] + [f.at[v] for f in first]
        w = pos(i, 1, 0)
        return [here] + [f.at[w, v] for f in first] + [S["slot1_%d" % i].at[d, 1, v] for d in (0, 1)]

    def half(ref, which, level, a):
        if level == 2 and TALL[a] == 1:
            return ref.at[..., pl.ds(896, 768) if which else pl.ds(0, 896)]
        n = ref.shape[0] // 2
        return ref.at[pl.ds(n * which, n)]

    def parts(key):
        r = []
        for i, u in enumerate(UNITS):
            if u[:2] == key:
                for lo, hi in ((0, 896), (896, 1664)):
                    a, b = max(lo, u[2]), min(hi, u[2] + u[3])
                    if a < b:
                        r.append((i, pl.ds(a - u[2], b - a), pl.ds(a, b - a), lo > 0))
        return r

    def cut(ref, cs):
        return ref.at[..., cs]

    def event(ev):
        kind, level, key, s, k = ev
        l, a = UNITS[key][:2] if level < 2 else key
        tag = "%d" % key if level < 2 else "%d%s" % key
        dim = UNITS[key][4][level] if level < 2 else LASTDIM[a]
        h = SIZE[dim] // 2
        if kind == "end":
            finish(l, a)
            return
        slot, rsem, ssem = (S["%s%d_%s" % (n, level, tag)] for n in ("slot", "r", "s"))

        def send(src, d, k):
            dst = lambda: slot.at[d, k] if k else half(slot.at[d, 0], d, level, a)
            remote(lambda: remote_copy(src(), dst(), ssem.at[d, k], rsem.at[d, k], near[dim, 1 - 2 * d]))

        if kind == "start":
            if level == 1:
                wait_terms(key, 0)
                fetch_own(key)
                assert key in own_fetched
                pltpu.make_async_copy(own_buffer(key), own_buffer(key), S["ownsem"].at[key]).wait()
            dst = (lambda: S["first_" + tag]) if level == 2 else (lambda: region(S["loc_" + a], key, level, pos(key, level, h)))
            if level < 2:
                addsum(dst(), operands(level, key, h))
            else:
                for i, uc, sc, _ in parts(key):
                    addsum(cut(dst(), sc), [cut(o, uc) for o in operands(level, i, h)])
            for d in (0, 1):
                send(lambda d=d: half(dst(), d, level, a), d, 0)
            if level == 0:
                fetch_own(key)
                fetch_ahead(a)
            return
        d = 0 if s > 0 else 1
        block = slot.at[d, k - 1]
        got = half(block, d, level, a) if k == 1 else block
        remote_copy(got, got, ssem.at[d, k - 1], rsem.at[d, k - 1], sib).wait_recv()
        if k == h:
            if level == 0:
                fetch_own(key)
            return
        off = s * (h - k)
        if level < 2:
            ops = operands(level, key, off)
            if k > 1:
                addsum(block, [block] + ops)
            else:
                for w in (0, 1):
                    hm = half(block, w, level, a)
                    addsum(hm, ([hm] if w == d else []) + [half(r, w, level, a) for r in ops])
        else:
            for i, uc, sc, w in parts(key):
                ops = [cut(o, uc) for o in operands(level, i, off)]
                m = cut(block, sc)
                if k > 1:
                    addsum(m, [m] + ops)
                elif TALL[a] == 1:
                    addsum(m, ([m] if w == (d == 1) else []) + ops)
                else:
                    for w in (0, 1):
                        hm = half(m, w, level, a)
                        addsum(hm, ([hm] if w == d else []) + [half(r, w, level, a) for r in ops])
        send(lambda: slot.at[d, k - 1], d, k)
        if (level, d, k) == (0, 0, 1):
            sent[key] = pend.pop()
        if level == 0:
            fetch_ahead(a)

    def finish(l, a):
        h = SIZE[LASTDIM[a]] // 2
        for i, uc, sc, _ in parts((l, a)):
            ops = [cut(o, uc) for o in operands(2, i, 0)] + [cut(S["slot2_%d%s" % (l, a)].at[d, h - 1], sc) for d in (0, 1)]
            addsum(cut(S["red_" + a].at[l], sc), ops)

    for a in "ugd":
        fetch_ahead(a)
    first = 0
    for n, events in zip(TASKS, steps, strict=False):
        for ev in events:
            event(ev)
        if not first:
            for cp in whole:
                cp.wait()

        def task(j, _):
            p = lax.rem(j, 2)
            for cp in inputs(j, p):
                cp.wait()

            @pl.when(j < 12)
            def _():
                for cp in inputs(j + 1, 1 - p):
                    cp.start()

            @pl.when(j >= 2)
            def _():
                for cp in outputs_done(p):
                    cp.wait()
            dh = dot(S["dh"][...], S["wd"][p], NT)
            S["res_d"][p] = dot(S["ht"][p], S["dh"][...]).reshape(32, 8, 1024).astype(BF)
            _, dgate, dup = silu_back(S["gate"][p], S["up"][p], dh.astype(BF).astype(F32))
            S["res_u"][p] = dot(S["at"][...], dup).reshape(4, 4, 8, 8, 256).astype(BF)
            S["res_g"][p] = dot(S["at"][...], dgate).reshape(4, 4, 8, 8, 256).astype(BF)
            for cp in outputs(j, p):
                cp.start()
            return 0
        lax.fori_loop(first, first + n, task, 0)
        first += n
    for p in (1, 0):
        for cp in outputs_done(p):
            cp.wait()
    exchange(0)
    layers.add(0)
    for a in "ugd":
        fetch_ahead(a)
    for ev in steps[-1]:
        event(ev)
    for i, off in jobs:
        exchanged(i, off).wait_send()
        wait_terms(i, off)

    total = jnp.zeros((8, 128), F32)
    for a in "ugd":
        for l in (0, 1):
            for t in range(TALL[a]):
                for q in range(WIDTH[a] // 128):
                    g = S["red_" + a][l, t, :, q * 128:q * 128 + 128].astype(F32)
                    if a == "d":
                        row = lax.broadcasted_iota(jnp.int32, (8, 128), 0) + 8 * t
                        g = jnp.where((row >= 2 * zz) & (row < 2 * zz + 26), g, 0.0)
                    total = total + g * g
    total = jnp.sum(total, axis=0, keepdims=True)
    for r, (buf, ds) in enumerate(((S["ar_z"], [(0, 0, q // 2, q % 2) for q in range(16)]), (S["ar_p"], [(q // 4, q % 4, 0, 0) for q in range(16)]))):
        buf[0] = total
        cps = []
        for q in range(1, 16):
            dx, dy, dz, dc = ds[q]
            to = device({"x": lax.rem(at["x"] + dx, 4), "y": lax.rem(at["y"] + dy, 4), "z": lax.rem(at["z"] + dz, 8), "c": lax.rem(c + dc, 2)})
            cps.append(remote(lambda q=q, to=to: remote_copy(buf.at[0], buf.at[q], S["arsem"].at[2 * r, q], S["arsem"].at[2 * r + 1, q], to)))
        for cp in cps:
            cp.wait_recv()
            cp.wait_send()
            pend.pop()
        total = buf[0]
        for q in range(1, 16):
            total = total + buf[q]
    mean = jnp.sum(total, axis=1, keepdims=True) / COUNT
    factor = jnp.minimum(1.0, 0.5 * lax.rsqrt(mean + 1e-30))
    for cp in moment_copies:
        cp.wait_recv() if cp.is_remote else cp.wait()

    def adamw(w, m, v, g):
        g = g * factor
        m = 0.9 * m + 0.1 * g
        v = 0.95 * v + 0.05 * g * g
        step = m * lax.rsqrt(v + 1e-8) + 0.1 * w
        return (w - 0.02 * step).astype(BF), m, v

    for a in "ug":
        mv, red, wv = S["mv_" + a], S["red_" + a], S["w_" + a]

        def body(q, _, mv=mv, red=red, wv=wv, a=a):
            cs = pl.ds(pl.multiple_of(q * 128, 128), 128)
            for l in (0, 1):
                m, v = (jnp.concatenate([mv[e, 0, l, :, cs], mv[e, 1, l, :, cs]], axis=0) for e in (0, 1))
                n, m, v = adamw(wv[l, 0, :, cs].astype(F32), m, v, red[l, 0, :, cs].astype(F32))
                wv[l, 0, :, cs] = n
                for e, t in enumerate((m, v)):
                    for s in (0, 1):
                        mv[e, s, l, :, cs] = t[4 * s:4 * s + 4]
            return 0
        lax.fori_loop(0, 13, body, 0)
    row = lax.broadcasted_iota(jnp.int32, (32, 32), 0)
    column = lax.broadcasted_iota(jnp.int32, (32, 32), 1)
    pick = (column == 2 * zz + 13 * (row >> 4) + (row & 15)) & ((row & 15) < 13)
    pick = jnp.where(pick, 1.0, 0.0).astype(BF)
    S["wide_d"][...] = jnp.zeros((2, 2, 16, 512), F32)
    for l in (0, 1):
        gd, wd = (jnp.dot(pick, S[n][l].reshape(32, 512), preferred_element_type=F32) for n in ("red_d", "w_d"))
        for s in (0, 1):
            rows = slice(16 * s, 16 * s + 13)
            n, m, v = adamw(wd[rows], S["mv_d"][0, s, :, l], S["mv_d"][1, s, :, l], gd[rows])
            S["wide_d"][l, s, 0:13] = n.astype(F32)
            S["new_d"][l, s] = S["wide_d"][l, s].astype(BF)
            S["mv_d"][0, s, :, l] = m
            S["mv_d"][1, s, :, l] = v
    ends = []
    for j, a in enumerate("ugd"):
        cp = pltpu.make_async_copy(S["new_d"] if a == "d" else S["w_" + a].at[:, 0], new[a], S["newsem"].at[j])
        cp.start()
        ends.append(cp.wait)
        for q in (0, 1):
            out = new_moments[a][q].at[:, :, halfcols(a, 1)]
            cp = remote_copy(S["mv_" + a].at[q, 1 - c], out, S["finsem"].at[j, q, 0], S["finsem"].at[j, q, 1], sib)
            cp.start()
            back = remote_copy(S["mv_" + a].at[q, 1 - c], new_moments[a][q].at[:, :, halfcols(a, 0)], S["finsem"].at[j, q, 0], S["finsem"].at[j, q, 1], sib)
            ends += [cp.wait_send, back.wait_recv]
            cp = pltpu.make_async_copy(S["mv_" + a].at[q, c], out, S["finsem"].at[j, q, 2])
            cp.start()
            ends.append(cp.wait)
    for wait in ends:
        wait()
    for make in pend:
        make().wait_send()


def reduce_scatter(grads, acts, weights, w_down, m, v):
    args = [g.reshape(4, 4, -1, 8, g.shape[-1]) for g in grads] + list(acts)
    args += [w.reshape(2, 4, 4, -1, 8, w.shape[-1]) for w in weights] + [w_down, *m, *v]
    sh = rs_scratch()
    any_ = pl.BlockSpec(memory_space=pl.ANY)
    outs = [jax.ShapeDtypeStruct(s, BF) for s in ((2, 2, 8, 1664), (2, 2, 16, 512))] + [jax.ShapeDtypeStruct(t.shape, F32) for t in (*m, *v)]
    outs += [jax.ShapeDtypeStruct(s, BF) for s in ((4, 4, 8, 8, 3328), (4, 4, 8, 8, 3328), (4, 104, 8, 1024))]
    outs = pl.pallas_call(
        functools.partial(rs_kernel, list(sh)), out_shape=outs, in_specs=[any_] * 18, out_specs=[any_] * 11, scratch_shapes=list(sh.values()), name="reduce_scatter",
        compiler_params=pltpu.CompilerParams(collective_id=0, has_side_effects=True, vmem_limit_bytes=VMEM_BYTES))(*args)
    return outs[:2], outs[2:5], outs[5:8]


def plan_ag():
    RATE, LAT = 46.0e3, 2.9
    free, heap, order, seq, got, now = {}, [], [], [0], {}, 1.0

    def push(t, ev):
        seq[0] += 1
        heapq.heappush(heap, (t, seq[0], ev))

    def send(t, link, nbytes):
        free[link] = max(free.get(link, 0.0), t) + nbytes / RATE
        return free[link] + LAT
    ring = {(2, a): (LASTDIM[a], {"u": 8 * 1664, "g": 8 * 1664, "d": 32 * 512}[a] * 4) for a in "ugd"}
    for i, (_, a, _, cols, o) in enumerate(UNITS):
        ring[1, i] = (o[1], DEPTH[a] * 8 * cols * 2)
        ring[0, i] = (o[0], 4 * DEPTH[a] * 8 * cols * 2)
    for a in "gdu":
        push(1.0, ("start", 2, a, 0, 0))
    while heap:
        t, _, ev = heapq.heappop(heap)
        kind, level, key, s, k = ev
        dim, nbytes = ring[level, key]
        h = SIZE[dim] // 2
        now = max(now, t) + 0.1
        order.append(ev)
        if kind == "start":
            for s in (1, -1):
                push(send(now, (dim, s), nbytes), ("step", level, key, s, 1))
            continue
        if k < h:
            push(send(now, (dim, s), nbytes if k < h - 1 else nbytes // 2), ("step", level, key, s, k + 1))
            continue
        got[level, key] = got.get((level, key), 0) + 1
        if got[level, key] < 2:
            continue
        if level == 2:
            for i, u in enumerate(UNITS):
                if u[1] == key:
                    push(now + (1.0 if key == "d" else 0), ("start", 1, i, 0, 0))
        elif level == 1:
            push(now, ("start", 0, key, 0, 0))
    return order, now, free


def ag_scratch():
    sem = pltpu.SemaphoreType.DMA
    sh = {"pc": pltpu.VMEM((8, 2, 2, 16, 512), BF), "asm": pltpu.VMEM((2, 26, 8, 512), BF), "loc": sem((4,)), "sr": sem((128,)), "ss": sem((128,))}
    for n in "rs":
        for a in "ugd":
            sh["%s2_%s" % (n, a)] = sem((2, SIZE[LASTDIM[a]] // 2))
        for i, u in enumerate(UNITS):
            for lv in (0, 1):
                sh["%s%d_%d" % (n, lv, i)] = sem((2, SIZE[u[4][lv]] // 2))
    return sh


def ag_kernel(names, *refs):
    own = {"u": refs[0].at[0], "g": refs[0].at[1], "d": refs[1]}
    out = {a: refs[2 + j] for j, a in enumerate("ugd")}
    S = dict(zip(names, refs[5:], strict=True))
    at = coords()
    c, x, y, z = at["c"], at["x"], at["y"], at["z"]
    sib = device({**at, "c": 1 - c})
    order, _, _ = plan_ag()
    spots, near = places(at)
    peers = [sib, *near.values()]
    bar = pltpu.get_barrier_semaphore()
    for p in peers:
        pl.semaphore_signal(bar, inc=1, device_id=p, device_id_type=MESH)

    def hc(a, col=0, n=None):
        return pl.ds(pl.multiple_of(c * WIDTH[a] + col, 128), WIDTH[a] if n is None else n)
    local = [pltpu.make_async_copy(own["u"], out["u"].at[:, x, y, z, :, hc("u")], S["loc"].at[0]),
             pltpu.make_async_copy(own["g"], out["g"].at[:, x, y, z, :, hc("g")], S["loc"].at[1]),
             pltpu.make_async_copy(own["d"], S["pc"].at[z], S["loc"].at[2])]
    for cp in local:
        cp.start()
    pl.semaphore_wait(bar, len(peers))
    for cp in local:
        cp.wait()
    pend, twin = [], []

    def remote(src, ss, rs, to):
        cp = remote_copy(src, src, ss, rs, to)
        cp.start()
        pend.append(cp)

    def to_sibling(ref):
        n = len(twin)
        remote(ref, S["ss"].at[n], S["sr"].at[n], sib)
        twin.append(ref)

    def region(level, key, v):
        if level == 2:
            if key == "d":
                return S["pc"].at[v]
            return out["u"].at[:, x, v, z, :, hc("u")] if key == "u" else out["g"].at[:, x, y, v, :, hc("g")]
        l, a, col, n, o = UNITS[key]
        idx = view(a, o, at, level, v)
        return out[a].at[(l, *idx, *([ALL] * (4 - len(idx))), hc(a, col, n))]

    def half(ref, which):
        n = ref.shape[0] // 2
        return ref.at[pl.ds(n * which, n)]

    got = {}
    for kind, level, key, s, k in order:
        dim = UNITS[key][4][level] if level < 2 else LASTDIM[key]
        n = SIZE[dim]
        h = n // 2
        rsem, ssem = S["r%d_%s" % (level, key)], S["s%d_%s" % (level, key)]

        def send(src, d, k, dim=dim, rsem=rsem, ssem=ssem):
            remote(src, ssem.at[d, k], rsem.at[d, k], near[dim, 1 - 2 * d])

        if kind == "start":
            for d in (0, 1):
                send(region(level, key, at[dim]), d, 0)
            continue
        d = 0 if s > 0 else 1
        block = region(level, key, spots[dim][-s * k % n])
        if k == h:
            block = half(block, d)
        remote_copy(block, block, ssem.at[d, k - 1], rsem.at[d, k - 1], sib).wait_recv()
        if k < h - 1:
            send(block, d, k)
        elif k == h - 1:
            send(half(block, d), d, k)
        if level < 2:
            to_sibling(block)
        if k == h:
            got[level, key] = got.get((level, key), 0) + 1
            if level == 2 and got[level, key] == 2:
                if key == "d":
                    q = lax.broadcasted_iota(jnp.int32, (208, 256), 1)
                    r = lax.broadcasted_iota(jnp.int32, (208, 256), 0)
                    e = q & 15
                    pick = (r == 26 * (q >> 5) + 13 * ((q >> 4) & 1) + e) & (e < 13)
                    pick = jnp.where(pick, 1.0, 0.0).astype(BF)
                    for l in (0, 1):
                        rows = jnp.dot(pick, S["pc"][:, l].reshape(256, 512), preferred_element_type=F32)
                        S["asm"][l] = rows.reshape(26, 8, 512).astype(BF)
                    cp = pltpu.make_async_copy(S["asm"], out["d"].at[:, x, y, :, :, hc("d")], S["loc"].at[3])
                    cp.start()
                    cp.wait()
                idx = (ALL, x, ALL, z, ALL) if key == "u" else (ALL, x, y, ALL, ALL)
                to_sibling(out[key].at[(*idx, hc(key))])
    for n, ref in enumerate(twin):
        remote_copy(ref, ref, S["ss"].at[n], S["sr"].at[n], sib).wait_recv()
    for cp in pend:
        cp.wait_send()


def all_gather(ug, d):
    sh = ag_scratch()
    any_ = pl.BlockSpec(memory_space=pl.ANY)
    outs = [jax.ShapeDtypeStruct((2, 4, 4, TILES[a], 8, 2 * WIDTH[a]), BF) for a in "ugd"]
    return pl.pallas_call(
        functools.partial(ag_kernel, list(sh)), out_shape=outs, in_specs=[any_] * 2, out_specs=[any_] * 3, scratch_shapes=list(sh.values()), name="all_gather",
        compiler_params=pltpu.CompilerParams(collective_id=1, has_side_effects=True, vmem_limit_bytes=AG_VMEM))(ug, d)


def settle_kernel(*refs):
    ins, outs, sem = refs[:3], refs[3:6], refs[6]
    copies = [pltpu.make_async_copy(ins[n].at[l, x], outs[n].at[l, x], sem.at[n, l, x]) for l in (0, 1) for x in range(4) for n in range(3)]
    for cp in copies:
        cp.start()
    for cp in copies:
        cp.wait()


def settle(*gathered):
    any_ = pl.BlockSpec(memory_space=pl.ANY)
    return pl.pallas_call(
        settle_kernel, out_shape=[jax.ShapeDtypeStruct(t.shape, t.dtype) for t in gathered], in_specs=[any_] * 3, out_specs=[pl.BlockSpec(memory_space=pltpu.HBM)] * 3,
        scratch_shapes=[pltpu.SemaphoreType.DMA((3, 2, 4))], name="settle", compiler_params=pltpu.CompilerParams(vmem_limit_bytes=2**20))(*gathered)


def solution(mesh):
    def step(x, dy, w_gate, w_up, w_down, *moments):
        x, dy = x[0], dy[0]
        gate0, up0, hid0, h1, a0 = layer0(x, w_gate, w_up, w_down)
        down1, gate1, up1, dh1 = layer1(h1, dy, w_gate, w_up, w_down)
        m, v = moments[:3], moments[3:]
        order = lambda t: (t[1], t[0], t[2])
        turned = lambda t: (*t[:2], t[2].transpose(1, 0, 2))
        acts = (dh1, a0, gate0, up0, hid0)
        new, m, v = reduce_scatter((up1, gate1, down1), acts, order((w_gate, w_up, w_down)), w_down, turned(order(m)), turned(order(v)))
        u, g, d = settle(*all_gather(*new))
        w = (g.reshape(w_gate.shape), u.reshape(w_up.shape), d.reshape(w_down.shape))
        return (*w, *order(turned(m)), *order(turned(v)))

    data, whole, rows = P(("rep", "dp"), None, None), P(), P(None, "dp", None)
    out = P("rep", None, None)
    return jax.shard_map(step, mesh=mesh, in_specs=(data, data) + (whole,) * 3 + (rows,) * 6, out_specs=(out,) * 3 + (P("rep", "dp", None),) * 6, check_vma=False)
```
